128 devices in a mesh: data: 1, chip: 16 (over z, y), dap: 8 (over x, core).
Axes of the slice: x: 4, y: 4, z: 4, core: 2. Of those that a mesh axis runs over, the one named last changes fastest.
Arguments:
- m: bfloat16 [256, 512, 256], P(('data', 'chip', 'dap'))
- z: bfloat16 [512, 512, 128], P(('data', 'chip', 'dap'))
- msa_mask: int32 [256, 512], P('data')
- res_mask: int32 [512], P('data')
- w_row_in: bfloat16 [256, 1024], replicated
- w_row_bias: bfloat16 [128, 8], replicated
- w_row_out: bfloat16 [256, 256], replicated
- w_col_in: bfloat16 [256, 1024], replicated
- w_col_out: bfloat16 [256, 256], replicated
- w_opm_in: bfloat16 [256, 64], replicated
- w_opm_out: bfloat16 [1024, 128], replicated
- w_start_in: bfloat16 [128, 512], replicated
- w_start_bias: bfloat16 [128, 4], replicated
- w_start_out: bfloat16 [128, 128], replicated
- w_end_in: bfloat16 [128, 512], replicated
- w_end_bias: bfloat16 [128, 4], replicated
- w_end_out: bfloat16 [128, 128], replicated
Outputs:
- output 1: bfloat16 [256, 512, 256], P(('data', 'chip', 'dap'))
- output 2: bfloat16 [512, 512, 128], P(('data', 'chip', 'dap'))
All inputs are finite; a program needn't handle non-finite values.
Results may differ from the reference program's by a relative error of at most 0.0123337.
Values are sent between devices in bfloat16 or wider.
A program may use at most 1 GiB of HBM per device.

```python
import jax
import jax.numpy as jnp
from jax import lax

NUM_SEQ = 256
NUM_RES = 512
C_M = 256
C_Z = 128
HEADS_M = 8
HEAD_M = 32
HEADS_T = 4
HEAD_T = 32
OPM = 32


def layer_norm(x):
    values = x.astype(jnp.float32)
    centred = values - jnp.mean(values, axis=-1, keepdims=True)
    variance = jnp.mean(centred * centred, axis=-1, keepdims=True)
    return (centred * lax.rsqrt(variance + 1e-5)).astype(jnp.bfloat16)


def project(x, weight):
    return jnp.dot(x, weight, preferred_element_type=jnp.float32).astype(jnp.bfloat16)


def add_residual(state, update):
    return (state.astype(jnp.float32) + update).astype(jnp.bfloat16)


def gated_rows(projected, head_bias, key_ok, heads, head_dim):
    length = projected.shape[0]
    split_proj = projected.reshape(length, 4, heads, head_dim).astype(jnp.float32)
    scores = jnp.einsum('ihd,jhd->hij', split_proj[:, 0], split_proj[:, 1]) * head_dim ** -0.5
    if head_bias is not None:
        scores = scores + head_bias.astype(jnp.float32)
    scores = jnp.where(key_ok[None, None, :], scores, -1e9)
    attn_prob = jax.nn.softmax(scores, axis=-1).astype(jnp.bfloat16).astype(jnp.float32)
    mixed = jnp.einsum('hij,jhd->ihd', attn_prob, split_proj[:, 2])
    gated = (mixed * jax.nn.sigmoid(split_proj[:, 3])).astype(jnp.bfloat16)
    return gated.reshape(length, heads * head_dim)


def draw_masks(mask_key):
    seq_key, res_key = jax.random.split(mask_key)
    seq_idx = jnp.arange(NUM_SEQ)[:, None]
    res_idx = jnp.arange(NUM_RES)
    msa_draw = jax.random.randint(seq_key, (NUM_SEQ, NUM_RES), 0, 4)
    msa_mask = ((msa_draw != 0) | (seq_idx == 0) | (res_idx[None, :] == 0)).astype(jnp.int32)
    res_draw = jax.random.randint(res_key, (NUM_RES,), 0, 4)
    res_mask = ((res_draw != 0) | (res_idx == 0)).astype(jnp.int32)
    return msa_mask, res_mask


def dense(weight_key, rows, cols, gain):
    draw = jax.random.normal(weight_key, (rows, cols), jnp.float32)
    return (draw * (gain * rows ** -0.5)).astype(jnp.bfloat16)


def attn_in(weight_key, rows, heads, head_dim):
    draw = jax.random.normal(weight_key, (rows, 4, heads * head_dim), jnp.float32)
    boost = jnp.array([1.5, 1.5, 1.0, 1.0], jnp.float32)[None, :, None]
    return (draw * boost * rows ** -0.5).reshape(rows, 4 * heads * head_dim).astype(jnp.bfloat16)


def setup_inputs(seed: int = 0, part: int = 0) -> dict:
    part_keys = jax.random.split(jax.random.fold_in(jax.random.key(seed), part), 4)
    weight_keys = jax.random.split(jax.random.key(seed + 1), 13)
    profile = jax.random.normal(part_keys[0], (1, NUM_RES, C_M), jnp.float32)
    noise = jax.random.normal(part_keys[1], (NUM_SEQ, NUM_RES, C_M), jnp.float32)
    pair = jax.random.normal(part_keys[2], (NUM_RES, NUM_RES, C_Z), jnp.float32)
    msa_mask, res_mask = draw_masks(part_keys[3])
    return {
        'm': (profile + noise).astype(jnp.bfloat16),
        'z': pair.astype(jnp.bfloat16),
        'msa_mask': msa_mask,
        'res_mask': res_mask,
        'w_row_in': attn_in(weight_keys[0], C_M, HEADS_M, HEAD_M),
        'w_row_bias': dense(weight_keys[1], C_Z, HEADS_M, 1.5),
        'w_row_out': dense(weight_keys[2], HEADS_M * HEAD_M, C_M, 1.0),
        'w_col_in': attn_in(weight_keys[3], C_M, HEADS_M, HEAD_M),
        'w_col_out': dense(weight_keys[4], HEADS_M * HEAD_M, C_M, 1.0),
        'w_opm_in': dense(weight_keys[5], C_M, 2 * OPM, 1.0),
        'w_opm_out': dense(weight_keys[6], OPM * OPM, C_Z, 1.0),
        'w_start_in': attn_in(weight_keys[7], C_Z, HEADS_T, HEAD_T),
        'w_start_bias': dense(weight_keys[8], C_Z, HEADS_T, 1.5),
        'w_start_out': dense(weight_keys[9], HEADS_T * HEAD_T, C_Z, 1.0),
        'w_end_in': attn_in(weight_keys[10], C_Z, HEADS_T, HEAD_T),
        'w_end_bias': dense(weight_keys[11], C_Z, HEADS_T, 1.5),
        'w_end_out': dense(weight_keys[12], HEADS_T * HEAD_T, C_Z, 1.0),
    }


def reference(m, z, msa_mask, res_mask, w_row_in, w_row_bias, w_row_out, w_col_in, w_col_out,
              w_opm_in, w_opm_out, w_start_in, w_start_bias, w_start_out, w_end_in, w_end_bias, w_end_out):
    msa_ok = msa_mask != 0
    res_ok = res_mask != 0

    row_bias = jnp.transpose(project(layer_norm(z), w_row_bias), (2, 0, 1))
    row_proj = project(layer_norm(m), w_row_in)

    def row_step(step_in):
        return gated_rows(step_in[0], row_bias, step_in[1], HEADS_M, HEAD_M)

    row_gated = lax.map(row_step, (row_proj, msa_ok))
    m = add_residual(m, jnp.dot(row_gated, w_row_out, preferred_element_type=jnp.float32))

    col_proj = jnp.swapaxes(project(layer_norm(m), w_col_in), 0, 1)

    def col_step(step_in):
        return gated_rows(step_in[0], None, step_in[1], HEADS_M, HEAD_M)

    col_gated = jnp.swapaxes(lax.map(col_step, (col_proj, msa_ok.T)), 0, 1)
    m = add_residual(m, jnp.dot(col_gated, w_col_out, preferred_element_type=jnp.float32))

    outer_proj = project(layer_norm(m), w_opm_in)
    mask_w = msa_mask.astype(jnp.bfloat16)
    left = outer_proj[:, :, :OPM] * mask_w[:, :, None]
    right = (outer_proj[:, :, OPM:] * mask_w[:, :, None]).astype(jnp.float32)
    pair_norm = jnp.dot(mask_w.T, mask_w, preferred_element_type=jnp.float32)

    def outer_step(step_in):
        outer = jnp.einsum('sa,sjc->jac', step_in[0].astype(jnp.float32), right).astype(jnp.bfloat16)
        mapped = jnp.dot(outer.reshape(NUM_RES, OPM * OPM), w_opm_out, preferred_element_type=jnp.float32)
        return mapped / (1e-3 + step_in[1][:, None])

    z = add_residual(z, lax.map(outer_step, (jnp.swapaxes(left, 0, 1), pair_norm)))

    start_norm = layer_norm(z)
    start_proj = project(start_norm, w_start_in)
    start_bias = jnp.transpose(project(start_norm, w_start_bias), (2, 0, 1))

    def start_step(row_in):
        return gated_rows(row_in, start_bias, res_ok, HEADS_T, HEAD_T)

    start_gated = lax.map(start_step, start_proj)
    z = add_residual(z, jnp.dot(start_gated, w_start_out, preferred_element_type=jnp.float32))

    end_norm = layer_norm(z)
    end_proj = jnp.swapaxes(project(end_norm, w_end_in), 0, 1)
    end_bias = jnp.transpose(project(end_norm, w_end_bias), (2, 1, 0))

    def end_step(col_in):
        return gated_rows(col_in, end_bias, res_ok, HEADS_T, HEAD_T)

    end_gated = jnp.swapaxes(lax.map(end_step, end_proj), 0, 1)
    z = add_residual(z, jnp.dot(end_gated, w_end_out, preferred_element_type=jnp.float32))
    return m, z
```

```python
import functools

import jax
import jax.numpy as jnp
from jax import lax
from jax.experimental import pallas as pl
from jax.experimental.pallas import tpu as pltpu
from jax.sharding import PartitionSpec as P

N0 = 0
N1 = 1
N2 = 2
N3 = 3
N4 = 4
N7 = 7
N8 = 8
N15 = 15
N16 = 16
N32 = 32
N63 = 63
N64 = 64
N127 = 127
N128 = 128
N256 = 256
N384 = 384
N512 = 512
N768 = 768
N1024 = 1024
N2048 = 2048
N4096 = 4096
ALL = Ellipsis
MESH = pl.DeviceIdType.MESH
F32 = jnp.float32
BF16 = jnp.bfloat16
VMEM_LIMIT = 60 * N1024 * N1024


def layer_norm(x):
    values = x.astype(F32)
    centred = values - jnp.mean(values, axis=-N1, keepdims=True)
    variance = jnp.mean(centred * centred, axis=-N1, keepdims=True)
    return (centred * lax.rsqrt(variance + 1e-5)).astype(BF16)


def dot(a, b):
    return jnp.dot(a, b, preferred_element_type=F32)


def dot_t(a, b):
    return lax.dot_general(a, b, (((N1,), (N1,)), ((), ())), preferred_element_type=F32)


def dev(p):
    return (N0, p // N8, lax.rem(p, N8))


def my_index():
    return lax.axis_index('chip') * N8 + lax.axis_index('dap')


def loop(n, body):
    def step(i, carry):
        body(i)
        return carry
    lax.fori_loop(N0, n, step, N0)


def barrier_all(me):
    bar = pltpu.get_barrier_semaphore()

    def signal(k):
        pl.semaphore_signal(bar, inc=N1, device_id=dev(lax.rem(me + N1 + k, N128)), device_id_type=MESH)
    loop(N127, signal)
    pl.semaphore_wait(bar, N127)


def send(src, dst, send_sem, recv_sem, p):
    pltpu.make_async_remote_copy(src_ref=src, dst_ref=dst, send_sem=send_sem, recv_sem=recv_sem,
                                 device_id=dev(p), device_id_type=MESH).start()


def wait_bytes(ref, sem):
    pltpu.make_async_copy(ref, ref, sem).wait()


def head_rep(queries, heads):
    rows = queries * heads
    r = lax.broadcasted_iota(jnp.int32, (rows, queries), N0)
    c = lax.broadcasted_iota(jnp.int32, (rows, queries), N1)
    return (r // heads == c).astype(F32).astype(BF16)


def head_mask(rows, heads, width):
    r = lax.broadcasted_iota(jnp.int32, (rows, width), N0)
    c = lax.broadcasted_iota(jnp.int32, (rows, width), N1)
    return (lax.rem(r, heads) == c // N32).astype(F32)


def softmax_rows(t):
    e = jnp.exp(t - jnp.max(t, axis=N1, keepdims=True))
    return (e * (1.0 / jnp.sum(e, axis=N1, keepdims=True))).astype(BF16)


def put(ref, value):
    for t in range(ref.shape[N0]):
        ref[t] = value[:, t * N128:(t + N1) * N128]


def take(ref, start, size, stride):
    return jnp.concatenate([ref[t, pl.ds(start, size, stride=stride), :] for t in range(ref.shape[N0])], axis=N1)


def join(ref):
    return jnp.concatenate([ref[t] for t in range(ref.shape[N0])], axis=N1)


def spread(ref, start, size, stride, value):
    for t in range(ref.shape[N0]):
        ref[t, pl.ds(start, size, stride=stride), :] = value[:, t * N128:(t + N1) * N128]


def collapse(r_ref, queries, heads):
    lane = lax.broadcasted_iota(jnp.int32, (queries, N128), N1) // N32
    parts = []
    for t in range(r_ref.shape[N0]):
        out = r_ref[t, pl.ds(N4 * t, queries, stride=heads), :]
        for h in range(N1, N4):
            out = jnp.where(lane == h, r_ref[t, pl.ds(N4 * t + h, queries, stride=heads), :], out)
        parts.append(out)
    return jnp.concatenate(parts, axis=N1) if len(parts) > N1 else parts[N0]


def gate(o, g):
    return (o * jax.nn.sigmoid(g.astype(F32))).astype(BF16)


SCALE = N32 ** -0.5


def kernel_a(m_ref, z_ref, rmask_ref, cmask_ref, cmexp_ref, wbias_t_ref, w_row_in, w_row_out, w_col_in, w_col_out,
             w_left, w_right_t, mcols_ref, left_ref, right_ref,
             x_ref, slab_f, slab, bias, xn_ref, kv_ref, q_ref, g_ref, gt_ref, rep_ref, hm_ref, r_ref, y_ref, sendf, sendb,
             recvb, xs, qkvg, yf, gsem, xsem, ssem, asem, bsem):
    me = my_index()
    core = lax.rem(me, N2)
    chip = me // N2
    half = me // N64
    barrier_all(me)
    send(m_ref, x_ref.at[pl.ds(N2 * core, N2)], xsem.at[N0], xsem.at[N1], me + N1 - N2 * core)

    for il in range(N4):
        zn = layer_norm(z_ref[il])
        slab_f[il * N8:(il + N1) * N8, :] = dot_t(wbias_t_ref[ALL], zn)
    slab[ALL] = slab_f[ALL].astype(BF16)
    slot = me - N64 * half

    def send_slab(k):
        c = lax.rem(chip + N1 + k, N64)
        p = N2 * c + half

        @pl.when(p != me)
        def _():
            send(slab, bias.at[slot], ssem, gsem.at[slot // N16], p)
    loop(N64, send_slab)

    @pl.when(core == half)
    def _():
        bias[slot] = slab[ALL]

    rep_ref[ALL] = head_rep(N64, N8)
    hm_ref[ALL] = head_mask(N512, N8, N256)

    def project(s):
        xn_ref[ALL] = layer_norm(x_ref[s])
        kv_ref[s] = dot(xn_ref[ALL], w_row_in[:, N256:N768]).astype(BF16)
        xh = xn_ref[pl.ds(pl.multiple_of(core * N256, N256), N256), :]
        q_ref[s] = dot(xh, w_row_in[:, N0:N256]).astype(BF16)
        g_ref[s] = dot(xh, w_row_in[:, N768:N1024]).astype(BF16)

    def own(s):
        x_ref[N2 * core + s] = m_ref[s]
        project(N2 * core + s)
    loop(N2, own)
    wait_bytes(m_ref, xsem.at[N1])
    loop(N2, lambda s: project(N2 - N2 * core + s))

    def attend(b, s):
        qx = (dot(rep_ref[ALL], q_ref[s, pl.ds(pl.multiple_of(b * N64, N64), N64), :]) * hm_ref[ALL]).astype(BF16)
        t = dot_t(qx, kv_ref[s, :, N0:N256]) * SCALE + bias[pl.ds(b * N16, N16)].reshape(N512, N512).astype(F32)
        t = jnp.where(rmask_ref[pl.ds(s, N1), :] > N0, t, -1e9)
        put(r_ref, dot(softmax_rows(t), kv_ref[s, :, N256:N512]))
        rows = pl.ds(pl.multiple_of(b * N64, N64), N64)
        gt_ref[s, rows, :] = gate(collapse(r_ref, N64, N8), g_ref[s, rows, :])

    def block(b):
        @pl.when(jnp.logical_and(core == half, b == slot // N16))
        def _():
            wait_bytes(bias.at[pl.ds(N0, N15)], gsem.at[b])

        @pl.when(jnp.logical_not(jnp.logical_and(core == half, b == slot // N16)))
        def _():
            wait_bytes(bias.at[pl.ds(N0, N16)], gsem.at[b])
        loop(N4, lambda s: attend(b, s))
    loop(N4, block)

    def finish(s):
        rows = pl.ds(pl.multiple_of(core * N256, N256), N256)
        put(y_ref, x_ref[s, rows, :].astype(F32) + dot(gt_ref[s], w_row_out[ALL]))
        for jl in range(N4):
            spread(sendf, s * N4 + jl, N64, N16, take(y_ref, jl, N64, N4))
    loop(N4, finish)
    sendb[ALL] = join(sendf).astype(BF16).reshape(N64, N16, N256)

    def send_cols(k0):
        k = lax.rem(slot + N1 + k0, N64)
        q = N64 * core + k

        @pl.when(q != me)
        def _():
            send(sendb.at[k], recvb.at[chip], asem.at[N0], asem.at[N1], q)
    loop(N64, send_cols)

    @pl.when(core == half)
    def _():
        recvb[chip] = sendb[slot]
        wait_bytes(recvb.at[pl.ds(N0, N63)], asem.at[N1])

    @pl.when(core != half)
    def _():
        wait_bytes(recvb, asem.at[N1])
    put(xs, recvb[ALL].astype(F32).reshape(N1024, N256))

    for jl in range(N4):
        x = take(xs, jl, N256, N4)
        qkvg[ALL] = dot(layer_norm(x), w_col_in[ALL]).astype(BF16)

        def col_block(b, jl=jl):
            rows = pl.ds(pl.multiple_of(b * N64, N64), N64)
            qx = (dot(rep_ref[ALL], qkvg[rows, N0:N256]) * hm_ref[ALL]).astype(BF16)
            t = dot_t(qx, qkvg[:, N256:N512]) * SCALE
            t = jnp.where(cmask_ref[jl:jl + N1, :] > N0, t, -1e9)
            put(r_ref, dot(softmax_rows(t), qkvg[:, N512:N768]))
            gt_ref[N0, rows, :] = gate(collapse(r_ref, N64, N8), qkvg[rows, N768:N1024])
        loop(N4, col_block)
        y = (x + dot(gt_ref[N0], w_col_out[ALL])).astype(BF16)
        spread(yf, jl, N256, N4, y.astype(F32))
        xn2 = layer_norm(y)
        right = dot_t(w_right_t[ALL], xn2).astype(BF16).astype(F32) * cmask_ref[jl:jl + N1, :]
        right_ref[jl * N32:(jl + N1) * N32, :] = right.astype(BF16)
        part = dot(xn2, w_left[jl])
        y_ref[N0] = part if jl == N0 else y_ref[N0] + part
    left_ref[ALL] = (y_ref[N0].astype(BF16).astype(F32) * cmexp_ref[ALL]).astype(BF16)
    mcols_ref[ALL] = join(yf).astype(BF16).reshape(N128, N8, N256)

    wait_bytes(m_ref, xsem.at[N0])

    @pl.when(core == half)
    def _():
        wait_bytes(bias.at[pl.ds(N0, N63)], ssem)
        wait_bytes(recvb.at[pl.ds(N0, N63)], asem.at[N0])

    @pl.when(core != half)
    def _():
        wait_bytes(bias, ssem)
        wait_bytes(recvb, asem.at[N0])


def kernel_b(left_ref, right_ref, z_ref, mcols_ref, recip_ref, w_ref, zout_ref, mout_ref,
             l_ref, r_ref, zin, o_ref, bd_ref, acc, zs, csem, asem, zsem, msem, osem):
    me = my_index()
    u = me // N8
    v = lax.rem(me, N8)
    barrier_all(me)

    def send_c(k):
        send(right_ref, r_ref.at[u], csem.at[N0], csem.at[N1], lax.rem(u + N1 + k, N16) * N8 + v)
    loop(N15, send_c)

    def send_a(k):
        d = lax.rem(v + N1 + k, N8)
        send(left_ref, l_ref.at[v], asem.at[N0], asem.at[N1], u * N8 + d)
        send(z_ref.at[d], zin.at[v], zsem.at[N0], zsem.at[N1], u * N8 + d)
    loop(N7, send_a)

    def send_m(k):
        p = lax.rem(me + N1 + k, N128)
        send(mcols_ref.at[p], mout_ref.at[me], msem.at[N0], msem.at[N1], p)
    loop(N127, send_m)
    r_ref[u] = right_ref[ALL]
    l_ref[v] = left_ref[ALL]
    zin[v] = z_ref[v]
    mout_ref[me] = mcols_ref[me]

    bd_ref[ALL] = jnp.zeros_like(bd_ref)

    def build(c2):
        for e in range(N2):
            w = w_ref[pl.ds(pl.multiple_of((N2 * c2 + e) * N32, N32), N32), :]
            for il in range(N4):
                bd_ref[c2, e * N128 + il * N32:e * N128 + (il + N1) * N32, il * N128:(il + N1) * N128] = w
    loop(N16, build)
    wait_bytes(r_ref.at[pl.ds(N0, N15)], csem.at[N1])
    wait_bytes(l_ref.at[pl.ds(N0, N7)], asem.at[N1])

    def outer(d):
        o_ref[pl.ds(pl.multiple_of(d * N2048, N2048), N2048), :] = dot(r_ref[ALL].reshape(N2048, N256), l_ref[d])
    loop(N8, outer)
    acc[ALL] = jnp.zeros_like(acc)

    def mix(c2):
        lo = o_ref[pl.ds(N2 * c2, N512, stride=N32), :].astype(BF16)
        hi = o_ref[pl.ds(N2 * c2 + N1, N512, stride=N32), :].astype(BF16)
        acc[ALL] += dot(jnp.concatenate([lo, hi], axis=N1), bd_ref[c2])
    loop(N16, mix)
    wait_bytes(zin.at[pl.ds(N0, N7)], zsem.at[N1])

    def update(d):
        rows = pl.ds(pl.multiple_of(d * N64, N64), N64)
        for il in range(N4):
            cols = slice(il * N128, (il + N1) * N128)
            upd = acc[rows, cols] * recip_ref[d, :, il:il + N1]
            zs[d, :, cols] = (zin[d, :, cols].astype(F32) + upd).astype(BF16)
    loop(N8, update)

    def send_z(k):
        d = lax.rem(v + N1 + k, N8)
        send(zs.at[d], zout_ref.at[v], osem.at[N0], osem.at[N1], u * N8 + d)
    loop(N7, send_z)
    zout_ref[v] = zs[v]
    wait_bytes(zout_ref.at[pl.ds(N0, N7)], osem.at[N1])
    wait_bytes(mout_ref.at[pl.ds(N0, N127)], msem.at[N1])
    wait_bytes(r_ref.at[pl.ds(N0, N15)], csem.at[N0])
    wait_bytes(l_ref.at[pl.ds(N0, N7)], asem.at[N0])
    wait_bytes(zin.at[pl.ds(N0, N7)], zsem.at[N0])
    wait_bytes(zout_ref.at[pl.ds(N0, N7)], osem.at[N0])
    wait_bytes(mout_ref.at[pl.ds(N0, N127)], msem.at[N0])


def kernel_c(z_ref, rmask_ref, cmask_ref, wsb_t, w_s_in, w_s_out, web_t, w_e_in, w_e_in_t, w_e_out, zo_ref,
             x_ref, slab_f, slab, bias, biasf, xn_ref, kv_ref, q_ref, g_ref, gt_ref, rep_ref, hm_ref, rept_ref, hmt_ref,
             r_ref, sendf, sendb, ebf, eslab, ebias, ebiasf, recvb, xs, kx, vx, zf, zb,
             gsem, xsem, ssem, asem, esem, osem):
    me = my_index()
    core = lax.rem(me, N2)
    chip = me // N2
    half = me // N64
    slot = me - N64 * half
    barrier_all(me)
    send(z_ref, x_ref.at[pl.ds(N4 * core, N4)], xsem.at[N0], xsem.at[N1], me + N1 - N2 * core)
    for il in range(N4):
        slab_f[N0:N4, :] = dot_t(wsb_t[ALL], layer_norm(z_ref[il]))
        ebf[il * N4:(il + N1) * N4, :] = slab_f[N0:N4, :]
    slab[ALL] = ebf[N0:N16, :].astype(BF16)

    def send_slab(k):
        c = lax.rem(chip + N1 + k, N64)
        p = N2 * c + half

        @pl.when(p != me)
        def _():
            send(slab, bias.at[slot], ssem.at[N0], gsem.at[slot // N32], p)
    loop(N64, send_slab)

    @pl.when(core == half)
    def _():
        bias[slot] = slab[ALL]

    rep_ref[ALL] = head_rep(N128, N4)
    hm_ref[ALL] = head_mask(N512, N4, N128)
    r = lax.broadcasted_iota(jnp.int32, (N128, N512), N0)
    c = lax.broadcasted_iota(jnp.int32, (N128, N512), N1)
    rept_ref[ALL] = (c // N4 == r).astype(F32).astype(BF16)
    hmt_ref[ALL] = (lax.rem(c, N4) == r // N32).astype(F32)

    def project(i):
        xn_ref[ALL] = layer_norm(x_ref[i])
        xn = xn_ref[ALL]
        kv_ref[i, :, N0:N128] = (dot(xn, w_s_in[:, N128:N256]) * cmask_ref[ALL]).astype(BF16)
        kv_ref[i, :, N128:N256] = dot(xn, w_s_in[:, N256:N384]).astype(BF16)
        xh = xn_ref[pl.ds(pl.multiple_of(core * N256, N256), N256), :]
        q_ref[i] = dot(xh, w_s_in[:, N0:N128]).astype(BF16)
        g_ref[i] = dot(xh, w_s_in[:, N384:N512]).astype(BF16)

    def own(i):
        x_ref[N4 * core + i] = z_ref[i]
        project(N4 * core + i)
    loop(N4, own)
    wait_bytes(z_ref, xsem.at[N1])
    loop(N4, lambda i: project(N4 - N4 * core + i))

    def attend(b, i):
        rows = pl.ds(pl.multiple_of(b * N128, N128), N128)
        qx = (dot(rep_ref[ALL], q_ref[i, rows, :]) * hm_ref[ALL]).astype(BF16)
        t = dot_t(qx, kv_ref[i, :, N0:N128]) * SCALE + biasf[ALL]
        r_ref[N0] = dot(softmax_rows(t), kv_ref[i, :, N128:N256])
        gt_ref[i, rows, :] = gate(collapse(r_ref, N128, N4), g_ref[i, rows, :])

    def block(b):
        @pl.when(jnp.logical_and(core == half, b == slot // N32))
        def _():
            wait_bytes(bias.at[pl.ds(N0, 31)], gsem.at[b])

        @pl.when(jnp.logical_not(jnp.logical_and(core == half, b == slot // N32)))
        def _():
            wait_bytes(bias.at[pl.ds(N0, N32)], gsem.at[b])
        got = bias[pl.ds(b * N32, N32)].reshape(N512, N512).astype(F32)
        biasf[ALL] = jnp.where(rmask_ref[ALL] > N0, got, -1e9)
        loop(N8, lambda i: attend(b, i))
    loop(N2, block)

    for i in range(N8):
        rows = pl.ds(pl.multiple_of(core * N256, N256), N256)
        y = (x_ref[i, rows, :].astype(F32) + dot(gt_ref[i], w_s_out[ALL])).astype(BF16)
        sendf[:, i] = y.astype(F32).reshape(N32, N8, N128)
        slab_f[N0:N4, N0:N256] = dot_t(web_t[ALL], layer_norm(y))
        ebf[i * N4:(i + N1) * N4, N0:N256] = slab_f[N0:N4, N0:N256]
    eslab[ALL] = ebf[:, N0:N256].astype(BF16)
    sendb[ALL] = sendf[ALL].astype(BF16).reshape(N32, N64, N128)

    def send_cols(k0):
        k = lax.rem(chip + N1 + k0, N32)
        for e in range(N2):
            q = N64 * core + N2 * k + e

            @pl.when(q != me)
            def _(q=q):
                send(sendb.at[k], recvb.at[chip], asem.at[N0], asem.at[N1], q)
    loop(N32, send_cols)

    def send_bias(k0):
        k = lax.rem(chip + N1 + k0, N64)
        send(eslab, ebias.at[chip], esem.at[N0], esem.at[N1], N2 * k + core)
    loop(N63, send_bias)
    ebias[chip] = eslab[ALL]

    @pl.when(core == half)
    def _():
        recvb[chip] = sendb[chip - N32 * core]
        wait_bytes(recvb.at[pl.ds(N0, N63)], asem.at[N1])

    @pl.when(core != half)
    def _():
        wait_bytes(recvb, asem.at[N1])
    xs[ALL] = recvb[ALL].astype(F32).reshape(N4096, N128)
    wait_bytes(ebias.at[pl.ds(N0, N63)], esem.at[N1])

    def widen(b):
        rows = pl.ds(pl.multiple_of(b * N512, N512), N512)
        keep = dot(rep_ref[ALL], cmask_ref[pl.ds(pl.multiple_of(b * N128, N128), N128), :].astype(BF16))
        got = ebias[pl.ds(b * N16, N16)].reshape(N512, N256).astype(F32)
        ebiasf[rows, N0:N128] = jnp.where(keep > N0, got[:, N0:N128], -1e9)
        ebiasf[rows, N128:N256] = jnp.where(keep > N0, got[:, N128:N256], -1e9)
    loop(N4, widen)

    def column(j):
        x = xs[pl.ds(j, N512, stride=N8), :]
        xn_ref[ALL] = layer_norm(x)
        xn = xn_ref[ALL]
        kv_ref[N0, :, N0:N128] = (dot(xn, w_e_in[:, N128:N256]) * cmask_ref[ALL]).astype(BF16)
        vt = dot_t(w_e_in_t[N256:N384, :], xn).astype(BF16)
        xh = xn_ref[pl.ds(pl.multiple_of(core * N256, N256), N256), :]
        q = dot(xh, w_e_in[:, N0:N128]).astype(BF16)
        gt = dot_t(w_e_in_t[N384:N512, :], xh).astype(BF16)
        for b in range(N4):
            kx[b * N512:(b + N1) * N512, :] = (dot(rep_ref[ALL], kv_ref[N0, b * N128:(b + N1) * N128, N0:N128]) * hm_ref[ALL]).astype(BF16)
            vx[:, b * N512:(b + N1) * N512] = (dot(vt[:, b * N128:(b + N1) * N128], rept_ref[ALL]) * hmt_ref[ALL]).astype(BF16)
        t = (dot_t(kx[ALL], q) * SCALE + ebiasf[ALL]).reshape(N256, N8, N256)
        top = jnp.max(t, axis=N0)
        top = jnp.maximum(top, pltpu.roll(top, N4, N0))
        e = jnp.exp(t - top[None])
        total = jnp.sum(e, axis=N0)
        total = total + pltpu.roll(total, N4, N0)
        p = (e * (1.0 / total)[None]).astype(BF16).reshape(N2048, N256)
        gated = gate(dot(vx[ALL], p), gt)
        y = lax.dot_general(gated, w_e_out[ALL], (((N0,), (N0,)), ((), ())), preferred_element_type=F32)
        res = xs[pl.ds(core * N2048 + j, N256, stride=N8), :]
        zf[pl.ds(j, N256, stride=N8), :] = res + y
    loop(N8, column)
    zb[ALL] = zf[ALL].astype(BF16).reshape(N64, N32, N128)

    def send_back(k0):
        k = lax.rem(slot + N1 + k0, N64)
        q = N64 * core + k

        @pl.when(q != me)
        def _():
            send(zb.at[k], zo_ref.at[chip], osem.at[N0], osem.at[N1], q)
    loop(N64, send_back)

    @pl.when(core == half)
    def _():
        zo_ref[chip] = zb[slot]
        wait_bytes(zo_ref.at[pl.ds(N0, N63)], osem.at[N1])
        wait_bytes(zo_ref.at[pl.ds(N0, N63)], osem.at[N0])
        wait_bytes(bias.at[pl.ds(N0, N63)], ssem.at[N0])
        wait_bytes(recvb.at[pl.ds(N0, N63)], asem.at[N0])

    @pl.when(core != half)
    def _():
        wait_bytes(zo_ref, osem.at[N1])
        wait_bytes(zo_ref, osem.at[N0])
        wait_bytes(bias, ssem.at[N0])
        wait_bytes(recvb, asem.at[N0])
    wait_bytes(z_ref, xsem.at[N0])
    wait_bytes(ebias.at[pl.ds(N0, N63)], esem.at[N0])


def shape(dims, dtype=BF16):
    return jax.ShapeDtypeStruct(dims, dtype)


def call(body, outs, scratch, cid, args):
    vm = pl.BlockSpec(memory_space=pltpu.VMEM)
    many = len(outs) > N1
    return pl.pallas_call(
        body, out_shape=tuple(outs) if many else outs[N0],
        in_specs=[vm] * len(args), out_specs=tuple([vm] * len(outs)) if many else vm, scratch_shapes=scratch,
        compiler_params=pltpu.CompilerParams(collective_id=cid, has_side_effects=True, vmem_limit_bytes=VMEM_LIMIT),
    )(*args)


def stage_a(m_blk, z_blk, msa_mask, me, w_row_in, w_row_bias, w_row_out, w_col_in, w_col_out, w_opm_in):
    rmask = lax.dynamic_slice_in_dim(msa_mask, (me // N2) * N4, N4, axis=N0).astype(F32)
    cols = lax.dynamic_slice_in_dim(msa_mask, me * N4, N4, axis=N1).astype(F32)
    w_left = jnp.stack([jnp.pad(w_opm_in[:, :N32], ((N0, N0), (N32 * jl, 96 - N32 * jl))) for jl in range(N4)])
    dma, V = pltpu.SemaphoreType.DMA, pltpu.VMEM
    scratch = [V((N4, N512, N256), BF16), V((N32, N512), F32), V((N32, N512), BF16), V((N64, N32, N512), BF16), V((N512, N256), BF16),
               V((N4, N512, N512), BF16), V((N4, N256, N256), BF16), V((N4, N256, N256), BF16), V((N4, N256, N256), BF16),
               V((N512, N64), BF16), V((N512, N256), F32), V((N2, N512, N128), F32), V((N2, N256, N128), F32), V((N2, N1024, N128), F32),
               V((N64, N16, N256), BF16), V((N64, N16, N256), BF16), V((N2, N1024, N128), F32), V((N256, N1024), BF16), V((N2, N1024, N128), F32),
               dma((N4,)), dma((N2,)), dma, dma((N2,)), dma((N2,))]
    return call(kernel_a, [shape((N128, N8, N256)), shape((N256, N128)), shape((N128, N256))], scratch, N0,
                [m_blk, z_blk, rmask, cols.T, jnp.repeat(cols, N32, axis=N1), w_row_bias.T, w_row_in, w_row_out, w_col_in,
                 w_col_out, w_left, w_opm_in[:, N32:].T])


def stage_b(left, right, z_blk, mcols, msa_mask, chip, dap, w_opm_out):
    mask = msa_mask.astype(BF16)
    mask_i = lax.dynamic_slice_in_dim(mask, chip * N32, N32, axis=N1)
    mask_j = lax.dynamic_slice_in_dim(mask.reshape(N256, N16, N8, N4), dap, N1, axis=N2).reshape(N256, N64)
    norm = lax.dot_general(mask_j, mask_i, (((N0,), (N0,)), ((), ())), preferred_element_type=F32)
    recip = (1.0 / (1e-3 + norm)).reshape(N64, N8, N4).transpose(N1, N0, N2)
    w_cmajor = w_opm_out.reshape(N32, N32, N128).transpose(N1, N0, N2).reshape(N1024, N128)
    z_split = z_blk.reshape(N4, N16, N8, N4, N128).transpose(N2, N1, N3, N0, N4).reshape(N8, N64, N512)
    dma, V = pltpu.SemaphoreType.DMA, pltpu.VMEM
    scratch = [V((N8, N256, N128), BF16), V((N16, N128, N256), BF16), V((N8, N64, N512), BF16), V((16384, N128), F32),
               V((N16, N256, N512), BF16), V((N512, N512), F32), V((N8, N64, N512), BF16)] + [dma((N2,))] * 5
    zout, mout = call(kernel_b, [shape((N8, N64, N512)), shape((N128, N8, N256))], scratch, N1,
                      [left, right, z_split, mcols, recip, w_cmajor])
    z_new = zout.reshape(N8, N16, N4, N4, N128).transpose(N3, N1, N0, N2, N4).reshape(N4, N512, N128)
    m_out = mout.reshape(N128, N2, N4, N256).transpose(N1, N0, N2, N3).reshape(N2, N512, N256)
    return z_new, m_out


def stage_c(z_blk, res_mask, w_start_in, w_start_bias, w_start_out, w_end_in, w_end_bias, w_end_out):
    keep = res_mask.astype(F32)
    dma, V = pltpu.SemaphoreType.DMA, pltpu.VMEM
    scratch = [V((N8, N512, N128), BF16), V((N8, N512), F32), V((N16, N512), BF16), V((N64, N16, N512), BF16), V((N512, N512), F32),
               V((N512, N128), BF16), V((N8, N512, N256), BF16), V((N8, N256, N128), BF16), V((N8, N256, N128), BF16),
               V((N8, N256, N128), BF16), V((N512, N128), BF16), V((N512, N128), F32), V((N128, N512), BF16), V((N128, N512), F32),
               V((N1, N512, N128), F32), V((N32, N8, N8, N128), F32), V((N32, N64, N128), BF16), V((N32, N512), F32), V((N32, N256), BF16),
               V((N64, N32, N256), BF16), V((N2048, N256), F32), V((N64, N64, N128), BF16), V((N4096, N128), F32), V((N2048, N128), BF16),
               V((N128, N2048), BF16), V((N2048, N128), F32), V((N64, N32, N128), BF16),
               dma((N2,)), dma((N2,)), dma((N1,)), dma((N2,)), dma((N2,)), dma((N2,))]
    zo = call(kernel_c, [shape((N64, N32, N128))], scratch, N2,
              [z_blk, keep[None, :], jnp.broadcast_to(keep[:, None], (N512, N128)), w_start_bias.T, w_start_in, w_start_out,
               w_end_bias.T, w_end_in, w_end_in.T, w_end_out])
    return zo.reshape(N64, N4, N8, N128).transpose(N1, N0, N2, N3).reshape(N4, N512, N128)


def solution(mesh):
    rows = P(('data', 'chip', 'dap'))
    in_specs = (rows, rows, P('data'), P('data')) + (P(),) * 13

    def per_device(m_blk, z_blk, msa_mask, res_mask, w_row_in, w_row_bias, w_row_out, w_col_in, w_col_out,
                   w_opm_in, w_opm_out, w_start_in, w_start_bias, w_start_out, w_end_in, w_end_bias, w_end_out):
        chip, dap = lax.axis_index('chip'), lax.axis_index('dap')
        mcols, left, right = stage_a(m_blk, z_blk, msa_mask, chip * N8 + dap, w_row_in, w_row_bias, w_row_out,
                                     w_col_in, w_col_out, w_opm_in)
        z_new, m_out = stage_b(left, right, z_blk, mcols, msa_mask, chip, dap, w_opm_out)
        z_out = stage_c(z_new, res_mask, w_start_in, w_start_bias, w_start_out, w_end_in, w_end_bias, w_end_out)
        return m_out, z_out

    return jax.shard_map(per_device, mesh=mesh, in_specs=in_specs, out_specs=(rows, rows), check_vma=False)
```

```python
import functools
from types import SimpleNamespace

import jax
import jax.numpy as jnp
from jax import lax
from jax.experimental import pallas as pl
from jax.experimental.pallas import tpu as pltpu
from jax.sharding import PartitionSpec as P

N0 = 0
N1 = 1
N2 = 2
N4 = 4
N7 = 7
N8 = 8
N15 = 15
N16 = 16
N32 = 32
N63 = 63
N64 = 64
N127 = 127
N128 = 128
N256 = 256
N384 = 384
N512 = 512
N768 = 768
N1024 = 1024
N2048 = 2048
N4096 = 4096
ALL = Ellipsis
MESH = pl.DeviceIdType.MESH
F32 = jnp.float32
BF16 = jnp.bfloat16
VMEM_LIMIT = 67043328


def layer_norm(x):
    values = x.astype(F32)
    centred = values - jnp.mean(values, axis=-N1, keepdims=True)
    variance = jnp.mean(centred * centred, axis=-N1, keepdims=True)
    return (centred * lax.rsqrt(variance + 1e-5)).astype(BF16)


def dot(a, b):
    return jnp.dot(a, b, preferred_element_type=F32)


def dot_t(a, b):
    return lax.dot_general(a, b, (((N1,), (N1,)), ((), ())), preferred_element_type=F32)


def dev(p):
    return (N0, p // N8, lax.rem(p, N8))


def my_index():
    return lax.axis_index('chip') * N8 + lax.axis_index('dap')


def loop(n, body):
    def step(i, carry):
        body(i)
        return carry
    lax.fori_loop(N0, n, step, N0)


def send(src, dst, send_sem, recv_sem, p):
    pltpu.make_async_remote_copy(src_ref=src, dst_ref=dst, send_sem=send_sem, recv_sem=recv_sem,
                                 device_id=dev(p), device_id_type=MESH).start()


def wait_bytes(ref, sem):
    pltpu.make_async_copy(ref, ref, sem).wait()


def head_rep(queries, heads):
    rows = queries * heads
    r = lax.broadcasted_iota(jnp.int32, (rows, queries), N0)
    c = lax.broadcasted_iota(jnp.int32, (rows, queries), N1)
    return (r // heads == c).astype(F32).astype(BF16)


def head_mask(rows, heads, width):
    r = lax.broadcasted_iota(jnp.int32, (rows, width), N0)
    c = lax.broadcasted_iota(jnp.int32, (rows, width), N1)
    return (lax.rem(r, heads) == c // N32).astype(F32)


def softmax_rows(t):
    e = jnp.exp(t - jnp.max(t, axis=N1, keepdims=True))
    return (e * (1.0 / jnp.sum(e, axis=N1, keepdims=True))).astype(BF16)


def put(ref, value):
    for t in range(ref.shape[N0]):
        ref[t] = value[:, t * N128:(t + N1) * N128]


def take(ref, start, size, stride):
    return jnp.concatenate([ref[t, pl.ds(start, size, stride=stride), :] for t in range(ref.shape[N0])], axis=N1)


def join(ref):
    return jnp.concatenate([ref[t] for t in range(ref.shape[N0])], axis=N1)


def spread(ref, start, size, stride, value):
    for t in range(ref.shape[N0]):
        ref[t, pl.ds(start, size, stride=stride), :] = value[:, t * N128:(t + N1) * N128]


def collapse(r_ref, queries, heads):
    lane = lax.broadcasted_iota(jnp.int32, (queries, N128), N1) // N32
    parts = []
    for t in range(r_ref.shape[N0]):
        out = r_ref[t, pl.ds(N4 * t, queries, stride=heads), :]
        for h in range(N1, N4):
            out = jnp.where(lane == h, r_ref[t, pl.ds(N4 * t + h, queries, stride=heads), :], out)
        parts.append(out)
    return jnp.concatenate(parts, axis=N1) if len(parts) > N1 else parts[N0]


def gate(o, g):
    return (o * jax.nn.sigmoid(g.astype(F32))).astype(BF16)


SCALE = N32 ** -0.5


def dot_c(a, b, da, db):
    return lax.dot_general(a, b, (((da,), (db,)), ((), ())), preferred_element_type=F32)


def iota(rows, cols, dim):
    return lax.broadcasted_iota(jnp.int32, (rows, cols), dim)


def one_hot(cond):
    return cond.astype(F32).astype(BF16)


def ready(cond, ref, few, many, sem):
    @pl.when(cond)
    def _():
        wait_bytes(ref.at[pl.ds(N0, few)], sem)

    @pl.when(jnp.logical_not(cond))
    def _():
        wait_bytes(ref.at[pl.ds(N0, many)], sem)


def kernel(scratch_names, m_ref, z_ref, mask_ref, keep_ref, w_row_in, w_row_bias, w_row_out, w_col_in, w_col_out,
           w_opm_in, w_opm_out, w_s_in, w_s_bias, w_s_out, w_e_in, w_e_bias, w_e_out, m_out, z_out, *scratch):
    r = SimpleNamespace(**dict(zip(scratch_names, scratch)))
    me = my_index()
    core, chip, half = lax.rem(me, N2), me // N2, me // N64
    u, v = me // N8, lax.rem(me, N8)
    slot = me - N64 * half
    mine = core == half
    hrows = pl.ds(pl.multiple_of(core * N256, N256), N256)
    bar = pltpu.get_barrier_semaphore()
    loop(N127, lambda k: pl.semaphore_signal(bar, inc=N1, device_id=dev(lax.rem(me + N1 + k, N128)), device_id_type=MESH))

    for il in range(N4):
        r.slab_f[il * N8:(il + N1) * N8, :] = dot_c(w_row_bias[ALL], layer_norm(z_ref[il]), N0, N1)
    r.slab_a[ALL] = r.slab_f[ALL].astype(BF16)
    pl.semaphore_wait(bar, N127)
    send(m_ref, r.xm.at[pl.ds(N2 * core, N2)], r.xsem.at[N0], r.xsem.at[N1], me + N1 - N2 * core)

    def send_slab_a(k):
        p = N2 * lax.rem(chip + N1 + k, N64) + half

        @pl.when(p != me)
        def _():
            send(r.slab_a, r.bias_a.at[slot], r.sa, r.ga.at[slot // N16], p)
    loop(N64, send_slab_a)

    @pl.when(mine)
    def _():
        r.bias_a[slot] = r.slab_a[ALL]

    r.rep8[ALL] = head_rep(N64, N8)
    r.hm8[ALL] = head_mask(N512, N8, N256)
    maskb = mask_ref[ALL].astype(F32).astype(BF16)
    r.rmask[ALL] = dot(one_hot(iota(N4, N256, N1) == N4 * chip + iota(N4, N256, N0)), maskb)
    r.cmask[ALL] = dot_c(one_hot(iota(N4, N512, N1) == N4 * me + iota(N4, N512, N0)), maskb, N1, N1)
    r.cmexp[ALL] = dot(maskb, one_hot(iota(N512, N128, N0) == N4 * me + iota(N512, N128, N1) // N32))
    lane = iota(N512, N64, N1)
    mask_j = dot(maskb, one_hot(iota(N512, N64, N0) == N32 * lax.rem(lane, N16) + N4 * v + lane // N16)).astype(BF16)
    mask_i = dot(maskb, one_hot(iota(N512, N32, N0) == N32 * u + iota(N512, N32, N1))).astype(BF16)
    r.recip[ALL] = 1.0 / (1e-3 + dot_c(mask_j, mask_i, N0, N0))

    def project_m(s):
        r.xn_m[ALL] = layer_norm(r.xm[s])
        r.kv_m[s] = dot(r.xn_m[ALL], w_row_in[:, N256:N768]).astype(BF16)
        xh = r.xn_m[hrows, :]
        r.q_m[s] = dot(xh, w_row_in[:, N0:N256]).astype(BF16)
        r.g_m[s] = dot(xh, w_row_in[:, N768:N1024]).astype(BF16)

    def own_m(s):
        r.xm[N2 * core + s] = m_ref[s]
        project_m(N2 * core + s)
    loop(N2, own_m)
    wait_bytes(m_ref, r.xsem.at[N1])
    loop(N2, lambda s: project_m(N2 - N2 * core + s))

    for il in range(N4):
        r.zf[il] = z_ref[il].astype(F32)

    def split_z(d):
        for il in range(N4):
            for jl in range(N4):
                r.zsplit[d, jl * N16:(jl + N1) * N16, il * N128:(il + N1) * N128] = r.zf[il, pl.ds(d * N4 + jl, N16, stride=N32), :].astype(BF16)
    loop(N8, split_z)

    def send_z_in(k):
        d = lax.rem(v + N1 + k, N8)
        send(r.zsplit.at[d], r.zin.at[v], r.zsem.at[N0], r.zsem.at[N1], u * N8 + d)
    loop(N7, send_z_in)
    r.zin[v] = r.zsplit[v]

    def attend_m(b, s):
        rows = pl.ds(pl.multiple_of(b * N64, N64), N64)
        qx = (dot(r.rep8[ALL], r.q_m[s, rows, :]) * r.hm8[ALL]).astype(BF16)
        t = dot_t(qx, r.kv_m[s, :, N0:N256]) * SCALE + r.bias_a[pl.ds(b * N16, N16)].reshape(N512, N512).astype(F32)
        t = jnp.where(r.rmask[pl.ds(s, N1), :] > N0, t, -1e9)
        put(r.pv, dot(softmax_rows(t), r.kv_m[s, :, N256:N512]))
        r.gt_m[s, rows, :] = gate(collapse(r.pv, N64, N8), r.g_m[s, rows, :])

    def block_m(b):
        ready(jnp.logical_and(mine, b == slot // N16), r.bias_a, N15, N16, r.ga.at[b])
        loop(N4, lambda s: attend_m(b, s))
    loop(N4, block_m)

    def finish_m(s):
        put(r.y_m, r.xm[s, hrows, :].astype(F32) + dot(r.gt_m[s], w_row_out[ALL]))
        for jl in range(N4):
            spread(r.f_m, s * N4 + jl, N64, N16, take(r.y_m, jl, N64, N4))
    loop(N4, finish_m)
    r.send_m[ALL] = join(r.f_m).astype(BF16).reshape(N64, N16, N256)

    def send_cols_m(k0):
        k = lax.rem(slot + N1 + k0, N64)
        q = N64 * core + k

        @pl.when(q != me)
        def _():
            send(r.send_m.at[k], r.recv_m.at[chip], r.am.at[N0], r.am.at[N1], q)
    loop(N64, send_cols_m)

    @pl.when(mine)
    def _():
        r.recv_m[chip] = r.send_m[slot]

    r.bd[ALL] = jnp.zeros_like(r.bd)
    r.wf[ALL] = w_opm_out[ALL].astype(F32)

    def build(c2):
        for e in range(N2):
            w = r.wf[pl.ds(N2 * c2 + e, N32, stride=N32), :].astype(BF16)
            for il in range(N4):
                r.bd[c2, e * N128 + il * N32:e * N128 + (il + N1) * N32, il * N128:(il + N1) * N128] = w
    loop(N16, build)
    r.rep4[ALL] = head_rep(N128, N4)
    r.hm4[ALL] = head_mask(N512, N4, N128)
    r.rept[ALL] = one_hot(iota(N128, N512, N1) // N4 == iota(N128, N512, N0))
    r.hmt[ALL] = (lax.rem(iota(N128, N512, N1), N4) == iota(N128, N512, N0) // N32).astype(F32)
    for e in range(N2):
        r.wet[e] = jnp.transpose(w_e_in[:, N256 + e * N128:N384 + e * N128].astype(F32)).astype(BF16)
    keep = jnp.where(iota(N8, N512, N0) == N0, keep_ref[ALL].astype(F32), 0.0).astype(BF16)
    r.keepc[ALL] = dot_c(keep, one_hot(iota(N8, N128, N0) < N8), N0, N0)
    r.keepr[ALL] = keep_ref[ALL].astype(F32)
    ready(mine, r.recv_m, N63, N64, r.am.at[N1])
    put(r.xs_m, r.recv_m[ALL].astype(F32).reshape(N1024, N256))

    for jl in range(N4):
        x = take(r.xs_m, jl, N256, N4)
        r.qkvg[ALL] = dot(layer_norm(x), w_col_in[ALL]).astype(BF16)

        def col_block(b, jl=jl):
            rows = pl.ds(pl.multiple_of(b * N64, N64), N64)
            qx = (dot(r.rep8[ALL], r.qkvg[rows, N0:N256]) * r.hm8[ALL]).astype(BF16)
            t = dot_t(qx, r.qkvg[:, N256:N512]) * SCALE
            t = jnp.where(r.cmask[jl:jl + N1, :] > N0, t, -1e9)
            put(r.pv, dot(softmax_rows(t), r.qkvg[:, N512:N768]))
            r.gt_m[N0, rows, :] = gate(collapse(r.pv, N64, N8), r.qkvg[rows, N768:N1024])
        loop(N4, col_block)
        y = (x + dot(r.gt_m[N0], w_col_out[ALL])).astype(BF16)
        spread(r.yf_m, jl, N256, N4, y.astype(F32))
        ab = dot(layer_norm(y), w_opm_in[ALL]).astype(BF16)
        right = dot_c(one_hot(iota(N32, N64, N1) == iota(N32, N64, N0) + N32), ab, N1, N1) * r.cmask[jl:jl + N1, :]
        r.right[jl * N32:(jl + N1) * N32, :] = right.astype(BF16)
        part = dot(ab, one_hot(iota(N64, N128, N1) == iota(N64, N128, N0) + N32 * jl) * one_hot(iota(N64, N128, N0) < N32))
        r.y_m[N0] = part if jl == N0 else r.y_m[N0] + part
    r.left[ALL] = (r.y_m[N0] * r.cmexp[ALL]).astype(BF16)

    def send_c(k):
        send(r.right, r.rall.at[u], r.csem.at[N0], r.csem.at[N1], lax.rem(u + N1 + k, N16) * N8 + v)
    loop(N15, send_c)

    def send_a(k):
        d = lax.rem(v + N1 + k, N8)
        send(r.left, r.lall.at[v], r.lsem.at[N0], r.lsem.at[N1], u * N8 + d)
    loop(N7, send_a)
    r.rall[u] = r.right[ALL]
    r.lall[v] = r.left[ALL]
    r.mcols[ALL] = join(r.yf_m).astype(BF16).reshape(N128, N8, N256)
    r.acc[ALL] = jnp.zeros_like(r.acc)
    wait_bytes(r.rall.at[pl.ds(N0, N15)], r.csem.at[N1])
    wait_bytes(r.lall.at[pl.ds(N0, N7)], r.lsem.at[N1])

    def outer(d):
        r.o[pl.ds(pl.multiple_of(d * N2048, N2048), N2048), :] = dot(r.rall[ALL].reshape(N2048, N256), r.lall[d])
    loop(N8, outer)

    def mix(c2):
        parts = []
        for e in range(N2):
            rows = [r.o[pl.ds(d * N2048 + jl * N32 + N2 * c2 + e, N16, stride=N128), :] for d in range(N8) for jl in range(N4)]
            parts.append(jnp.concatenate(rows, axis=N0).astype(BF16))
        r.acc[ALL] += dot(jnp.concatenate(parts, axis=N1), r.bd[c2])
    loop(N16, mix)
    wait_bytes(r.zin.at[pl.ds(N0, N7)], r.zsem.at[N1])
    for d in range(N8):
        for il in range(N4):
            cols = slice(il * N128, (il + N1) * N128)
            upd = r.acc[d * N64:(d + N1) * N64, cols] * r.recip[:, d * N4 + il:d * N4 + il + N1]
            r.zs[d, :, cols] = (r.zin[d, :, cols].astype(F32) + upd).astype(BF16)

    def send_z(k):
        d = lax.rem(v + N1 + k, N8)
        send(r.zs.at[d], r.zback.at[v], r.bsem.at[N0], r.bsem.at[N1], u * N8 + d)
    loop(N7, send_z)
    r.zback[v] = r.zs[v]
    wait_bytes(r.zback.at[pl.ds(N0, N7)], r.bsem.at[N1])

    def merge_z(d):
        for il in range(N4):
            for jl in range(N4):
                r.zf[il, pl.ds(d * N4 + jl, N16, stride=N32), :] = r.zback[d, jl * N16:(jl + N1) * N16, il * N128:(il + N1) * N128].astype(F32)
    loop(N8, merge_z)

    for il in range(N4):
        r.zb[il] = r.zf[il].astype(BF16)
        r.e_f[il * N4:(il + N1) * N4, :] = dot_c(w_s_bias[ALL], layer_norm(r.zb[il]), N0, N1)
    r.slab_s[ALL] = r.e_f[N0:N16, :].astype(BF16)
    send(r.zb, r.xz.at[pl.ds(N4 * core, N4)], r.ysem.at[N0], r.ysem.at[N1], me + N1 - N2 * core)

    def send_slab_s(k):
        p = N2 * lax.rem(chip + N1 + k, N64) + half

        @pl.when(p != me)
        def _():
            send(r.slab_s, r.bias_s.at[slot], r.ss, r.gs.at[slot // N32], p)
    loop(N64, send_slab_s)

    @pl.when(mine)
    def _():
        r.bias_s[slot] = r.slab_s[ALL]

    def send_m_out(k):
        p = lax.rem(me + N1 + k, N128)
        send(r.mcols.at[p], r.mback.at[me], r.msem.at[N0], r.msem.at[N1], p)
    loop(N127, send_m_out)
    r.mback[me] = r.mcols[me]

    def project_z(i):
        r.xn_z[ALL] = layer_norm(r.xz[i])
        xn = r.xn_z[ALL]
        r.kv_z[i, :, N0:N128] = (dot(xn, w_s_in[:, N128:N256]) * r.keepc[ALL]).astype(BF16)
        r.kv_z[i, :, N128:N256] = dot(xn, w_s_in[:, N256:N384]).astype(BF16)
        xh = r.xn_z[hrows, :]
        r.q_z[i] = dot(xh, w_s_in[:, N0:N128]).astype(BF16)
        r.g_z[i] = dot(xh, w_s_in[:, N384:N512]).astype(BF16)

    def own_z(i):
        r.xz[N4 * core + i] = r.zb[i]
        project_z(N4 * core + i)
    loop(N4, own_z)
    wait_bytes(r.zb, r.ysem.at[N1])
    loop(N4, lambda i: project_z(N4 - N4 * core + i))

    def attend_z(b, i):
        rows = pl.ds(pl.multiple_of(b * N128, N128), N128)
        qx = (dot(r.rep4[ALL], r.q_z[i, rows, :]) * r.hm4[ALL]).astype(BF16)
        t = dot_t(qx, r.kv_z[i, :, N0:N128]) * SCALE + r.biasf[ALL]
        r.pv[N0] = dot(softmax_rows(t), r.kv_z[i, :, N128:N256])
        r.gt_z[i, rows, :] = gate(collapse(r.pv.at[N0:N1], N128, N4), r.g_z[i, rows, :])

    def block_z(b):
        ready(jnp.logical_and(mine, b == slot // N32), r.bias_s, 31, N32, r.gs.at[b])
        got = r.bias_s[pl.ds(b * N32, N32)].reshape(N512, N512).astype(F32)
        r.biasf[ALL] = jnp.where(r.keepr[ALL] > N0, got, -1e9)
        loop(N8, lambda i: attend_z(b, i))
    loop(N2, block_z)

    for i in range(N8):
        y = (r.xz[i, hrows, :].astype(F32) + dot(r.gt_z[i], w_s_out[ALL])).astype(BF16)
        r.f_z[:, i] = y.astype(F32).reshape(N32, N8, N128)
        r.e_f[i * N4:(i + N1) * N4, N0:N256] = dot_c(w_e_bias[ALL], layer_norm(y), N0, N1)
    r.slab_e[ALL] = r.e_f[:, N0:N256].astype(BF16)
    r.send_zc[ALL] = r.f_z[ALL].astype(BF16).reshape(N32, N64, N128)

    def send_cols_z(k0):
        k = lax.rem(chip + N1 + k0, N32)
        for e in range(N2):
            q = N64 * core + N2 * k + e

            @pl.when(q != me)
            def _(q=q):
                send(r.send_zc.at[k], r.recv_zc.at[chip], r.az.at[N0], r.az.at[N1], q)
    loop(N32, send_cols_z)

    def send_slab_e(k0):
        send(r.slab_e, r.bias_e.at[chip], r.esem.at[N0], r.esem.at[N1], N2 * lax.rem(chip + N1 + k0, N64) + core)
    loop(N63, send_slab_e)
    r.bias_e[chip] = r.slab_e[ALL]

    @pl.when(mine)
    def _():
        r.recv_zc[chip] = r.send_zc[chip - N32 * core]

    wait_bytes(r.mback.at[pl.ds(N0, N127)], r.msem.at[N1])
    put(r.yf_m, r.mback[ALL].astype(F32).reshape(N1024, N256))
    for sl in range(N2):
        for jl in range(N4):
            spread(r.f_m, sl * N512 + jl, N128, N4, take(r.yf_m, sl * N4 + jl, N128, N8))
    m_out[ALL] = join(r.f_m).astype(BF16).reshape(N2, N512, N256)

    ready(mine, r.recv_zc, N63, N64, r.az.at[N1])
    r.xs_z[ALL] = r.recv_zc[ALL].astype(F32).reshape(N4096, N128)
    wait_bytes(r.bias_e.at[pl.ds(N0, N63)], r.esem.at[N1])

    def widen(b):
        rows = pl.ds(pl.multiple_of(b * N512, N512), N512)
        kept = dot(r.rep4[ALL], r.keepc[pl.ds(pl.multiple_of(b * N128, N128), N128), :].astype(BF16))
        got = r.bias_e[pl.ds(b * N16, N16)].reshape(N512, N256).astype(F32)
        for t in range(N2):
            r.biasf_e[rows, t * N128:(t + N1) * N128] = jnp.where(kept > N0, got[:, t * N128:(t + N1) * N128], -1e9)
    loop(N4, widen)

    def column(j):
        r.xn_z[ALL] = layer_norm(r.xs_z[pl.ds(j, N512, stride=N8), :])
        xn = r.xn_z[ALL]
        r.kv_z[N0, :, N0:N128] = (dot(xn, w_e_in[:, N128:N256]) * r.keepc[ALL]).astype(BF16)
        vt = dot_t(r.wet[N0], xn).astype(BF16)
        xh = r.xn_z[hrows, :]
        q = dot(xh, w_e_in[:, N0:N128]).astype(BF16)
        gt = dot_t(r.wet[N1], xh).astype(BF16)
        for b in range(N4):
            r.kx[b * N512:(b + N1) * N512, :] = (dot(r.rep4[ALL], r.kv_z[N0, b * N128:(b + N1) * N128, N0:N128]) * r.hm4[ALL]).astype(BF16)
            r.vx[:, b * N512:(b + N1) * N512] = (dot(vt[:, b * N128:(b + N1) * N128], r.rept[ALL]) * r.hmt[ALL]).astype(BF16)
        t = (dot_t(r.kx[ALL], q) * SCALE + r.biasf_e[ALL]).reshape(N256, N8, N256)
        top = jnp.max(t, axis=N0)
        top = jnp.maximum(top, pltpu.roll(top, N4, N0))
        e = jnp.exp(t - top[None])
        total = jnp.sum(e, axis=N0)
        total = total + pltpu.roll(total, N4, N0)
        p = (e * (1.0 / total)[None]).astype(BF16).reshape(N2048, N256)
        gated = gate(dot(r.vx[ALL], p), gt)
        y = dot_c(gated, w_e_out[ALL], N0, N0)
        r.y_z[pl.ds(j, N256, stride=N8), :] = r.xs_z[pl.ds(core * N2048 + j, N256, stride=N8), :] + y
    loop(N8, column)
    r.send_o[ALL] = r.y_z[ALL].astype(BF16).reshape(N64, N32, N128)

    def send_back(k0):
        k = lax.rem(slot + N1 + k0, N64)
        q = N64 * core + k

        @pl.when(q != me)
        def _():
            send(r.send_o.at[k], r.recv_o.at[chip], r.osem.at[N0], r.osem.at[N1], q)
    loop(N64, send_back)

    @pl.when(mine)
    def _():
        r.recv_o[chip] = r.send_o[slot]
    for ref, sem in ((r.bias_a, r.sa), (r.recv_m, r.am.at[N0]), (r.bias_s, r.ss), (r.recv_zc, r.az.at[N0])):
        ready(mine, ref, N63, N64, sem)
    wait_bytes(m_ref, r.xsem.at[N0])
    wait_bytes(r.zb, r.ysem.at[N0])
    wait_bytes(r.zin.at[pl.ds(N0, N7)], r.zsem.at[N0])
    wait_bytes(r.rall.at[pl.ds(N0, N15)], r.csem.at[N0])
    wait_bytes(r.lall.at[pl.ds(N0, N7)], r.lsem.at[N0])
    wait_bytes(r.zback.at[pl.ds(N0, N7)], r.bsem.at[N0])
    wait_bytes(r.mback.at[pl.ds(N0, N127)], r.msem.at[N0])
    wait_bytes(r.bias_e.at[pl.ds(N0, N63)], r.esem.at[N0])
    ready(mine, r.recv_o, N63, N64, r.osem.at[N1])
    got = r.recv_o[ALL].astype(F32).reshape(N64, N4, N8, N128)
    for il in range(N4):
        z_out[il] = got[:, il].reshape(N512, N128).astype(BF16)
    ready(mine, r.recv_o, N63, N64, r.osem.at[N0])


BUFFERS = dict(
    slab_a=(N32, N512), bias_a=(N64, N32, N512), xm=(N4, N512, N256), xn_m=(N512, N256), kv_m=(N4, N512, N512), q_m=(N4, N256, N256),
    g_m=(N4, N256, N256), gt_m=(N4, N256, N256), rep8=(N512, N64), zsplit=(N8, N64, N512), zin=(N8, N64, N512), send_m=(N64, N16, N256),
    recv_m=(N64, N16, N256), qkvg=(N256, N1024), left=(N256, N128), right=(N128, N256), lall=(N8, N256, N128), rall=(N16, N128, N256),
    mcols=(N128, N8, N256), mback=(N128, N8, N256), bd=(N16, N256, N512), zs=(N8, N64, N512), zback=(N8, N64, N512), zb=(N4, N512, N128),
    xz=(N8, N512, N128), slab_s=(N16, N512), bias_s=(N64, N16, N512), xn_z=(N512, N128), kv_z=(N8, N512, N256), q_z=(N8, N256, N128),
    g_z=(N8, N256, N128), gt_z=(N8, N256, N128), rep4=(N512, N128), rept=(N128, N512), wet=(N2, N128, N128), slab_e=(N32, N256),
    bias_e=(N64, N32, N256), send_zc=(N32, N64, N128), recv_zc=(N64, N64, N128), kx=(N2048, N128), vx=(N128, N2048),
    send_o=(N64, N32, N128), recv_o=(N64, N32, N128))
FLOATS = dict(
    slab_f=(N32, N512), rmask=(N4, N512), cmask=(N4, N256), cmexp=(N256, N128), recip=(N64, N32), hm8=(N512, N256), hm4=(N512, N128),
    hmt=(N128, N512), keepc=(N512, N128), keepr=(N1, N512), zf=(N4, N512, N128), pv=(N2, N512, N128), y_m=(N2, N256, N128),
    f_m=(N2, N1024, N128), xs_m=(N2, N1024, N128), yf_m=(N2, N1024, N128), wf=(N1024, N128), o=(16384, N128), acc=(N512, N512),
    e_f=(N32, N512), biasf=(N512, N512), f_z=(N32, N8, N8, N128), biasf_e=(N2048, N256), xs_z=(N4096, N128), y_z=(N2048, N128))
SEMS = dict(ga=N4, gs=N2, xsem=N2, ysem=N2, zsem=N2, am=N2, csem=N2, lsem=N2, bsem=N2, msem=N2, az=N2, esem=N2, osem=N2, sa=None, ss=None)


def solution(mesh):
    rows = P(('data', 'chip', 'dap'))
    in_specs = (rows, rows, P('data'), P('data')) + (P(),) * 13
    specs = {name: pltpu.VMEM(dims, BF16) for name, dims in BUFFERS.items()}
    specs.update({name: pltpu.VMEM(dims, F32) for name, dims in FLOATS.items()})
    specs.update({name: pltpu.SemaphoreType.DMA if n is None else pltpu.SemaphoreType.DMA((n,)) for name, n in SEMS.items()})

    def per_device(m_blk, z_blk, msa_mask, res_mask, *weights):
        args = (m_blk, z_blk, msa_mask, res_mask.reshape(N1, N512)) + weights
        vm = pl.BlockSpec(memory_space=pltpu.VMEM)
        return pl.pallas_call(
            functools.partial(kernel, tuple(specs)),
            out_shape=(jax.ShapeDtypeStruct(m_blk.shape, BF16), jax.ShapeDtypeStruct(z_blk.shape, BF16)),
            in_specs=[vm] * len(args), out_specs=(vm, vm), scratch_shapes=list(specs.values()),
            compiler_params=pltpu.CompilerParams(collective_id=N0, has_side_effects=True, vmem_limit_bytes=VMEM_LIMIT),
        )(*args)

    return jax.shard_map(per_device, mesh=mesh, in_specs=in_specs, out_specs=(rows, rows), check_vma=False)
```

```python
import functools
from types import SimpleNamespace

import jax
import jax.numpy as jnp
from jax import lax
from jax.experimental import pallas as pl
from jax.experimental.pallas import tpu as pltpu
from jax.sharding import PartitionSpec as P

N0 = 0
N1 = 1
N2 = 2
N3 = 3
N4 = 4
N7 = 7
N8 = 8
N15 = 15
N16 = 16
N32 = 32
N63 = 63
N64 = 64
N127 = 127
N128 = 128
N256 = 256
N384 = 384
N512 = 512
N768 = 768
N1024 = 1024
N2048 = 2048
N4096 = 4096
ALL = Ellipsis
MESH = pl.DeviceIdType.MESH
F32 = jnp.float32
BF16 = jnp.bfloat16
VMEM_LIMIT = 67043328
UNROLL_A, UNROLL_B, UNROLL_C, UNROLL_D = N2, N1, N2, N1


def layer_norm(x):
    values = x.astype(F32)
    centred = values - jnp.mean(values, axis=-N1, keepdims=True)
    variance = jnp.mean(centred * centred, axis=-N1, keepdims=True)
    return (centred * lax.rsqrt(variance + 1e-5)).astype(BF16)


def dot(a, b):
    return jnp.dot(a, b, preferred_element_type=F32)


def dot_t(a, b):
    return lax.dot_general(a, b, (((N1,), (N1,)), ((), ())), preferred_element_type=F32)


def dev(p):
    return (N0, p // N8, lax.rem(p, N8))


def my_index():
    return lax.axis_index('chip') * N8 + lax.axis_index('dap')


def loop(n, body, unroll=N1):
    def step(i, carry):
        body(i)
        return carry
    lax.fori_loop(N0, n, step, N0, unroll=unroll)


def send(src, dst, send_sem, recv_sem, p):
    pltpu.make_async_remote_copy(src_ref=src, dst_ref=dst, send_sem=send_sem, recv_sem=recv_sem,
                                 device_id=dev(p), device_id_type=MESH).start()


def wait_bytes(ref, sem):
    pltpu.make_async_copy(ref, ref, sem).wait()


def head_rep(queries, heads):
    rows = queries * heads
    r = lax.broadcasted_iota(jnp.int32, (rows, queries), N0)
    c = lax.broadcasted_iota(jnp.int32, (rows, queries), N1)
    return (r // heads == c).astype(F32).astype(BF16)


def head_mask(rows, heads, width):
    r = lax.broadcasted_iota(jnp.int32, (rows, width), N0)
    c = lax.broadcasted_iota(jnp.int32, (rows, width), N1)
    return (lax.rem(r, heads) == c // N32).astype(F32)


def softmax_rows(t):
    e = jnp.exp2(t - jnp.max(t, axis=N1, keepdims=True))
    return (e * (1.0 / jnp.sum(e, axis=N1, keepdims=True))).astype(BF16)


def put(ref, value):
    for t in range(ref.shape[N0]):
        ref[t] = value[:, t * N128:(t + N1) * N128]


def take(ref, start, size, stride):
    return jnp.concatenate([ref[t, pl.ds(start, size, stride=stride), :] for t in range(ref.shape[N0])], axis=N1)


def join(ref):
    return jnp.concatenate([ref[t] for t in range(ref.shape[N0])], axis=N1)


def spread(ref, start, size, stride, value):
    for t in range(ref.shape[N0]):
        ref[t, pl.ds(start, size, stride=stride), :] = value[:, t * N128:(t + N1) * N128]


def collapse(r_ref, queries, heads):
    lane = lax.broadcasted_iota(jnp.int32, (queries, N128), N1) // N32
    parts = []
    for t in range(r_ref.shape[N0]):
        out = r_ref[t, pl.ds(N4 * t, queries, stride=heads), :]
        for h in range(N1, N4):
            out = jnp.where(lane == h, r_ref[t, pl.ds(N4 * t + h, queries, stride=heads), :], out)
        parts.append(out)
    return jnp.concatenate(parts, axis=N1) if len(parts) > N1 else parts[N0]


def gate(o, g):
    return (o * jax.nn.sigmoid(g.astype(F32))).astype(BF16)


LOG2E = 1.4426950408889634
SCALE = N32 ** -0.5 * LOG2E
LOW = -1e9 * LOG2E


def dot_c(a, b, da, db):
    return lax.dot_general(a, b, (((da,), (db,)), ((), ())), preferred_element_type=F32)


def iota(rows, cols, dim):
    return lax.broadcasted_iota(jnp.int32, (rows, cols), dim)


def one_hot(cond):
    return cond.astype(F32).astype(BF16)


def ready(cond, ref, few, many, sem):
    @pl.when(cond)
    def _():
        wait_bytes(ref.at[pl.ds(N0, few)], sem)

    @pl.when(jnp.logical_not(cond))
    def _():
        wait_bytes(ref.at[pl.ds(N0, many)], sem)


def kernel(scratch_names, m_ref, z_ref, mask_ref, keep_ref, w_row_in, w_row_bias, w_row_out, w_col_in, w_col_out,
           w_opm_in, w_opm_out, w_s_in, w_s_bias, w_s_out, w_e_in, w_e_bias, w_e_out, m_out, z_out, *scratch):
    r = SimpleNamespace(**dict(zip(scratch_names, scratch)))
    me = my_index()
    core, chip, half = lax.rem(me, N2), me // N2, me // N64
    u, v = me // N8, lax.rem(me, N8)
    slot = me - N64 * half
    mine = core == half
    hrows = pl.ds(pl.multiple_of(core * N256, N256), N256)
    bar = pltpu.get_barrier_semaphore()
    loop(N127, lambda k: pl.semaphore_signal(bar, inc=N1, device_id=dev(lax.rem(me + N1 + k, N128)), device_id_type=MESH))

    for il in range(N4):
        r.slab_f[il * N8:(il + N1) * N8, :] = dot_t(w_row_bias[ALL], layer_norm(z_ref[il]))
    r.slab_a[ALL] = r.slab_f[ALL].astype(BF16)
    pl.semaphore_wait(bar, N127)
    send(m_ref, r.xm.at[pl.ds(N2 * core, N2)], r.xsem.at[N0], r.xsem.at[N1], me + N1 - N2 * core)

    def send_slab_a(k):
        p = N2 * lax.rem(chip + N1 + k, N64) + half

        @pl.when(p != me)
        def _():
            send(r.slab_a, r.bias_a.at[slot], r.sa, r.ga.at[slot // N16], p)
    loop(N64, send_slab_a)

    @pl.when(mine)
    def _():
        r.bias_a[slot] = r.slab_a[ALL]

    r.rep8[ALL] = head_rep(N64, N8)
    r.hm8[ALL] = head_mask(N512, N8, N256)
    maskb = mask_ref[ALL].astype(F32).astype(BF16)
    r.rmask[ALL] = dot(one_hot(iota(N4, N256, N1) == N4 * chip + iota(N4, N256, N0)), maskb)
    r.cmask[ALL] = dot_c(one_hot(iota(N4, N512, N1) == N4 * me + iota(N4, N512, N0)), maskb, N1, N1)
    lane = iota(N512, N64, N1)
    mask_j = dot(maskb, one_hot(iota(N512, N64, N0) == N32 * lax.rem(lane, N16) + N4 * v + lane // N16)).astype(BF16)
    mask_i = dot(maskb, one_hot(iota(N512, N32, N0) == N32 * u + iota(N512, N32, N1))).astype(BF16)
    r.recip[ALL] = 1.0 / (1e-3 + dot_c(mask_j, mask_i, N0, N0))

    def project_m(s):
        r.xn_m[ALL] = layer_norm(r.xm[s])
        r.kv_m[s] = dot(r.xn_m[ALL], w_row_in[:, N256:N768]).astype(BF16)
        xh = r.xn_m[hrows, :]
        r.q_m[s] = dot(xh, w_row_in[:, N0:N256]).astype(BF16)
        r.g_m[s] = dot(xh, w_row_in[:, N768:N1024]).astype(BF16)

    def own_m(s):
        r.xm[N2 * core + s] = m_ref[s]
        project_m(N2 * core + s)
    loop(N2, own_m)
    wait_bytes(m_ref, r.xsem.at[N1])
    loop(N2, lambda s: project_m(N2 - N2 * core + s))

    def attend_m(b, s):
        rows = pl.ds(pl.multiple_of(b * N64, N64), N64)
        qx = (dot(r.rep8[ALL], r.q_m[s, rows, :]) * r.hm8[ALL]).astype(BF16)
        t = dot_t(qx, r.kv_m[s, :, N0:N256]) * SCALE + r.biasf[ALL]
        t = jnp.where(r.rmask[pl.ds(s, N1), :] > N0, t, LOW)
        put(r.pv, dot(softmax_rows(t), r.kv_m[s, :, N256:N512]))
        r.gt_m[s, rows, :] = gate(collapse(r.pv, N64, N8), r.g_m[s, rows, :])

    def finish_m(b, s):
        rows = pl.ds(pl.multiple_of(b * N64, N64), N64)
        put(r.y_m, r.xm[s, pl.ds(pl.multiple_of(core * N256 + b * N64, N64), N64), :].astype(F32) + dot(r.gt_m[s, rows, :], w_row_out[ALL]))
        for jl in range(N4):
            spread(r.f_b, s * N4 + jl, N16, N16, take(r.y_m, jl, N16, N4))

    def block_m(step):
        b = lax.rem(jnp.where(chip // N32 == core, (chip - N32 * core) // N8, N0) + N3 - step, N4)
        ready(jnp.logical_and(mine, b == slot // N16), r.bias_a, N15, N16, r.ga.at[b])
        r.biasf[ALL] = r.bias_a[pl.ds(b * N16, N16)].reshape(N512, N512).astype(F32) * LOG2E
        loop(N4, lambda s: attend_m(b, s), UNROLL_A)
        loop(N4, lambda s: finish_m(b, s))
        r.send_m[pl.ds(b * N16, N16)] = join(r.f_b).astype(BF16).reshape(N16, N16, N256)

        def send_cols_m(k0):
            k = b * N16 + lax.rem(slot + N1 + k0, N16)
            q = N64 * core + k

            @pl.when(q != me)
            def _():
                send(r.send_m.at[k], r.recv_m.at[chip], r.am.at[N0], r.am.at[N1], q)
        loop(N16, send_cols_m)
    loop(N4, block_m)

    @pl.when(mine)
    def _():
        r.recv_m[chip] = r.send_m[slot]

    r.bd[ALL] = jnp.zeros_like(r.bd)
    r.wf[ALL] = w_opm_out[ALL].astype(F32)

    def build(c2):
        for e in range(N2):
            w = r.wf[pl.ds(N2 * c2 + e, N32, stride=N32), :].astype(BF16)
            for il in range(N4):
                r.bd[c2, e * N128 + il * N32:e * N128 + (il + N1) * N32, il * N128:(il + N1) * N128] = w
    loop(N16, build)
    r.rep4[ALL] = head_rep(N128, N4)
    r.hm4[ALL] = head_mask(N512, N4, N128)
    r.rept[ALL] = one_hot(iota(N128, N512, N1) // N4 == iota(N128, N512, N0))
    r.hmt[ALL] = (lax.rem(iota(N128, N512, N1), N4) == iota(N128, N512, N0) // N32).astype(F32)
    for e in range(N2):
        r.wet[e] = jnp.transpose(w_e_in[:, N256 + e * N128:N384 + e * N128].astype(F32)).astype(BF16)
    keep = jnp.where(iota(N8, N512, N0) == N0, keep_ref[ALL].astype(F32), 0.0).astype(BF16)
    r.keepc[ALL] = dot_c(keep, one_hot(iota(N8, N128, N0) < N8), N0, N0)
    r.keepr[ALL] = keep_ref[ALL].astype(F32)
    for il in range(N4):
        r.zf[il] = z_ref[il].astype(F32)

    def split_z(d):
        for il in range(N4):
            for jl in range(N4):
                r.zsplit[d, jl * N16:(jl + N1) * N16, il * N128:(il + N1) * N128] = r.zf[il, pl.ds(d * N4 + jl, N16, stride=N32), :].astype(BF16)
    loop(N8, split_z)

    ready(mine, r.recv_m, N63, N64, r.am.at[N1])
    def send_z_in(k):
        d = lax.rem(v + N1 + k, N8)
        send(r.zsplit.at[d], r.zin.at[v], r.zsem.at[N0], r.zsem.at[N1], u * N8 + d)
    loop(N7, send_z_in)
    r.zin[v] = r.zsplit[v]

    put(r.xs_m, r.recv_m[ALL].astype(F32).reshape(N1024, N256))

    for jl in range(N4):
        x = take(r.xs_m, jl, N256, N4)
        r.qkvg[ALL] = dot(layer_norm(x), w_col_in[ALL]).astype(BF16)

        def col_block(b, jl=jl):
            rows = pl.ds(pl.multiple_of(b * N64, N64), N64)
            qx = (dot(r.rep8[ALL], r.qkvg[rows, N0:N256]) * r.hm8[ALL]).astype(BF16)
            t = dot_t(qx, r.qkvg[:, N256:N512]) * SCALE
            t = jnp.where(r.cmask[jl:jl + N1, :] > N0, t, LOW)
            put(r.pv, dot(softmax_rows(t), r.qkvg[:, N512:N768]))
            r.gt_m[N0, rows, :] = gate(collapse(r.pv, N64, N8), r.qkvg[rows, N768:N1024])
        loop(N4, col_block, UNROLL_B)
        y = (x + dot(r.gt_m[N0], w_col_out[ALL])).astype(BF16)
        spread(r.yf_m, jl, N256, N4, y.astype(F32))
        ab = dot_t(layer_norm(y), w_opm_in[ALL]).astype(BF16)
        for side, ref in ((N0, r.left), (N1, r.right)):
            pick = one_hot(iota(N32, N64, N1) == iota(N32, N64, N0) + N32 * side)
            ref[jl] = (dot_c(pick, ab, N1, N1) * r.cmask[jl:jl + N1, :]).astype(BF16)

        def send_c(k, jl=jl):
            send(r.right.at[jl], r.rall.at[jl, u], r.csem.at[N0], r.csem.at[N1], lax.rem(u + N1 + k, N16) * N8 + v)
        loop(N15, send_c)

        def send_a(k, jl=jl):
            send(r.left.at[jl], r.lall.at[v, jl], r.lsem.at[N0], r.lsem.at[N1], u * N8 + lax.rem(v + N1 + k, N8))
        loop(N7, send_a)
        r.rall[jl, u] = r.right[jl]
        r.lall[v, jl] = r.left[jl]

    r.mcols[ALL] = join(r.yf_m).astype(BF16).reshape(N128, N8, N256)
    r.acc[ALL] = jnp.zeros_like(r.acc)
    wait_bytes(r.rall.at[:, pl.ds(N0, N15)], r.csem.at[N1])
    wait_bytes(r.lall.at[pl.ds(N0, N7)], r.lsem.at[N1])

    put(r.rf, r.rall[ALL].astype(F32).reshape(N2048, N256))

    def reorder(c):
        r.rc[c] = take(r.rf, c, N64, N32).astype(BF16)
    loop(N32, reorder, N4)

    def outer(d):
        r.o[d] = dot_t(r.rc[ALL].reshape(N2048, N256), r.lall[d].reshape(N128, N256)).astype(BF16).reshape(N32, N64, N128)
    loop(N8, outer)

    def mix(c2):
        parts = [r.o[:, N2 * c2 + e].reshape(N512, N128) for e in range(N2)]
        r.acc[ALL] += dot(jnp.concatenate(parts, axis=N1), r.bd[c2])
    loop(N16, mix)
    wait_bytes(r.zin.at[pl.ds(N0, N7)], r.zsem.at[N1])
    for d in range(N8):
        for il in range(N4):
            cols = slice(il * N128, (il + N1) * N128)
            upd = r.acc[d * N64:(d + N1) * N64, cols] * r.recip[:, d * N4 + il:d * N4 + il + N1]
            r.zs[d, :, cols] = (r.zin[d, :, cols].astype(F32) + upd).astype(BF16)

    def send_z(k):
        d = lax.rem(v + N1 + k, N8)
        send(r.zs.at[d], r.zback.at[v], r.bsem.at[N0], r.bsem.at[N1], u * N8 + d)
    loop(N7, send_z)
    r.zback[v] = r.zs[v]
    wait_bytes(r.zback.at[pl.ds(N0, N7)], r.bsem.at[N1])

    def merge_z(d):
        for il in range(N4):
            for jl in range(N4):
                r.zf[il, pl.ds(d * N4 + jl, N16, stride=N32), :] = r.zback[d, jl * N16:(jl + N1) * N16, il * N128:(il + N1) * N128].astype(F32)
    loop(N8, merge_z)

    for il in range(N4):
        r.zb[il] = r.zf[il].astype(BF16)
        r.e_f[il * N4:(il + N1) * N4, :] = dot_t(w_s_bias[ALL], layer_norm(r.zb[il]))
    r.slab_s[ALL] = r.e_f[N0:N16, :].astype(BF16)
    send(r.zb, r.xz.at[pl.ds(N4 * core, N4)], r.ysem.at[N0], r.ysem.at[N1], me + N1 - N2 * core)

    def send_slab_s(k):
        p = N2 * lax.rem(chip + N1 + k, N64) + half

        @pl.when(p != me)
        def _():
            send(r.slab_s, r.bias_s.at[slot], r.ss, r.gs.at[slot // N32], p)
    loop(N64, send_slab_s)

    @pl.when(mine)
    def _():
        r.bias_s[slot] = r.slab_s[ALL]

    def send_m_out(k):
        p = lax.rem(me + N1 + k, N128)
        send(r.mcols.at[p], r.mback.at[me], r.msem.at[N0], r.msem.at[N1], p)
    loop(N127, send_m_out)
    r.mback[me] = r.mcols[me]

    def project_z(i):
        r.xn_z[ALL] = layer_norm(r.xz[i])
        xn = r.xn_z[ALL]
        r.kv_z[i, :, N0:N128] = (dot(xn, w_s_in[:, N128:N256]) * r.keepc[ALL]).astype(BF16)
        r.kv_z[i, :, N128:N256] = dot(xn, w_s_in[:, N256:N384]).astype(BF16)
        xh = r.xn_z[hrows, :]
        r.q_z[i] = dot(xh, w_s_in[:, N0:N128]).astype(BF16)
        r.g_z[i] = dot(xh, w_s_in[:, N384:N512]).astype(BF16)

    def own_z(i):
        r.xz[N4 * core + i] = r.zb[i]
        project_z(N4 * core + i)
    loop(N4, own_z)
    wait_bytes(r.zb, r.ysem.at[N1])
    loop(N4, lambda i: project_z(N4 - N4 * core + i))

    def attend_z(b, i):
        rows = pl.ds(pl.multiple_of(b * N128, N128), N128)
        qx = (dot(r.rep4[ALL], r.q_z[i, rows, :]) * r.hm4[ALL]).astype(BF16)
        t = dot_t(qx, r.kv_z[i, :, N0:N128]) * SCALE + r.biasf[ALL]
        r.pv[N0] = dot(softmax_rows(t), r.kv_z[i, :, N128:N256])
        r.gt_z[i, rows, :] = gate(collapse(r.pv.at[N0:N1], N128, N4), r.g_z[i, rows, :])

    def block_z(step):
        b = lax.rem(jnp.where(chip // N32 == core, (chip - N32 * core) // N16, N0) + N1 + step, N2)
        ready(jnp.logical_and(mine, b == slot // N32), r.bias_s, 31, N32, r.gs.at[b])
        got = r.bias_s[pl.ds(b * N32, N32)].reshape(N512, N512).astype(F32)
        r.biasf[ALL] = jnp.where(r.keepr[ALL] > N0, got * LOG2E, LOW)
        loop(N8, lambda i: attend_z(b, i), UNROLL_C)
    loop(N2, block_z)

    for i in range(N8):
        y = (r.xz[i, hrows, :].astype(F32) + dot(r.gt_z[i], w_s_out[ALL])).astype(BF16)
        r.f_z[:, i] = y.astype(F32).reshape(N32, N8, N128)
        r.e_f[i * N4:(i + N1) * N4, N0:N256] = dot_t(w_e_bias[ALL], layer_norm(y))
    r.slab_e[ALL] = r.e_f[:, N0:N256].astype(BF16)
    r.send_zc[ALL] = r.f_z[ALL].astype(BF16).reshape(N32, N64, N128)

    def send_cols_z(k0):
        k = N32 * core + lax.rem(chip + N1 + k0, N32)
        q = N2 * k + half

        @pl.when(q != me)
        def _():
            send(r.send_zc.at[k - N32 * core], r.recv_zc.at[chip], r.az.at[N0], r.az.at[N1], q)
    loop(N32, send_cols_z)

    @pl.when(mine)
    def _():
        r.recv_zc[chip] = r.send_zc[chip - N32 * core]

    def send_slab_e(k0):
        send(r.slab_e, r.bias_e.at[chip], r.esem.at[N0], r.esem.at[N1], N2 * lax.rem(chip + N1 + k0, N64) + core)
    loop(N63, send_slab_e)
    r.bias_e[chip] = r.slab_e[ALL]

    wait_bytes(r.mback.at[pl.ds(N0, N127)], r.msem.at[N1])
    put(r.yf_m, r.mback[ALL].astype(F32).reshape(N1024, N256))
    for sl in range(N2):
        for jl in range(N4):
            spread(r.f_m, sl * N512 + jl, N128, N4, take(r.yf_m, sl * N4 + jl, N128, N8))
    m_out[ALL] = join(r.f_m).astype(BF16).reshape(N2, N512, N256)

    ready(mine, r.recv_zc, 31, N32, r.az.at[N1])
    taken = r.recv_zc.at[pl.ds(N32 * core, N32)]
    send(taken, taken, r.fsem.at[N0], r.fsem.at[N1], me + N1 - N2 * core)
    wait_bytes(taken, r.fsem.at[N1])
    r.xs_z[ALL] = r.recv_zc[ALL].astype(F32).reshape(N4096, N128)
    def project_e(j):
        r.xn_z[ALL] = layer_norm(r.xs_z[pl.ds(j, N512, stride=N8), :])
        xn = r.xn_z[ALL]
        r.k_e[j] = (dot(xn, w_e_in[:, N128:N256]) * r.keepc[ALL]).astype(BF16)
        r.v_e[j] = dot_t(r.wet[N0], xn).astype(BF16)
        xh = r.xn_z[hrows, :]
        r.q_z[j] = dot(xh, w_e_in[:, N0:N128]).astype(BF16)
        r.g_e[j] = dot_t(r.wet[N1], xh).astype(BF16)
    loop(N8, project_e)
    wait_bytes(r.bias_e.at[pl.ds(N0, N63)], r.esem.at[N1])

    def widen(b):
        rows = pl.ds(pl.multiple_of(b * N512, N512), N512)
        kept = dot(r.rep4[ALL], r.keepc[pl.ds(pl.multiple_of(b * N128, N128), N128), :].astype(BF16))
        got = r.bias_e[pl.ds(b * N16, N16)].reshape(N512, N256).astype(F32)
        for t in range(N2):
            r.biasf_e[rows, t * N128:(t + N1) * N128] = jnp.where(kept > N0, got[:, t * N128:(t + N1) * N128] * LOG2E, LOW)
    loop(N4, widen)

    def column(j):
        for b in range(N4):
            r.kx[b * N512:(b + N1) * N512, :] = (dot(r.rep4[ALL], r.k_e[j, b * N128:(b + N1) * N128, :]) * r.hm4[ALL]).astype(BF16)
            r.vx[:, b * N512:(b + N1) * N512] = (dot(r.v_e[j, :, b * N128:(b + N1) * N128], r.rept[ALL]) * r.hmt[ALL]).astype(BF16)
        t = (dot_t(r.kx[ALL], r.q_z[j]) * SCALE + r.biasf_e[ALL]).reshape(N256, N8, N256)
        top = jnp.max(t, axis=N0)
        top = jnp.maximum(top, pltpu.roll(top, N4, N0))
        e = jnp.exp2(t - top[None])
        total = jnp.sum(e, axis=N0)
        total = total + pltpu.roll(total, N4, N0)
        p = (e * (1.0 / total)[None]).astype(BF16).reshape(N2048, N256)
        gated = gate(dot(r.vx[ALL], p), r.g_e[j])
        y = dot_c(gated, w_e_out[ALL], N0, N0)
        r.y_z[pl.ds(j, N256, stride=N8), :] = r.xs_z[pl.ds(core * N2048 + j, N256, stride=N8), :] + y
    loop(N8, column, UNROLL_D)
    r.send_o[ALL] = r.y_z[ALL].astype(BF16).reshape(N64, N32, N128)

    def send_back(k0):
        k = lax.rem(slot + N1 + k0, N64)
        q = N64 * core + k

        @pl.when(q != me)
        def _():
            send(r.send_o.at[k], r.recv_o.at[chip], r.osem.at[N0], r.osem.at[N1], q)
    loop(N64, send_back)

    @pl.when(mine)
    def _():
        r.recv_o[chip] = r.send_o[slot]
    for ref, sem in ((r.bias_a, r.sa), (r.recv_m, r.am.at[N0]), (r.bias_s, r.ss)):
        ready(mine, ref, N63, N64, sem)
    ready(mine, r.recv_zc, 31, N32, r.az.at[N0])
    wait_bytes(taken, r.fsem.at[N0])
    wait_bytes(m_ref, r.xsem.at[N0])
    wait_bytes(r.zb, r.ysem.at[N0])
    wait_bytes(r.zin.at[pl.ds(N0, N7)], r.zsem.at[N0])
    wait_bytes(r.rall.at[:, pl.ds(N0, N15)], r.csem.at[N0])
    wait_bytes(r.lall.at[pl.ds(N0, N7)], r.lsem.at[N0])
    wait_bytes(r.zback.at[pl.ds(N0, N7)], r.bsem.at[N0])
    wait_bytes(r.mback.at[pl.ds(N0, N127)], r.msem.at[N0])
    wait_bytes(r.bias_e.at[pl.ds(N0, N63)], r.esem.at[N0])
    ready(mine, r.recv_o, N63, N64, r.osem.at[N1])
    got = r.recv_o[ALL].astype(F32).reshape(N64, N4, N8, N128)
    for il in range(N4):
        z_out[il] = got[:, il].reshape(N512, N128).astype(BF16)
    ready(mine, r.recv_o, N63, N64, r.osem.at[N0])


BUFFERS = dict(
    slab_a=(N32, N512), bias_a=(N64, N32, N512), xm=(N4, N512, N256), xn_m=(N512, N256), kv_m=(N4, N512, N512), q_m=(N4, N256, N256),
    g_m=(N4, N256, N256), gt_m=(N4, N256, N256), rep8=(N512, N64), zsplit=(N8, N64, N512), zin=(N8, N64, N512), send_m=(N64, N16, N256),
    recv_m=(N64, N16, N256), qkvg=(N256, N1024), left=(N4, N32, N256), right=(N4, N32, N256), lall=(N8, N4, N32, N256), rall=(N4, N16, N32, N256),
    mcols=(N128, N8, N256), o=(N8, N32, N64, N128), rc=(N32, N64, N256), mback=(N128, N8, N256), bd=(N16, N256, N512), zs=(N8, N64, N512), zback=(N8, N64, N512), zb=(N4, N512, N128),
    xz=(N8, N512, N128), slab_s=(N16, N512), bias_s=(N64, N16, N512), xn_z=(N512, N128), kv_z=(N8, N512, N256), q_z=(N8, N256, N128),
    g_z=(N8, N256, N128), gt_z=(N8, N256, N128), rep4=(N512, N128), rept=(N128, N512), wet=(N2, N128, N128), slab_e=(N32, N256),
    bias_e=(N64, N32, N256), send_zc=(N32, N64, N128), recv_zc=(N64, N64, N128), k_e=(N8, N512, N128), v_e=(N8, N128, N512), g_e=(N8, N128, N256), kx=(N2048, N128), vx=(N128, N2048),
    send_o=(N64, N32, N128), recv_o=(N64, N32, N128))
FLOATS = dict(
    slab_f=(N32, N512), rmask=(N4, N512), cmask=(N4, N256), recip=(N64, N32), hm8=(N512, N256), hm4=(N512, N128),
    hmt=(N128, N512), keepc=(N512, N128), keepr=(N1, N512), zf=(N4, N512, N128), pv=(N2, N512, N128), y_m=(N2, N64, N128), f_b=(N2, N256, N128),
    f_m=(N2, N1024, N128), xs_m=(N2, N1024, N128), yf_m=(N2, N1024, N128), wf=(N1024, N128), rf=(N2, N2048, N128), acc=(N512, N512),
    e_f=(N32, N512), biasf=(N512, N512), f_z=(N32, N8, N8, N128), biasf_e=(N2048, N256), xs_z=(N4096, N128), y_z=(N2048, N128))
SEMS = dict(ga=N4, gs=N2, xsem=N2, ysem=N2, zsem=N2, am=N2, csem=N2, lsem=N2, bsem=N2, msem=N2, az=N2, fsem=N2, esem=N2, osem=N2, sa=None, ss=None)


def solution(mesh):
    rows = P(('data', 'chip', 'dap'))
    in_specs = (rows, rows, P('data'), P('data')) + (P(),) * 13
    specs = {name: pltpu.VMEM(dims, BF16) for name, dims in BUFFERS.items()}
    specs.update({name: pltpu.VMEM(dims, F32) for name, dims in FLOATS.items()})
    specs.update({name: pltpu.SemaphoreType.DMA if n is None else pltpu.SemaphoreType.DMA((n,)) for name, n in SEMS.items()})

    def per_device(m_blk, z_blk, msa_mask, res_mask, *weights):
        w = list(weights)
        for k in (N1, 5, N8, 11):
            w[k] = w[k].T
        args = (m_blk, z_blk, msa_mask, res_mask.reshape(N1, N512), *w)
        vm = pl.BlockSpec(memory_space=pltpu.VMEM)
        return pl.pallas_call(
            functools.partial(kernel, tuple(specs)),
            out_shape=(jax.ShapeDtypeStruct(m_blk.shape, BF16), jax.ShapeDtypeStruct(z_blk.shape, BF16)),
            in_specs=[vm] * len(args), out_specs=(vm, vm), scratch_shapes=list(specs.values()),
            compiler_params=pltpu.CompilerParams(collective_id=N0, has_side_effects=True, vmem_limit_bytes=VMEM_LIMIT),
        )(*args)

    return jax.shard_map(per_device, mesh=mesh, in_specs=in_specs, out_specs=(rows, rows), check_vma=False)
```

```python
import functools
from types import SimpleNamespace

import jax
import jax.numpy as jnp
from jax import lax
from jax.experimental import pallas as pl
from jax.experimental.pallas import tpu as pltpu
from jax.sharding import PartitionSpec as P

N0 = 0
N1 = 1
N2 = 2
N3 = 3
N4 = 4
N7 = 7
N8 = 8
N15 = 15
N16 = 16
N32 = 32
N63 = 63
N64 = 64
N127 = 127
N128 = 128
N256 = 256
N384 = 384
N512 = 512
N768 = 768
N1024 = 1024
N2048 = 2048
N4096 = 4096
ALL = Ellipsis
MESH = pl.DeviceIdType.MESH
F32 = jnp.float32
BF16 = jnp.bfloat16
VMEM_LIMIT = 67043328
UNROLL_D = N1


def layer_norm(x):
    values = x.astype(F32)
    centred = values - jnp.mean(values, axis=-N1, keepdims=True)
    variance = jnp.mean(centred * centred, axis=-N1, keepdims=True)
    return (centred * lax.rsqrt(variance + 1e-5)).astype(BF16)


def dot(a, b):
    return jnp.dot(a, b, preferred_element_type=F32)


def dot_t(a, b):
    return lax.dot_general(a, b, (((N1,), (N1,)), ((), ())), preferred_element_type=F32)


def dev(p):
    return (N0, p // N8, lax.rem(p, N8))


def my_index():
    return lax.axis_index('chip') * N8 + lax.axis_index('dap')


def loop(n, body, unroll=N1):
    def step(i, carry):
        body(i)
        return carry
    lax.fori_loop(N0, n, step, N0, unroll=unroll)


def send(src, dst, send_sem, recv_sem, p):
    pltpu.make_async_remote_copy(src_ref=src, dst_ref=dst, send_sem=send_sem, recv_sem=recv_sem,
                                 device_id=dev(p), device_id_type=MESH).start()


def wait_bytes(ref, sem):
    pltpu.make_async_copy(ref, ref, sem).wait()


def head_rep(queries, heads):
    rows = queries * heads
    r = lax.broadcasted_iota(jnp.int32, (rows, queries), N0)
    c = lax.broadcasted_iota(jnp.int32, (rows, queries), N1)
    return (r // heads == c).astype(F32).astype(BF16)


def head_mask(rows, heads, width):
    r = lax.broadcasted_iota(jnp.int32, (rows, width), N0)
    c = lax.broadcasted_iota(jnp.int32, (rows, width), N1)
    return (lax.rem(r, heads) == c // N32).astype(F32)


def softmax_rows(t):
    e = jnp.exp2(t - jnp.max(t, axis=N1, keepdims=True))
    return (e * (1.0 / jnp.sum(e, axis=N1, keepdims=True))).astype(BF16)


def put(ref, value):
    for t in range(ref.shape[N0]):
        ref[t] = value[:, t * N128:(t + N1) * N128]


def take(ref, start, size, stride):
    return jnp.concatenate([ref[t, pl.ds(start, size, stride=stride), :] for t in range(ref.shape[N0])], axis=N1)


def join(ref):
    return jnp.concatenate([ref[t] for t in range(ref.shape[N0])], axis=N1)


def spread(ref, start, size, stride, value):
    for t in range(ref.shape[N0]):
        ref[t, pl.ds(start, size, stride=stride), :] = value[:, t * N128:(t + N1) * N128]


def collapse(r_ref, queries, heads):
    lane = lax.broadcasted_iota(jnp.int32, (queries, N128), N1) // N32
    parts = []
    for t in range(r_ref.shape[N0]):
        out = r_ref[t, pl.ds(N4 * t, queries, stride=heads), :]
        for h in range(N1, N4):
            out = jnp.where(lane == h, r_ref[t, pl.ds(N4 * t + h, queries, stride=heads), :], out)
        parts.append(out)
    return jnp.concatenate(parts, axis=N1) if len(parts) > N1 else parts[N0]


def gate(o, g):
    return (o * jax.nn.sigmoid(g.astype(F32))).astype(BF16)


LOG2E = 1.4426950408889634
SCALE = N32 ** -0.5 * LOG2E
LOW = -1e9 * LOG2E


def dot_c(a, b, da, db):
    return lax.dot_general(a, b, (((da,), (db,)), ((), ())), preferred_element_type=F32)


def iota(rows, cols, dim):
    return lax.broadcasted_iota(jnp.int32, (rows, cols), dim)


def one_hot(cond):
    return cond.astype(F32).astype(BF16)


def ready(cond, ref, few, many, sem):
    @pl.when(cond)
    def _():
        wait_bytes(ref.at[pl.ds(N0, few)], sem)

    @pl.when(jnp.logical_not(cond))
    def _():
        wait_bytes(ref.at[pl.ds(N0, many)], sem)


class Gather:
    def __init__(self, slab, buf, p1, p2, pz, py, s1, s2, s3):
        self.slab, self.buf, self.p1, self.p2, self.pz, self.py = slab, buf, p1, p2, pz, py
        self.s1, self.s2, self.s3 = s1, s2, s3
        me = my_index()
        self.me, self.core, chip, self.half = me, lax.rem(me, N2), me // N2, me // N64
        self.x, self.y, self.z = lax.rem(chip, N4), lax.rem(chip // N4, N4), chip // N16
        self.mine = self.core == self.half
        self.level = lax.rem(self.z, N2)
        self.own = jnp.where(self.core == N0, self.level * N16 + self.y * N4 + self.x, N32 + self.y * N8 + self.x * N2 + self.level)

    def to(self, dz, dy, dx, c):
        return N2 * (lax.rem(self.z + dz, N4) * N16 + lax.rem(self.y + dy, N4) * N4 + lax.rem(self.x + dx, N4)) + c

    def slots(self, start, n):
        return self.buf.at[pl.ds(start, n)]

    def first(self):
        for k in (N1, N3, N2, N0):
            p = jnp.where(self.core == N0, self.to(N0, N0, k, self.half), self.to(k, N0, N0, self.half))

            @pl.when(p != self.me)
            def _(p=p):
                send(self.slab, self.buf.at[self.own], self.s1, self.p1.at[self.core], p)

        @pl.when(self.mine)
        def _():
            self.buf[self.own] = self.slab[ALL]

    def second(self):
        @pl.when(self.mine)
        def _():
            ready(self.core == N0, self.buf, N3, N4, self.p1.at[N0])
            line = self.slots(self.level * N16 + self.y * N4, N4)
            for k in (N1, N3, N2):
                send(line, line, self.s2.at[N0], self.p2.at[N0], self.to(N0, k, N0, self.core))
        ready(jnp.logical_and(self.mine, self.core == N1), self.buf, N1, N2, self.p1.at[N1])
        pair = self.slots(N32 + self.y * N8 + self.x * N2, N2)
        for k in (N1, N3, N2):
            send(pair, pair, self.s2.at[N1], self.p2.at[N1], self.to(N0, N0, k, self.core))

    def third(self):
        @pl.when(self.mine)
        def _():
            wait_bytes(self.slots(N0, 12), self.p2.at[N0])
            plane = self.slots(self.level * N16, N16)
            for k in (N1, N3, N2):
                send(plane, plane, self.s3.at[N0], self.pz.at[self.level], self.to(k, N0, N0, self.core))
        wait_bytes(self.slots(N0, 6), self.p2.at[N1])
        row = self.slots(N32 + self.y * N8, N8)
        for k in (N1, N3, N2):
            send(row, row, self.s3.at[N1], self.py.at[self.y], self.to(N0, k, N0, self.core))

    def plane_ready(self, level):
        @pl.when(jnp.logical_not(jnp.logical_and(self.mine, level == self.level)))
        def _():
            wait_bytes(self.slots(N0, N16), self.pz.at[level])

    def row_ready(self, y):
        @pl.when(y != self.y)
        def _():
            wait_bytes(self.slots(N0, N8), self.py.at[y])

    def sent(self):
        ready(self.mine, self.buf, N3, N4, self.s1)

        @pl.when(self.mine)
        def _():
            wait_bytes(self.slots(N0, 12), self.s2.at[N0])
            wait_bytes(self.slots(N0, 48), self.s3.at[N0])
        wait_bytes(self.slots(N0, 6), self.s2.at[N1])
        wait_bytes(self.slots(N0, 24), self.s3.at[N1])


def slot_device(slot, half):
    first = slot < N32
    rest = slot - N32
    z = jnp.where(first, slot // N16, lax.rem(rest, N2))
    y = jnp.where(first, lax.rem(slot // N4, N4), rest // N8)
    x = jnp.where(first, lax.rem(slot, N4), lax.rem(rest // N2, N4))
    return half * N64 + z * N32 + y * N8 + x * N2 + jnp.where(first, N0, N1)


def kernel(scratch_names, m_ref, z_ref, mask_ref, keep_ref, w_row_in, w_row_bias, w_row_out, w_col_in, w_col_out,
           w_opm_in, w_opm_out, w_s_in, w_s_bias, w_s_out, w_e_in, w_e_bias, w_e_out, m_out, z_out, *scratch):
    r = SimpleNamespace(**dict(zip(scratch_names, scratch)))
    me = my_index()
    core, chip, half = lax.rem(me, N2), me // N2, me // N64
    u, v = me // N8, lax.rem(me, N8)
    slot = me - N64 * half
    mine = core == half
    hrows = pl.ds(pl.multiple_of(core * N256, N256), N256)
    bar = pltpu.get_barrier_semaphore()
    loop(N127, lambda k: pl.semaphore_signal(bar, inc=N1, device_id=dev(lax.rem(me + N1 + k, N128)), device_id_type=MESH))

    for il in range(N4):
        r.slab_f[il * N8:(il + N1) * N8, :] = dot_t(w_row_bias[ALL], layer_norm(z_ref[il]))
    r.slab_a[ALL] = r.slab_f[ALL].astype(BF16)
    pl.semaphore_wait(bar, N127)
    send(m_ref, r.xm.at[pl.ds(N2 * core, N2)], r.xsem.at[N0], r.xsem.at[N1], me + N1 - N2 * core)

    ga = Gather(r.slab_a, r.bias_a, r.a1, r.a2, r.az3, r.ay3, r.as1, r.as2, r.as3)
    ga.first()
    r.rep8[ALL] = head_rep(N64, N8)
    row = iota(N256, N256, N0)
    r.perm[ALL] = one_hot(iota(N256, N256, N1) == N4 * slot_device(row // N4, N0) + lax.rem(row, N4))
    r.hm8[ALL] = head_mask(N512, N8, N256)
    maskb = mask_ref[ALL].astype(F32).astype(BF16)
    r.rmask[ALL] = dot(one_hot(iota(N4, N256, N1) == N4 * chip + iota(N4, N256, N0)), maskb)
    r.cmask[ALL] = dot_c(one_hot(iota(N4, N512, N1) == N4 * me + iota(N4, N512, N0)), maskb, N1, N1)
    lane = iota(N512, N64, N1)
    mask_j = dot(maskb, one_hot(iota(N512, N64, N0) == N32 * lax.rem(lane, N16) + N4 * v + lane // N16)).astype(BF16)
    mask_i = dot(maskb, one_hot(iota(N512, N32, N0) == N32 * u + iota(N512, N32, N1))).astype(BF16)
    recip = 1.0 / (1e-3 + dot_c(mask_j, mask_i, N0, N0))
    for d in range(N8):
        r.recip[d] = recip[:, d * N4:(d + N1) * N4]

    def project_m(s):
        r.xn_m[ALL] = layer_norm(r.xm[s])
        r.kv_m[s] = dot(r.xn_m[ALL], w_row_in[:, N256:N768]).astype(BF16)
        xh = dot(r.perm[ALL], r.xn_m[hrows, :]).astype(BF16)
        r.x_half[s] = dot(r.perm[ALL], r.xm[s, hrows, :]).astype(BF16)
        r.q_m[s] = dot(xh, w_row_in[:, N0:N256]).astype(BF16)
        r.g_m[s] = dot(xh, w_row_in[:, N768:N1024]).astype(BF16)

    def own_m(s):
        r.xm[N2 * core + s] = m_ref[s]
        project_m(N2 * core + s)
    loop(N2, own_m)
    ga.second()
    wait_bytes(m_ref, r.xsem.at[N1])
    loop(N2, lambda s: project_m(N2 - N2 * core + s))
    ga.third()

    def attend_m(b, s, pv):
        rows = pl.ds(pl.multiple_of(b * N64, N64), N64)
        qx = (dot(r.rep8[ALL], r.q_m[s, rows, :]) * r.hm8[ALL]).astype(BF16)
        t = dot_t(qx, r.kv_m[s, :, N0:N256]) * SCALE + r.biasf[ALL]
        t = jnp.where(r.rmask[pl.ds(s, N1), :] > N0, t, LOW)
        put(pv, dot(softmax_rows(t), r.kv_m[s, :, N256:N512]))
        r.gt_m[s, rows, :] = gate(collapse(pv, N64, N8), r.g_m[s, rows, :])

    def pair_m(b, s2):
        for e in range(N2):
            attend_m(b, N2 * s2 + e, r.pv.at[e])

    def finish_m(b, s):
        rows = pl.ds(pl.multiple_of(b * N64, N64), N64)
        put(r.y_m, r.x_half[s, rows, :].astype(F32) + dot(r.gt_m[s, rows, :], w_row_out[ALL]))
        for jl in range(N4):
            spread(r.f_b, s * N4 + jl, N16, N16, take(r.y_m, jl, N16, N4))

    def block_m(step):
        late = jnp.where(mine, N0, N2)
        planes = jnp.logical_or(step == late, step == N3)
        level = jnp.where(step == late, ga.level, N1 - ga.level)
        two = jnp.where(step == N1 - late // N2, ga.y // N2, N1 - ga.y // N2)
        b = jnp.where(planes, level, N2 + two)

        @pl.when(planes)
        def _():
            ga.plane_ready(level)

        @pl.when(jnp.logical_not(planes))
        def _():
            for e in range(N2):
                ga.row_ready(N2 * two + e)
        r.biasf[ALL] = r.bias_a[pl.ds(b * N16, N16)].reshape(N512, N512).astype(F32) * LOG2E
        loop(N2, lambda s2: pair_m(b, s2))
        loop(N4, lambda s: finish_m(b, s))
        r.send_m[pl.ds(b * N16, N16)] = join(r.f_b).astype(BF16).reshape(N16, N16, N256)

        def send_cols_m(k0):
            k = b * N16 + lax.rem(ga.own + N1 + k0, N16)
            q = slot_device(k, core)

            @pl.when(q != me)
            def _():
                send(r.send_m.at[k], r.recv_m.at[chip], r.am.at[N0], r.am.at[N1], q)
        loop(N16, send_cols_m)
    loop(N4, block_m)

    @pl.when(mine)
    def _():
        r.recv_m[chip] = r.send_m[ga.own]

    r.bd[ALL] = jnp.zeros_like(r.bd)
    r.wf[ALL] = w_opm_out[ALL].astype(F32)

    def build(c2):
        for e in range(N2):
            w = r.wf[pl.ds(N2 * c2 + e, N32, stride=N32), :].astype(BF16)
            for il in range(N4):
                r.bd[c2, e * N128 + il * N32:e * N128 + (il + N1) * N32, il * N128:(il + N1) * N128] = w
    loop(N16, build)
    r.rep4[ALL] = head_rep(N128, N4)
    r.hm4[ALL] = head_mask(N512, N4, N128)
    for e in range(N2):
        r.wet[e] = jnp.transpose(w_e_in[:, N256 + e * N128:N384 + e * N128].astype(F32)).astype(BF16)
    keep = jnp.where(iota(N8, N512, N0) == N0, keep_ref[ALL].astype(F32), 0.0).astype(BF16)
    r.keepc[ALL] = dot_c(keep, one_hot(iota(N8, N128, N0) < N8), N0, N0)
    r.keepr[ALL] = keep_ref[ALL].astype(F32)
    for il in range(N4):
        r.zf[il] = z_ref[il].astype(F32)

    def split_z(d):
        for il in range(N4):
            for jl in range(N4):
                r.zsplit[d, jl * N16:(jl + N1) * N16, il * N128:(il + N1) * N128] = r.zf[il, pl.ds(d * N4 + jl, N16, stride=N32), :].astype(BF16)
    loop(N8, split_z)

    ready(mine, r.recv_m, N63, N64, r.am.at[N1])
    def send_z_in(k):
        d = lax.rem(v + N1 + k, N8)
        send(r.zsplit.at[d], r.zin.at[v], r.zsem.at[N0], r.zsem.at[N1], u * N8 + d)
    loop(N7, send_z_in)
    r.zin[v] = r.zsplit[v]

    put(r.xs_m, r.recv_m[ALL].astype(F32).reshape(N1024, N256))

    for jl in range(N4):
        x = take(r.xs_m, jl, N256, N4)
        r.qkvg[ALL] = dot(layer_norm(x), w_col_in[ALL]).astype(BF16)

        for b in range(N4):
            rows, pv = slice(b * N64, (b + N1) * N64), r.pv.at[b]
            qx = (dot(r.rep8[ALL], r.qkvg[rows, N0:N256]) * r.hm8[ALL]).astype(BF16)
            t = dot_t(qx, r.qkvg[:, N256:N512]) * SCALE
            t = jnp.where(r.cmask[jl:jl + N1, :] > N0, t, LOW)
            put(pv, dot(softmax_rows(t), r.qkvg[:, N512:N768]))
            r.gt_m[N0, rows, :] = gate(collapse(pv, N64, N8), r.qkvg[rows, N768:N1024])
        y = (x + dot(r.gt_m[N0], w_col_out[ALL])).astype(BF16)
        spread(r.yf_m, jl, N256, N4, y.astype(F32))
        ab = dot_t(layer_norm(y), w_opm_in[ALL]).astype(BF16)
        for side, ref in ((N0, r.left), (N1, r.right)):
            pick = one_hot(iota(N32, N64, N1) == iota(N32, N64, N0) + N32 * side)
            ref[jl] = (dot_c(pick, ab, N1, N1) * r.cmask[jl:jl + N1, :]).astype(BF16)

        def send_c(k, jl=jl):
            send(r.right.at[jl], r.rall.at[jl, u], r.csem.at[N0], r.csem.at[N1], lax.rem(u + N1 + k, N16) * N8 + v)
        loop(N15, send_c)

        def send_a(k, jl=jl):
            send(r.left.at[jl], r.lall.at[v, jl], r.lsem.at[N0], r.lsem.at[N1], u * N8 + lax.rem(v + N1 + k, N8))
        loop(N7, send_a)
        r.rall[jl, u] = r.right[jl]
        r.lall[v, jl] = r.left[jl]

    r.mcols[ALL] = join(r.yf_m).astype(BF16).reshape(N128, N8, N256)
    wait_bytes(r.rall.at[:, pl.ds(N0, N15)], r.csem.at[N1])
    wait_bytes(r.lall.at[pl.ds(N0, N7)], r.lsem.at[N1])

    put(r.rf, r.rall[ALL].astype(F32).reshape(N2048, N256))

    def reorder(c):
        r.rc[c] = take(r.rf, c, N64, N32).astype(BF16)
    loop(N32, reorder, N4)

    wait_bytes(r.zin.at[pl.ds(N0, N7)], r.zsem.at[N1])

    def group(g):
        def outer(t):
            d = lax.rem(v + N1 + N4 * g + t, N8)
            r.o[t] = dot_t(r.rc[ALL].reshape(N2048, N256), r.lall[d].reshape(N128, N256)).astype(BF16).reshape(N32, N64, N128)
        loop(N4, outer)

        def mix(c4):
            total = None
            for e in range(N4):
                c = c4 * N8 + N2 * e
                part = dot(jnp.concatenate([r.o[:, c].reshape(N256, N128), r.o[:, c + N1].reshape(N256, N128)], axis=N1), r.bd[c4 * N4 + e])
                total = part if total is None else total + part
            r.acc[ALL] = jnp.where(c4 == N0, 0.0, r.acc[ALL]) + total
        loop(N4, mix)

        def update(t):
            d = lax.rem(v + N1 + N4 * g + t, N8)
            rows = pl.ds(pl.multiple_of(t * N64, N64), N64)
            for il in range(N4):
                cols = slice(il * N128, (il + N1) * N128)
                upd = r.acc[rows, cols] * r.recip[d, :, il:il + N1]
                r.zs[d, :, cols] = (r.zin[d, :, cols].astype(F32) + upd).astype(BF16)

            @pl.when(d != v)
            def _():
                send(r.zs.at[d], r.zback.at[v], r.bsem.at[N0], r.bsem.at[N1], u * N8 + d)
        loop(N4, update)
    loop(N2, group)
    r.zback[v] = r.zs[v]
    wait_bytes(r.zback.at[pl.ds(N0, N7)], r.bsem.at[N1])

    def merge_z(d):
        for il in range(N4):
            for jl in range(N4):
                r.zf[il, pl.ds(d * N4 + jl, N16, stride=N32), :] = r.zback[d, jl * N16:(jl + N1) * N16, il * N128:(il + N1) * N128].astype(F32)
    loop(N8, merge_z)

    for il in range(N4):
        r.zb[il] = r.zf[il].astype(BF16)
        r.e_f[il * N4:(il + N1) * N4, :] = dot_t(w_s_bias[ALL], layer_norm(r.zb[il]))
    r.slab_s[ALL] = r.e_f[N0:N16, :].astype(BF16)
    send(r.zb, r.xz.at[pl.ds(N4 * core, N4)], r.ysem.at[N0], r.ysem.at[N1], me + N1 - N2 * core)

    def send_slab_s(k):
        p = N2 * lax.rem(chip + N1 + k, N64) + half

        @pl.when(p != me)
        def _():
            send(r.slab_s, r.bias_s.at[slot], r.ss, r.gs.at[slot // N32], p)
    loop(N64, send_slab_s)

    @pl.when(mine)
    def _():
        r.bias_s[slot] = r.slab_s[ALL]

    def project_z(i):
        r.xn_z[ALL] = layer_norm(r.xz[i])
        xn = r.xn_z[ALL]
        r.kv_z[i, :, N0:N128] = (dot(xn, w_s_in[:, N128:N256]) * r.keepc[ALL]).astype(BF16)
        r.kv_z[i, :, N128:N256] = dot(xn, w_s_in[:, N256:N384]).astype(BF16)
        xh = r.xn_z[hrows, :]
        r.q_z[i] = dot(xh, w_s_in[:, N0:N128]).astype(BF16)
        r.g_z[i] = dot(xh, w_s_in[:, N384:N512]).astype(BF16)

    def own_z(i):
        r.xz[N4 * core + i] = r.zb[i]
        project_z(N4 * core + i)
    loop(N4, own_z)
    wait_bytes(r.zb, r.ysem.at[N1])
    loop(N4, lambda i: project_z(N4 - N4 * core + i))

    def send_m_out(k):
        p = lax.rem(me + N1 + k, N128)
        send(r.mcols.at[p], r.mback.at[me], r.msem.at[N0], r.msem.at[N1], p)
    loop(N127, send_m_out)
    r.mback[me] = r.mcols[me]

    def attend_z(b, i, pv):
        rows = pl.ds(pl.multiple_of(b * N128, N128), N128)
        qx = (dot(r.rep4[ALL], r.q_z[i, rows, :]) * r.hm4[ALL]).astype(BF16)
        t = dot_t(qx, r.kv_z[i, :, N0:N128]) * SCALE + r.biasf[ALL]
        put(pv, dot(softmax_rows(t), r.kv_z[i, :, N128:N256]))
        r.gt_z[i, rows, :] = gate(collapse(pv, N128, N4), r.g_z[i, rows, :])

    def pair_z(b, i2):
        for e in range(N2):
            attend_z(b, N2 * i2 + e, r.pv.at[e, N0:N1])

    def block_z(step):
        b = lax.rem(jnp.where(chip // N32 == core, (chip - N32 * core) // N16, N0) + N1 + step, N2)
        ready(jnp.logical_and(mine, b == slot // N32), r.bias_s, 31, N32, r.gs.at[b])
        got = r.bias_s[pl.ds(b * N32, N32)].reshape(N512, N512).astype(F32)
        r.biasf[ALL] = jnp.where(r.keepr[ALL] > N0, got * LOG2E, LOW)
        loop(N4, lambda i2: pair_z(b, i2))
    loop(N2, block_z)

    for i in range(N8):
        y = (r.xz[i, hrows, :].astype(F32) + dot(r.gt_z[i], w_s_out[ALL])).astype(BF16)
        r.f_z[:, i] = y.astype(F32).reshape(N32, N8, N128)
        spread(r.e_b, i, N4, N8, dot_t(w_e_bias[ALL], layer_norm(y)))
    r.slab_e[ALL] = join(r.e_b).astype(BF16)
    r.send_zc[ALL] = r.f_z[ALL].astype(BF16).reshape(N32, N64, N128)

    def send_cols_z(k0):
        k = N32 * core + lax.rem(chip + N1 + k0, N32)
        q = N2 * k + half

        @pl.when(q != me)
        def _():
            send(r.send_zc.at[k - N32 * core], r.recv_zc.at[chip], r.az.at[N0], r.az.at[N1], q)
    loop(N32, send_cols_z)

    @pl.when(mine)
    def _():
        r.recv_zc[chip] = r.send_zc[chip - N32 * core]

    def send_slab_e(k0):
        send(r.slab_e, r.bias_e.at[chip], r.esem.at[N0], r.esem.at[N1], N2 * lax.rem(chip + N1 + k0, N64) + core)
    loop(N63, send_slab_e)
    r.bias_e[chip] = r.slab_e[ALL]

    wait_bytes(r.mback.at[pl.ds(N0, N127)], r.msem.at[N1])
    put(r.yf_m, r.mback[ALL].astype(F32).reshape(N1024, N256))
    for sl in range(N2):
        for jl in range(N4):
            spread(r.f_m, sl * N512 + jl, N128, N4, take(r.yf_m, sl * N4 + jl, N128, N8))
    m_out[ALL] = join(r.f_m).astype(BF16).reshape(N2, N512, N256)

    ready(mine, r.recv_zc, 31, N32, r.az.at[N1])
    taken = r.recv_zc.at[pl.ds(N32 * core, N32)]
    send(taken, taken, r.fsem.at[N0], r.fsem.at[N1], me + N1 - N2 * core)
    wait_bytes(taken, r.fsem.at[N1])
    r.xs_z[ALL] = r.recv_zc[ALL].astype(F32).reshape(N4096, N128)
    def project_e(j):
        r.xn_z[ALL] = layer_norm(r.xs_z[pl.ds(j, N512, stride=N8), :])
        xn = r.xn_z[ALL]
        r.k_e[j] = (dot(xn, w_e_in[:, N128:N256]) * r.keepc[ALL]).astype(BF16)
        r.v_e[j] = dot_t(r.wet[N0], xn).astype(BF16)
        xh = r.xn_z[hrows, :]
        r.q_z[j] = dot(xh, w_e_in[:, N0:N128]).astype(BF16)
        r.g_e[j] = dot_t(r.wet[N1], xh).astype(BF16)
    loop(N8, project_e)
    wait_bytes(r.bias_e.at[pl.ds(N0, N63)], r.esem.at[N1])

    def widen(b):
        rows = pl.ds(pl.multiple_of(b * N128, N128), N128)
        kept = r.keepc[rows, :].reshape(N16, N8, N128)
        got = r.bias_e[pl.ds(b * N16, N16)].astype(F32).reshape(N16, N4, N8, N256) * LOG2E
        for h in range(N4):
            for t in range(N2):
                lanes = slice(t * N128, (t + N1) * N128)
                r.biasf_e[h, rows, lanes] = jnp.where(kept > N0, got[:, h, :, lanes], LOW).reshape(N128, N128)
    loop(N4, widen)

    def column(j):
        lane = iota(N256, N128, N1) // N32
        row = iota(N128, N512, N0) // N32
        probs, values = [], []
        for h in range(N4):
            qh = jnp.where(lane == h, r.q_z[j].astype(F32), 0.0).astype(BF16)
            t = dot_t(r.k_e[j], qh) * SCALE + r.biasf_e[h]
            e = jnp.exp2(t - jnp.max(t, axis=N0, keepdims=True))
            probs.append((e * (1.0 / jnp.sum(e, axis=N0, keepdims=True))).astype(BF16))
            values.append(jnp.where(row == h, r.v_e[j].astype(F32), 0.0).astype(BF16))
        gated = gate(dot(jnp.concatenate(values, axis=N1), jnp.concatenate(probs, axis=N0)), r.g_e[j])
        y = dot_c(gated, w_e_out[ALL], N0, N0)
        r.y_z[pl.ds(j, N256, stride=N8), :] = r.xs_z[pl.ds(core * N2048 + j, N256, stride=N8), :] + y
    loop(N8, column, UNROLL_D)
    r.send_o[ALL] = r.y_z[ALL].astype(BF16).reshape(N64, N32, N128)

    def send_back(k0):
        k = lax.rem(slot + N1 + k0, N64)
        q = N64 * core + k

        @pl.when(q != me)
        def _():
            send(r.send_o.at[k], r.recv_o.at[chip], r.osem.at[N0], r.osem.at[N1], q)
    loop(N64, send_back)

    @pl.when(mine)
    def _():
        r.recv_o[chip] = r.send_o[slot]
    ga.sent()
    ready(mine, r.recv_m, N63, N64, r.am.at[N0])
    ready(mine, r.bias_s, N63, N64, r.ss)
    ready(mine, r.recv_zc, 31, N32, r.az.at[N0])
    wait_bytes(taken, r.fsem.at[N0])
    wait_bytes(m_ref, r.xsem.at[N0])
    wait_bytes(r.zb, r.ysem.at[N0])
    wait_bytes(r.zin.at[pl.ds(N0, N7)], r.zsem.at[N0])
    wait_bytes(r.rall.at[:, pl.ds(N0, N15)], r.csem.at[N0])
    wait_bytes(r.lall.at[pl.ds(N0, N7)], r.lsem.at[N0])
    wait_bytes(r.zback.at[pl.ds(N0, N7)], r.bsem.at[N0])
    wait_bytes(r.mback.at[pl.ds(N0, N127)], r.msem.at[N0])
    wait_bytes(r.bias_e.at[pl.ds(N0, N63)], r.esem.at[N0])
    ready(mine, r.recv_o, N63, N64, r.osem.at[N1])
    got = r.recv_o[ALL].astype(F32).reshape(N64, N4, N8, N128)
    for il in range(N4):
        z_out[il] = got[:, il].reshape(N512, N128).astype(BF16)
    ready(mine, r.recv_o, N63, N64, r.osem.at[N0])


BUFFERS = dict(
    slab_a=(N32, N512), bias_a=(N64, N32, N512), xm=(N4, N512, N256), xn_m=(N512, N256), kv_m=(N4, N512, N512), q_m=(N4, N256, N256),
    g_m=(N4, N256, N256), gt_m=(N4, N256, N256), rep8=(N512, N64), perm=(N256, N256), x_half=(N4, N256, N256), zsplit=(N8, N64, N512), zin=(N8, N64, N512), send_m=(N64, N16, N256),
    recv_m=(N64, N16, N256), qkvg=(N256, N1024), left=(N4, N32, N256), right=(N4, N32, N256), lall=(N8, N4, N32, N256), rall=(N4, N16, N32, N256),
    mcols=(N128, N8, N256), o=(N4, N32, N64, N128), rc=(N32, N64, N256), mback=(N128, N8, N256), bd=(N16, N256, N512), zs=(N8, N64, N512), zback=(N8, N64, N512), zb=(N4, N512, N128),
    xz=(N8, N512, N128), slab_s=(N16, N512), bias_s=(N64, N16, N512), xn_z=(N512, N128), kv_z=(N8, N512, N256), q_z=(N8, N256, N128),
    g_z=(N8, N256, N128), gt_z=(N8, N256, N128), rep4=(N512, N128), wet=(N2, N128, N128), slab_e=(N32, N256),
    bias_e=(N64, N32, N256), send_zc=(N32, N64, N128), recv_zc=(N64, N64, N128), k_e=(N8, N512, N128), v_e=(N8, N128, N512), g_e=(N8, N128, N256),
    send_o=(N64, N32, N128), recv_o=(N64, N32, N128))
FLOATS = dict(
    slab_f=(N32, N512), rmask=(N4, N512), cmask=(N4, N256), recip=(N8, N64, N4), hm8=(N512, N256), hm4=(N512, N128),
    keepc=(N512, N128), keepr=(N1, N512), zf=(N4, N512, N128), pv=(N4, N2, N512, N128), y_m=(N2, N64, N128), f_b=(N2, N256, N128),
    f_m=(N2, N1024, N128), xs_m=(N2, N1024, N128), yf_m=(N2, N1024, N128), wf=(N1024, N128), rf=(N2, N2048, N128), acc=(N256, N512),
    e_f=(N32, N512), biasf=(N512, N512), f_z=(N32, N8, N8, N128), biasf_e=(N4, N512, N256), e_b=(N2, N32, N128), xs_z=(N4096, N128), y_z=(N2048, N128))
SEMS = dict(a1=N2, a2=N2, az3=N2, ay3=N4, as1=None, as2=N2, as3=N2, gs=N2, ss=None, xsem=N2, ysem=N2, zsem=N2, am=N2, csem=N2, lsem=N2, bsem=N2, msem=N2, az=N2, fsem=N2, esem=N2, osem=N2)


def solution(mesh):
    rows = P(('data', 'chip', 'dap'))
    in_specs = (rows, rows, P('data'), P('data')) + (P(),) * 13
    specs = {name: pltpu.VMEM(dims, BF16) for name, dims in BUFFERS.items()}
    specs.update({name: pltpu.VMEM(dims, F32) for name, dims in FLOATS.items()})
    specs.update({name: pltpu.SemaphoreType.DMA if n is None else pltpu.SemaphoreType.DMA((n,)) for name, n in SEMS.items()})

    def per_device(m_blk, z_blk, msa_mask, res_mask, *weights):
        w = list(weights)
        for k in (N1, 5, N8, 11):
            w[k] = w[k].T
        args = (m_blk, z_blk, msa_mask, res_mask.reshape(N1, N512), *w)
        vm = pl.BlockSpec(memory_space=pltpu.VMEM)
        return pl.pallas_call(
            functools.partial(kernel, tuple(specs)),
            out_shape=(jax.ShapeDtypeStruct(m_blk.shape, BF16), jax.ShapeDtypeStruct(z_blk.shape, BF16)),
            in_specs=[vm] * len(args), out_specs=(vm, vm), scratch_shapes=list(specs.values()),
            compiler_params=pltpu.CompilerParams(collective_id=N0, has_side_effects=True, vmem_limit_bytes=VMEM_LIMIT),
        )(*args)

    return jax.shard_map(per_device, mesh=mesh, in_specs=in_specs, out_specs=(rows, rows), check_vma=False)
```

```python
import functools
from types import SimpleNamespace

import jax
import jax.numpy as jnp
from jax import lax
from jax.experimental import pallas as pl
from jax.experimental.pallas import tpu as pltpu
from jax.sharding import PartitionSpec as P

N0 = 0
N1 = 1
N2 = 2
N3 = 3
N4 = 4
N7 = 7
N8 = 8
N15 = 15
N16 = 16
N32 = 32
N63 = 63
N64 = 64
N127 = 127
N128 = 128
N256 = 256
N384 = 384
N512 = 512
N768 = 768
N1024 = 1024
N2048 = 2048
N4096 = 4096
ALL = Ellipsis
MESH = pl.DeviceIdType.MESH
F32 = jnp.float32
BF16 = jnp.bfloat16
VMEM_LIMIT = 67043328


def layer_norm(x):
    values = x.astype(F32)
    centred = values - jnp.mean(values, axis=-N1, keepdims=True)
    variance = jnp.mean(centred * centred, axis=-N1, keepdims=True)
    return (centred * lax.rsqrt(variance + 1e-5)).astype(BF16)


def dot(a, b):
    return jnp.dot(a, b, preferred_element_type=F32)


def dot_t(a, b):
    return lax.dot_general(a, b, (((N1,), (N1,)), ((), ())), preferred_element_type=F32)


def dev(p):
    return (N0, p // N8, lax.rem(p, N8))


def my_index():
    return lax.axis_index('chip') * N8 + lax.axis_index('dap')


def loop(n, body, unroll=N1):
    def step(i, carry):
        body(i)
        return carry
    lax.fori_loop(N0, n, step, N0, unroll=unroll)


def send(src, dst, send_sem, recv_sem, p):
    pltpu.make_async_remote_copy(src_ref=src, dst_ref=dst, send_sem=send_sem, recv_sem=recv_sem,
                                 device_id=dev(p), device_id_type=MESH).start()


def wait_bytes(ref, sem):
    pltpu.make_async_copy(ref, ref, sem).wait()


def head_rep(queries, heads):
    rows = queries * heads
    r = lax.broadcasted_iota(jnp.int32, (rows, queries), N0)
    c = lax.broadcasted_iota(jnp.int32, (rows, queries), N1)
    return (r // heads == c).astype(F32).astype(BF16)


def head_mask(rows, heads, width):
    r = lax.broadcasted_iota(jnp.int32, (rows, width), N0)
    c = lax.broadcasted_iota(jnp.int32, (rows, width), N1)
    return (lax.rem(r, heads) == c // N32).astype(F32)


def softmax_rows(t):
    e = jnp.exp2(t - jnp.max(t, axis=N1, keepdims=True))
    return (e * (1.0 / jnp.sum(e, axis=N1, keepdims=True))).astype(BF16)


def put(ref, value):
    for t in range(ref.shape[N0]):
        ref[t] = value[:, t * N128:(t + N1) * N128]


def take(ref, start, size, stride):
    return jnp.concatenate([ref[t, pl.ds(start, size, stride=stride), :] for t in range(ref.shape[N0])], axis=N1)


def join(ref):
    return jnp.concatenate([ref[t] for t in range(ref.shape[N0])], axis=N1)


def spread(ref, start, size, stride, value):
    for t in range(ref.shape[N0]):
        ref[t, pl.ds(start, size, stride=stride), :] = value[:, t * N128:(t + N1) * N128]


def collapse(r_ref, queries, heads):
    lane = lax.broadcasted_iota(jnp.int32, (queries, N128), N1) // N32
    parts = []
    for t in range(r_ref.shape[N0]):
        out = r_ref[t, pl.ds(N4 * t, queries, stride=heads), :]
        for h in range(N1, N4):
            out = jnp.where(lane == h, r_ref[t, pl.ds(N4 * t + h, queries, stride=heads), :], out)
        parts.append(out)
    return jnp.concatenate(parts, axis=N1) if len(parts) > N1 else parts[N0]


def softmax_cols(t):
    e = jnp.exp2(t - jnp.max(t, axis=N0, keepdims=True))
    return (e * (1.0 / jnp.sum(e, axis=N0, keepdims=True))).astype(BF16)


def heads_attend(queries, keys, values, logits):
    lane, row = iota(*queries.shape, N1) // N32, iota(*values.shape, N0) // N32
    wide_q, wide_v = queries.astype(F32), values.astype(F32)
    probs, parts = [], []
    for h in range(N4):
        scores = dot_t(keys, jnp.where(lane == h, wide_q, 0.0).astype(BF16)) * SCALE
        probs.append(softmax_cols(logits(h, scores)))
        parts.append(jnp.where(row == h, wide_v, 0.0).astype(BF16))
    return dot(jnp.concatenate(parts, axis=N1), jnp.concatenate(probs, axis=N0))


def gate(o, g):
    return (o * jax.nn.sigmoid(g.astype(F32))).astype(BF16)


LOG2E = 1.4426950408889634
SCALE = N32 ** -0.5 * LOG2E
LOW = -1e9 * LOG2E


def dot_c(a, b, da, db):
    return lax.dot_general(a, b, (((da,), (db,)), ((), ())), preferred_element_type=F32)


def iota(rows, cols, dim):
    return lax.broadcasted_iota(jnp.int32, (rows, cols), dim)


def one_hot(cond):
    return cond.astype(F32).astype(BF16)


def ready(cond, ref, few, many, sem):
    @pl.when(cond)
    def _():
        wait_bytes(ref.at[pl.ds(N0, few)], sem)

    @pl.when(jnp.logical_not(cond))
    def _():
        wait_bytes(ref.at[pl.ds(N0, many)], sem)


class Gather:
    def __init__(self, slab, buf, p1, p2, pz, py, s1, s2, s3):
        self.slab, self.buf, self.p1, self.p2, self.pz, self.py = slab, buf, p1, p2, pz, py
        self.s1, self.s2, self.s3 = s1, s2, s3
        me = my_index()
        self.me, self.core, chip, self.half = me, lax.rem(me, N2), me // N2, me // N64
        self.x, self.y, self.z = lax.rem(chip, N4), lax.rem(chip // N4, N4), chip // N16
        self.mine = self.core == self.half
        self.level = lax.rem(self.z, N2)
        self.own = jnp.where(self.core == N0, self.level * N16 + self.y * N4 + self.x, N32 + self.y * N8 + self.x * N2 + self.level)

    def to(self, dz, dy, dx, c):
        return N2 * (lax.rem(self.z + dz, N4) * N16 + lax.rem(self.y + dy, N4) * N4 + lax.rem(self.x + dx, N4)) + c

    def slots(self, start, n):
        return self.buf.at[pl.ds(start, n)]

    def first(self):
        for k in (N1, N3, N2, N0):
            p = jnp.where(self.core == N0, self.to(N0, N0, k, self.half), self.to(k, N0, N0, self.half))

            @pl.when(p != self.me)
            def _(p=p):
                send(self.slab, self.buf.at[self.own], self.s1, self.p1.at[self.core], p)

        @pl.when(self.mine)
        def _():
            self.buf[self.own] = self.slab[ALL]

    def second(self):
        @pl.when(self.mine)
        def _():
            ready(self.core == N0, self.buf, N3, N4, self.p1.at[N0])
            line = self.slots(self.level * N16 + self.y * N4, N4)
            for k in (N1, N3, N2):
                send(line, line, self.s2.at[N0], self.p2.at[N0], self.to(N0, k, N0, self.core))
        ready(jnp.logical_and(self.mine, self.core == N1), self.buf, N1, N2, self.p1.at[N1])
        pair = self.slots(N32 + self.y * N8 + self.x * N2, N2)
        for k in (N1, N3, N2):
            send(pair, pair, self.s2.at[N1], self.p2.at[N1], self.to(N0, N0, k, self.core))

    def third(self):
        @pl.when(self.mine)
        def _():
            wait_bytes(self.slots(N0, 12), self.p2.at[N0])
            plane = self.slots(self.level * N16, N16)
            for k in (N1, N3, N2):
                send(plane, plane, self.s3.at[N0], self.pz.at[self.level], self.to(k, N0, N0, self.core))
        wait_bytes(self.slots(N0, 6), self.p2.at[N1])
        row = self.slots(N32 + self.y * N8, N8)
        for k in (N1, N3, N2):
            send(row, row, self.s3.at[N1], self.py.at[self.y], self.to(N0, k, N0, self.core))

    def plane_ready(self, level):
        @pl.when(jnp.logical_not(jnp.logical_and(self.mine, level == self.level)))
        def _():
            wait_bytes(self.slots(N0, N16), self.pz.at[level])

    def row_ready(self, y):
        @pl.when(y != self.y)
        def _():
            wait_bytes(self.slots(N0, N8), self.py.at[y])

    def sent(self):
        ready(self.mine, self.buf, N3, N4, self.s1)

        @pl.when(self.mine)
        def _():
            wait_bytes(self.slots(N0, 12), self.s2.at[N0])
            wait_bytes(self.slots(N0, 48), self.s3.at[N0])
        wait_bytes(self.slots(N0, 6), self.s2.at[N1])
        wait_bytes(self.slots(N0, 24), self.s3.at[N1])


def slot_device(slot, half):
    first = slot < N32
    rest = slot - N32
    z = jnp.where(first, slot // N16, lax.rem(rest, N2))
    y = jnp.where(first, lax.rem(slot // N4, N4), rest // N8)
    x = jnp.where(first, lax.rem(slot, N4), lax.rem(rest // N2, N4))
    return half * N64 + z * N32 + y * N8 + x * N2 + jnp.where(first, N0, N1)


def kernel(scratch_names, m_ref, z_ref, mask_ref, keep_ref, w_row_in, w_row_bias, w_row_out, w_col_in, w_col_out,
           w_opm_in, w_opm_out, w_s_in, w_s_bias, w_s_out, w_e_in, w_e_bias, w_e_out, m_out, z_out, *scratch):
    r = SimpleNamespace(**dict(zip(scratch_names, scratch)))
    me = my_index()
    core, chip, half = lax.rem(me, N2), me // N2, me // N64
    u, v = me // N8, lax.rem(me, N8)
    slot = me - N64 * half
    mine = core == half
    hrows = pl.ds(pl.multiple_of(core * N256, N256), N256)
    bar = pltpu.get_barrier_semaphore()
    loop(N127, lambda k: pl.semaphore_signal(bar, inc=N1, device_id=dev(lax.rem(me + N1 + k, N128)), device_id_type=MESH))

    for il in range(N4):
        r.slab_f[il * N8:(il + N1) * N8, :] = dot_t(w_row_bias[ALL], layer_norm(z_ref[il]))
    r.slab_a[ALL] = r.slab_f[ALL].astype(BF16)
    for e in range(N2):
        lanes = slice(N512 + e * N256, N768 + e * N256)
        r.wrt[e] = jnp.transpose(w_row_in[:, lanes].astype(F32)).astype(BF16)
    pl.semaphore_wait(bar, N127)
    send(m_ref, r.xm.at[pl.ds(N2 * core, N2)], r.xsem.at[N0], r.xsem.at[N1], me + N1 - N2 * core)

    ga = Gather(r.slab_a, r.bias_a, r.a1, r.a2, r.az3, r.ay3, r.as1, r.as2, r.as3)
    ga.first()
    row = iota(N256, N256, N0)
    r.perm[ALL] = one_hot(iota(N256, N256, N1) == N4 * slot_device(row // N4, N0) + lax.rem(row, N4))
    maskb = mask_ref[ALL].astype(F32).astype(BF16)
    wide = dot_c(maskb, one_hot(iota(N256, N512, N0) == N4 * chip + iota(N256, N512, N1) // N128), N0, N0)
    for e in range(N4):
        r.rmask[e] = wide[:, e * N128:(e + N1) * N128]
        r.cmaskc[e] = dot(maskb, one_hot(iota(N512, N128, N0) == N4 * me + e))
    r.cmask[ALL] = dot_c(one_hot(iota(N4, N512, N1) == N4 * me + iota(N4, N512, N0)), maskb, N1, N1)
    lane = iota(N512, N64, N1)
    mask_j = dot(maskb, one_hot(iota(N512, N64, N0) == N32 * lax.rem(lane, N16) + N4 * v + lane // N16)).astype(BF16)
    mask_i = dot(maskb, one_hot(iota(N512, N32, N0) == N32 * u + iota(N512, N32, N1))).astype(BF16)
    recip = 1.0 / (1e-3 + dot_c(mask_j, mask_i, N0, N0))
    for d in range(N8):
        r.recip[d] = recip[:, d * N4:(d + N1) * N4]

    def project_m(s):
        r.xn_m[ALL] = layer_norm(r.xm[s])
        r.k_m[s] = dot(r.xn_m[ALL], w_row_in[:, N256:N512]).astype(BF16)
        r.v_m[s] = dot_t(r.wrt[N0], r.xn_m[ALL]).astype(BF16)
        xh = dot(r.perm[ALL], r.xn_m[hrows, :]).astype(BF16)
        r.x_half[s] = dot(r.perm[ALL], r.xm[s, hrows, :]).astype(BF16)
        r.q_m[s] = dot(xh, w_row_in[:, N0:N256]).astype(BF16)
        g = dot_t(r.wrt[N1], xh).astype(BF16)
        r.g_m[N0, s] = g[:, N0:N128]
        r.g_m[N1, s] = g[:, N128:N256]

    def own_m(s):
        r.xm[N2 * core + s] = m_ref[s]
        project_m(N2 * core + s)
    loop(N2, own_m)
    ga.second()
    wait_bytes(m_ref, r.xsem.at[N1])
    loop(N2, lambda s: project_m(N2 - N2 * core + s))
    ga.third()

    def block_m(b):
        if b == N1:
            for y in range(N4):
                ga.row_ready(y)
        else:
            for level in range(N2):
                ga.plane_ready(level)
        put(r.wide_a, r.bias_a[pl.ds(b * N32, N32)].astype(F32).reshape(N1024, N512))

        def turn(h):
            for t in range(N4):
                r.bias_t[h, t * N128:(t + N1) * N128, :] = jnp.transpose(r.wide_a[t, pl.ds(h, N128, stride=N8), :]) * LOG2E
        loop(N8, turn)

        def attend_m(s):
            kept = r.rmask[s] > N0
            rows = slice(b * N128, (b + N1) * N128)
            parts = []
            for t in range(N2):
                lanes = slice(t * N128, (t + N1) * N128)
                parts.append(heads_attend(r.q_m[s, rows, lanes], r.k_m[s, :, lanes], r.v_m[s, lanes, :],
                                          lambda h, x, t=t: jnp.where(kept, x + r.bias_t[N4 * t + h], LOW)))
            gated = gate(jnp.concatenate(parts, axis=N0), r.g_m[b, s])
            put(r.y_m, r.x_half[s, rows, :].astype(F32) + dot_c(gated, w_row_out[ALL], N0, N0))
            for jl in range(N4):
                spread(r.f_b, s * N4 + jl, N32, N16, take(r.y_m, jl, N32, N4))
        loop(N4, attend_m)
        r.send_m[b * N32:(b + N1) * N32] = join(r.f_b).astype(BF16).reshape(N32, N16, N256)

        def send_cols_m(k0):
            k = b * N32 + lax.rem(ga.own + N1 + k0, N32)
            q = slot_device(k, core)

            @pl.when(q != me)
            def _():
                send(r.send_m.at[k], r.recv_m.at[chip], r.am.at[N0], r.am.at[N1], q)
        loop(N32, send_cols_m)
    block_m(N1)
    block_m(N0)

    @pl.when(mine)
    def _():
        r.recv_m[chip] = r.send_m[ga.own]

    r.bd[ALL] = jnp.zeros_like(r.bd)
    r.wf[ALL] = w_opm_out[ALL].astype(F32)

    def build(c2):
        for e in range(N2):
            w = r.wf[pl.ds(N2 * c2 + e, N32, stride=N32), :].astype(BF16)
            for il in range(N4):
                r.bd[c2, e * N128 + il * N32:e * N128 + (il + N1) * N32, il * N128:(il + N1) * N128] = w
    loop(N16, build)
    r.rep4[ALL] = head_rep(N128, N4)
    r.hm4[ALL] = head_mask(N512, N4, N128)
    for e in range(N2):
        r.wet[e] = jnp.transpose(w_e_in[:, N256 + e * N128:N384 + e * N128].astype(F32)).astype(BF16)
    keep = jnp.where(iota(N8, N512, N0) == N0, keep_ref[ALL].astype(F32), 0.0).astype(BF16)
    r.keepc[ALL] = dot_c(keep, one_hot(iota(N8, N128, N0) < N8), N0, N0)
    r.keepr[ALL] = keep_ref[ALL].astype(F32)
    for il in range(N4):
        r.zf[il] = z_ref[il].astype(F32)

    def split_z(d):
        for il in range(N4):
            for jl in range(N4):
                r.zsplit[d, jl * N16:(jl + N1) * N16, il * N128:(il + N1) * N128] = r.zf[il, pl.ds(d * N4 + jl, N16, stride=N32), :].astype(BF16)
    loop(N8, split_z)

    for e in range(N2):
        lanes = slice(N512 + e * N256, N768 + e * N256)
        r.wct[e] = jnp.transpose(w_col_in[:, lanes].astype(F32)).astype(BF16)
    ready(mine, r.recv_m, N63, N64, r.am.at[N1])
    def send_z_in(k):
        d = lax.rem(v + N1 + k, N8)
        send(r.zsplit.at[d], r.zin.at[v], r.zsem.at[N0], r.zsem.at[N1], u * N8 + d)
    loop(N7, send_z_in)
    r.zin[v] = r.zsplit[v]

    put(r.xs_m, r.recv_m[ALL].astype(F32).reshape(N1024, N256))

    for jl in range(N4):
        x = take(r.xs_m, jl, N256, N4)
        xn = layer_norm(x)
        qk = dot(xn, w_col_in[:, N0:N512]).astype(BF16)
        vt = dot_t(r.wct[N0], xn).astype(BF16)
        gt = dot_t(r.wct[N1], xn).astype(BF16)
        kept = jnp.concatenate([r.cmaskc[jl], r.cmaskc[jl]], axis=N1) > N0
        parts = []
        for t in range(N2):
            lanes = slice(t * N128, (t + N1) * N128)
            parts.append(heads_attend(qk[:, lanes], qk[:, N256 + t * N128:N384 + t * N128], vt[lanes, :],
                                      lambda h, y, kept=kept: jnp.where(kept, y, LOW)))
        y = (x + dot_c(gate(jnp.concatenate(parts, axis=N0), gt), w_col_out[ALL], N0, N0)).astype(BF16)
        spread(r.yf_m, jl, N256, N4, y.astype(F32))
        ab = dot_t(layer_norm(y), w_opm_in[ALL]).astype(BF16)
        for side, ref in ((N0, r.left), (N1, r.right)):
            pick = one_hot(iota(N32, N64, N1) == iota(N32, N64, N0) + N32 * side)
            ref[jl] = (dot_c(pick, ab, N1, N1) * r.cmask[jl:jl + N1, :]).astype(BF16)

        def send_c(k, jl=jl):
            send(r.right.at[jl], r.rall.at[jl, u], r.csem.at[N0], r.csem.at[N1], lax.rem(u + N1 + k, N16) * N8 + v)
        loop(N15, send_c)

        def send_a(k, jl=jl):
            send(r.left.at[jl], r.lall.at[v, jl], r.lsem.at[N0], r.lsem.at[N1], u * N8 + lax.rem(v + N1 + k, N8))
        loop(N7, send_a)
        r.rall[jl, u] = r.right[jl]
        r.lall[v, jl] = r.left[jl]

    r.mcols[ALL] = join(r.yf_m).astype(BF16).reshape(N128, N8, N256)
    wait_bytes(r.rall.at[:, pl.ds(N0, N15)], r.csem.at[N1])
    wait_bytes(r.lall.at[pl.ds(N0, N7)], r.lsem.at[N1])

    put(r.rf, r.rall[ALL].astype(F32).reshape(N2048, N256))

    def reorder(c):
        r.rc[c] = take(r.rf, c, N64, N32).astype(BF16)
    loop(N32, reorder, N4)

    wait_bytes(r.zin.at[pl.ds(N0, N7)], r.zsem.at[N1])

    def group(g):
        def outer(t):
            d = lax.rem(v + N1 + N4 * g + t, N8)
            r.o[t] = dot_t(r.rc[ALL].reshape(N2048, N256), r.lall[d].reshape(N128, N256)).astype(BF16).reshape(N32, N64, N128)
        loop(N4, outer)

        def mix(c4):
            total = None
            for e in range(N4):
                c = c4 * N8 + N2 * e
                part = dot(jnp.concatenate([r.o[:, c].reshape(N256, N128), r.o[:, c + N1].reshape(N256, N128)], axis=N1), r.bd[c4 * N4 + e])
                total = part if total is None else total + part
            r.acc[ALL] = jnp.where(c4 == N0, 0.0, r.acc[ALL]) + total
        loop(N4, mix)

        def update(t):
            d = lax.rem(v + N1 + N4 * g + t, N8)
            rows = pl.ds(pl.multiple_of(t * N64, N64), N64)
            for il in range(N4):
                cols = slice(il * N128, (il + N1) * N128)
                upd = r.acc[rows, cols] * r.recip[d, :, il:il + N1]
                r.zs[d, :, cols] = (r.zin[d, :, cols].astype(F32) + upd).astype(BF16)

            @pl.when(d != v)
            def _():
                send(r.zs.at[d], r.zback.at[v], r.bsem.at[N0], r.bsem.at[N1], u * N8 + d)
        loop(N4, update)
    loop(N2, group)
    r.zback[v] = r.zs[v]
    wait_bytes(r.zback.at[pl.ds(N0, N7)], r.bsem.at[N1])

    def merge_z(d):
        for il in range(N4):
            for jl in range(N4):
                r.zf[il, pl.ds(d * N4 + jl, N16, stride=N32), :] = r.zback[d, jl * N16:(jl + N1) * N16, il * N128:(il + N1) * N128].astype(F32)
    loop(N8, merge_z)

    for il in range(N4):
        r.zb[il] = r.zf[il].astype(BF16)
        r.e_f[il * N4:(il + N1) * N4, :] = dot_t(w_s_bias[ALL], layer_norm(r.zb[il]))
    r.slab_s[ALL] = r.e_f[N0:N16, :].astype(BF16)
    send(r.zb, r.xz.at[pl.ds(N4 * core, N4)], r.ysem.at[N0], r.ysem.at[N1], me + N1 - N2 * core)

    def send_slab_s(k):
        p = N2 * lax.rem(chip + N1 + k, N64) + half

        @pl.when(p != me)
        def _():
            send(r.slab_s, r.bias_s.at[slot], r.ss, r.gs.at[slot // N32], p)
    loop(N64, send_slab_s)

    @pl.when(mine)
    def _():
        r.bias_s[slot] = r.slab_s[ALL]

    def project_z(i):
        r.xn_z[ALL] = layer_norm(r.xz[i])
        xn = r.xn_z[ALL]
        r.kv_z[i, :, N0:N128] = (dot(xn, w_s_in[:, N128:N256]) * r.keepc[ALL]).astype(BF16)
        r.kv_z[i, :, N128:N256] = dot(xn, w_s_in[:, N256:N384]).astype(BF16)
        xh = r.xn_z[hrows, :]
        r.q_z[i] = dot(xh, w_s_in[:, N0:N128]).astype(BF16)
        r.g_z[i] = dot(xh, w_s_in[:, N384:N512]).astype(BF16)

    def own_z(i):
        r.xz[N4 * core + i] = r.zb[i]
        project_z(N4 * core + i)
    loop(N4, own_z)
    wait_bytes(r.zb, r.ysem.at[N1])
    loop(N4, lambda i: project_z(N4 - N4 * core + i))


    def attend_z(b, i, pv):
        rows = pl.ds(pl.multiple_of(b * N128, N128), N128)
        qx = (dot(r.rep4[ALL], r.q_z[i, rows, :]) * r.hm4[ALL]).astype(BF16)
        t = dot_t(qx, r.kv_z[i, :, N0:N128]) * SCALE + r.biasf[ALL]
        put(pv, dot(softmax_rows(t), r.kv_z[i, :, N128:N256]))
        r.gt_z[i, rows, :] = gate(collapse(pv, N128, N4), r.g_z[i, rows, :])

    def pair_z(b, i2):
        for e in range(N2):
            attend_z(b, N2 * i2 + e, r.pv.at[e, N0:N1])

    def block_z(step):
        b = lax.rem(jnp.where(chip // N32 == core, (chip - N32 * core) // N16, N0) + N1 + step, N2)
        ready(jnp.logical_and(mine, b == slot // N32), r.bias_s, 31, N32, r.gs.at[b])
        got = r.bias_s[pl.ds(b * N32, N32)].reshape(N512, N512).astype(F32)
        r.biasf[ALL] = jnp.where(r.keepr[ALL] > N0, got * LOG2E, LOW)
        loop(N4, lambda i2: pair_z(b, i2))
    loop(N2, block_z)

    for i in range(N8):
        y = (r.xz[i, hrows, :].astype(F32) + dot(r.gt_z[i], w_s_out[ALL])).astype(BF16)
        r.f_z[:, i] = y.astype(F32).reshape(N32, N8, N128)
        spread(r.e_b, i, N4, N8, dot_t(w_e_bias[ALL], layer_norm(y)))
    r.slab_e[ALL] = join(r.e_b).astype(BF16)
    r.send_zc[ALL] = r.f_z[ALL].astype(BF16).reshape(N32, N64, N128)

    def send_cols_z(k0):
        k = N32 * core + lax.rem(chip + N1 + k0, N32)
        q = N2 * k + half

        @pl.when(q != me)
        def _():
            send(r.send_zc.at[k - N32 * core], r.recv_zc.at[chip], r.az.at[N0], r.az.at[N1], q)
    loop(N32, send_cols_z)

    @pl.when(mine)
    def _():
        r.recv_zc[chip] = r.send_zc[chip - N32 * core]

    def send_slab_e(k0):
        send(r.slab_e, r.bias_e.at[chip], r.esem.at[N0], r.esem.at[N1], N2 * lax.rem(chip + N1 + k0, N64) + core)
    loop(N63, send_slab_e)
    r.bias_e[chip] = r.slab_e[ALL]

    ready(mine, r.recv_zc, 31, N32, r.az.at[N1])
    taken = r.recv_zc.at[pl.ds(N32 * core, N32)]
    send(taken, taken, r.fsem.at[N0], r.fsem.at[N1], me + N1 - N2 * core)
    wait_bytes(taken, r.fsem.at[N1])
    r.xs_z[ALL] = r.recv_zc[ALL].astype(F32).reshape(N4096, N128)
    def project_e(j):
        r.xn_z[ALL] = layer_norm(r.xs_z[pl.ds(j, N512, stride=N8), :])
        xn = r.xn_z[ALL]
        r.k_e[j] = (dot(xn, w_e_in[:, N128:N256]) * r.keepc[ALL]).astype(BF16)
        r.v_e[j] = dot_t(r.wet[N0], xn).astype(BF16)
        xh = r.xn_z[hrows, :]
        r.q_z[j] = dot(xh, w_e_in[:, N0:N128]).astype(BF16)
        r.g_e[j] = dot_t(r.wet[N1], xh).astype(BF16)
    loop(N8, project_e)
    wait_bytes(r.bias_e.at[pl.ds(N0, N63)], r.esem.at[N1])

    def widen(b):
        rows = pl.ds(pl.multiple_of(b * N128, N128), N128)
        kept = r.keepc[rows, :].reshape(N16, N8, N128)
        got = r.bias_e[pl.ds(b * N16, N16)].astype(F32).reshape(N16, N4, N8, N256) * LOG2E
        for h in range(N4):
            for t in range(N2):
                lanes = slice(t * N128, (t + N1) * N128)
                r.biasf_e[h, rows, lanes] = jnp.where(kept > N0, got[:, h, :, lanes], LOW).reshape(N128, N128)
    loop(N4, widen)

    def send_m_out(k):
        p = lax.rem(me + N1 + k, N128)
        send(r.mcols.at[p], r.mback.at[me], r.msem.at[N0], r.msem.at[N1], p)
    loop(N127, send_m_out)
    r.mback[me] = r.mcols[me]
    def column(part, j4):
        j = N4 * part + j4
        gated = gate(heads_attend(r.q_z[j], r.k_e[j], r.v_e[j], lambda h, x: x + r.biasf_e[h]), r.g_e[j])
        y = dot_c(gated, w_e_out[ALL], N0, N0)
        r.y_z[part, pl.ds(j4, N256, stride=N4), :] = r.xs_z[pl.ds(core * N2048 + j, N256, stride=N8), :] + y
    for part in range(N2):
        loop(N4, functools.partial(column, part))
        r.send_o[part] = r.y_z[part].astype(BF16).reshape(N64, N16, N128)

        def send_back(k0, part=part):
            k = lax.rem(slot + N1 + k0, N64)
            q = N64 * core + k

            @pl.when(q != me)
            def _():
                send(r.send_o.at[part, k], r.recv_o.at[part, chip], r.osem.at[part], r.oarr.at[part], q)
        loop(N64, send_back)

    @pl.when(mine)
    def _():
        for part in range(N2):
            r.recv_o[part, chip] = r.send_o[part, slot]
    ga.sent()
    ready(mine, r.recv_m, N63, N64, r.am.at[N0])
    ready(mine, r.bias_s, N63, N64, r.ss)
    ready(mine, r.recv_zc, 31, N32, r.az.at[N0])
    wait_bytes(taken, r.fsem.at[N0])
    wait_bytes(m_ref, r.xsem.at[N0])
    wait_bytes(r.zb, r.ysem.at[N0])
    wait_bytes(r.zin.at[pl.ds(N0, N7)], r.zsem.at[N0])
    wait_bytes(r.rall.at[:, pl.ds(N0, N15)], r.csem.at[N0])
    wait_bytes(r.lall.at[pl.ds(N0, N7)], r.lsem.at[N0])
    wait_bytes(r.zback.at[pl.ds(N0, N7)], r.bsem.at[N0])
    wait_bytes(r.mback.at[pl.ds(N0, N127)], r.msem.at[N0])
    wait_bytes(r.bias_e.at[pl.ds(N0, N63)], r.esem.at[N0])
    wait_bytes(r.mback.at[pl.ds(N0, N127)], r.msem.at[N1])
    put(r.yf_m, r.mback[ALL].astype(F32).reshape(N1024, N256))
    for sl in range(N2):
        for jl in range(N4):
            spread(r.f_m, sl * N512 + jl, N128, N4, take(r.yf_m, sl * N4 + jl, N128, N8))
    m_out[ALL] = join(r.f_m).astype(BF16).reshape(N2, N512, N256)

    for part in range(N2):
        ready(mine, r.recv_o.at[part], N63, N64, r.oarr.at[part])
    for part in range(N2):
        r.f_m[part] = r.recv_o[part].astype(F32).reshape(N1024, N128)
        for il in range(N4):
            for j4 in range(N4):
                r.zf[il, pl.ds(N4 * part + j4, N64, stride=N8), :] = r.f_m[part, pl.ds(il * N4 + j4, N64, stride=N16), :]
    for il in range(N4):
        z_out[il] = r.zf[il].astype(BF16)
    for part in range(N2):
        ready(mine, r.recv_o.at[part], N63, N64, r.osem.at[part])


BUFFERS = dict(
    slab_a=(N32, N512), bias_a=(N64, N32, N512), xm=(N4, N512, N256), xn_m=(N512, N256), k_m=(N4, N512, N256), v_m=(N4, N256, N512), q_m=(N4, N256, N256),
    g_m=(N2, N4, N256, N128), wrt=(N2, N256, N256), wct=(N2, N256, N256), perm=(N256, N256), x_half=(N4, N256, N256), zsplit=(N8, N64, N512), zin=(N8, N64, N512), send_m=(N64, N16, N256),
    recv_m=(N64, N16, N256), left=(N4, N32, N256), right=(N4, N32, N256), lall=(N8, N4, N32, N256), rall=(N4, N16, N32, N256),
    mcols=(N128, N8, N256), o=(N4, N32, N64, N128), rc=(N32, N64, N256), mback=(N128, N8, N256), bd=(N16, N256, N512), zs=(N8, N64, N512), zback=(N8, N64, N512), zb=(N4, N512, N128),
    xz=(N8, N512, N128), slab_s=(N16, N512), bias_s=(N64, N16, N512), xn_z=(N512, N128), kv_z=(N8, N512, N256), q_z=(N8, N256, N128),
    g_z=(N8, N256, N128), gt_z=(N8, N256, N128), rep4=(N512, N128), wet=(N2, N128, N128), slab_e=(N32, N256),
    bias_e=(N64, N32, N256), send_zc=(N32, N64, N128), recv_zc=(N64, N64, N128), k_e=(N8, N512, N128), v_e=(N8, N128, N512), g_e=(N8, N128, N256),
    send_o=(N2, N64, N16, N128), recv_o=(N2, N64, N16, N128))
FLOATS = dict(
    slab_f=(N32, N512), rmask=(N4, N512, N128), cmaskc=(N4, N256, N128), wide_a=(N4, N1024, N128), bias_t=(N8, N512, N128), cmask=(N4, N256), recip=(N8, N64, N4), hm4=(N512, N128),
    keepc=(N512, N128), keepr=(N1, N512), zf=(N4, N512, N128), pv=(N4, N2, N512, N128), y_m=(N2, N128, N128), f_b=(N2, N512, N128),
    f_m=(N2, N1024, N128), xs_m=(N2, N1024, N128), yf_m=(N2, N1024, N128), wf=(N1024, N128), rf=(N2, N2048, N128), acc=(N256, N512),
    e_f=(N32, N512), biasf=(N512, N512), f_z=(N32, N8, N8, N128), biasf_e=(N4, N512, N256), e_b=(N2, N32, N128), xs_z=(N4096, N128), y_z=(N2, N1024, N128))
SEMS = dict(a1=N2, a2=N2, az3=N2, ay3=N4, as1=None, as2=N2, as3=N2, gs=N2, ss=None, xsem=N2, ysem=N2, zsem=N2, am=N2, csem=N2, lsem=N2, bsem=N2, msem=N2, az=N2, fsem=N2, esem=N2, osem=N2, oarr=N2)


def solution(mesh):
    rows = P(('data', 'chip', 'dap'))
    in_specs = (rows, rows, P('data'), P('data')) + (P(),) * 13
    specs = {name: pltpu.VMEM(dims, BF16) for name, dims in BUFFERS.items()}
    specs.update({name: pltpu.VMEM(dims, F32) for name, dims in FLOATS.items()})
    specs.update({name: pltpu.SemaphoreType.DMA if n is None else pltpu.SemaphoreType.DMA((n,)) for name, n in SEMS.items()})

    def per_device(m_blk, z_blk, msa_mask, res_mask, *weights):
        w = list(weights)
        for k in (N1, 5, N8, 11):
            w[k] = w[k].T
        args = (m_blk, z_blk, msa_mask, res_mask.reshape(N1, N512), *w)
        vm = pl.BlockSpec(memory_space=pltpu.VMEM)
        return pl.pallas_call(
            functools.partial(kernel, tuple(specs)),
            out_shape=(jax.ShapeDtypeStruct(m_blk.shape, BF16), jax.ShapeDtypeStruct(z_blk.shape, BF16)),
            in_specs=[vm] * len(args), out_specs=(vm, vm), scratch_shapes=list(specs.values()),
            compiler_params=pltpu.CompilerParams(collective_id=N0, has_side_effects=True, vmem_limit_bytes=VMEM_LIMIT),
        )(*args)

    return jax.shard_map(per_device, mesh=mesh, in_specs=in_specs, out_specs=(rows, rows), check_vma=False)
```

```python
import functools
from types import SimpleNamespace

import jax
import jax.numpy as jnp
from jax import lax
from jax.experimental import pallas as pl
from jax.experimental.pallas import tpu as pltpu
from jax.sharding import PartitionSpec as P

N0 = 0
N1 = 1
N2 = 2
N3 = 3
N4 = 4
N7 = 7
N8 = 8
N15 = 15
N16 = 16
N32 = 32
N63 = 63
N64 = 64
N127 = 127
N128 = 128
N256 = 256
N384 = 384
N512 = 512
N768 = 768
N1024 = 1024
N2048 = 2048
N4096 = 4096
ALL = Ellipsis
MESH = pl.DeviceIdType.MESH
F32 = jnp.float32
BF16 = jnp.bfloat16
VMEM_LIMIT = 67043328


def layer_norm(x):
    values = x.astype(F32)
    centred = values - jnp.mean(values, axis=-N1, keepdims=True)
    variance = jnp.mean(centred * centred, axis=-N1, keepdims=True)
    return (centred * lax.rsqrt(variance + 1e-5)).astype(BF16)


def dot(a, b):
    return jnp.dot(a, b, preferred_element_type=F32)


def dot_t(a, b):
    return lax.dot_general(a, b, (((N1,), (N1,)), ((), ())), preferred_element_type=F32)


def dev(p):
    return (N0, p // N8, lax.rem(p, N8))


def my_index():
    return lax.axis_index('chip') * N8 + lax.axis_index('dap')


def loop(n, body, unroll=N1):
    def step(i, carry):
        body(i)
        return carry
    lax.fori_loop(N0, n, step, N0, unroll=unroll)


def send(src, dst, send_sem, recv_sem, p):
    pltpu.make_async_remote_copy(src_ref=src, dst_ref=dst, send_sem=send_sem, recv_sem=recv_sem,
                                 device_id=dev(p), device_id_type=MESH).start()


def wait_bytes(ref, sem):
    pltpu.make_async_copy(ref, ref, sem).wait()


def head_rep(queries, heads):
    rows = queries * heads
    r = lax.broadcasted_iota(jnp.int32, (rows, queries), N0)
    c = lax.broadcasted_iota(jnp.int32, (rows, queries), N1)
    return (r // heads == c).astype(F32).astype(BF16)


def head_mask(rows, heads, width):
    r = lax.broadcasted_iota(jnp.int32, (rows, width), N0)
    c = lax.broadcasted_iota(jnp.int32, (rows, width), N1)
    return (lax.rem(r, heads) == c // N32).astype(F32)


def softmax_rows(t):
    e = jnp.exp2(t - jnp.max(t, axis=N1, keepdims=True))
    return (e * (1.0 / jnp.sum(e, axis=N1, keepdims=True))).astype(BF16)


def put(ref, value):
    for t in range(ref.shape[N0]):
        ref[t] = value[:, t * N128:(t + N1) * N128]


def take(ref, start, size, stride):
    return jnp.concatenate([ref[t, pl.ds(start, size, stride=stride), :] for t in range(ref.shape[N0])], axis=N1)


def join(ref):
    return jnp.concatenate([ref[t] for t in range(ref.shape[N0])], axis=N1)


def spread(ref, start, size, stride, value):
    for t in range(ref.shape[N0]):
        ref[t, pl.ds(start, size, stride=stride), :] = value[:, t * N128:(t + N1) * N128]


def collapse(r_ref, queries, heads):
    lane = lax.broadcasted_iota(jnp.int32, (queries, N128), N1) // N32
    parts = []
    for t in range(r_ref.shape[N0]):
        out = r_ref[t, pl.ds(N4 * t, queries, stride=heads), :]
        for h in range(N1, N4):
            out = jnp.where(lane == h, r_ref[t, pl.ds(N4 * t + h, queries, stride=heads), :], out)
        parts.append(out)
    return jnp.concatenate(parts, axis=N1) if len(parts) > N1 else parts[N0]


def softmax_cols(t):
    e = jnp.exp2(t - jnp.max(t, axis=N0, keepdims=True))
    return (e * (1.0 / jnp.sum(e, axis=N0, keepdims=True))).astype(BF16)


def heads_attend(queries, keys, values, logits):
    lane, row = iota(*queries.shape, N1) // N32, iota(*values.shape, N0) // N32
    wide_q, wide_v = queries.astype(F32), values.astype(F32)
    probs, parts = [], []
    for h in range(N4):
        scores = dot_t(keys, jnp.where(lane == h, wide_q, 0.0).astype(BF16)) * SCALE
        probs.append(softmax_cols(logits(h, scores)))
        parts.append(jnp.where(row == h, wide_v, 0.0).astype(BF16))
    return dot(jnp.concatenate(parts, axis=N1), jnp.concatenate(probs, axis=N0))


def gate(o, g):
    return (o * jax.nn.sigmoid(g.astype(F32))).astype(BF16)


LOG2E = 1.4426950408889634
SCALE = N32 ** -0.5 * LOG2E
LOW = -1e9 * LOG2E


def dot_c(a, b, da, db):
    return lax.dot_general(a, b, (((da,), (db,)), ((), ())), preferred_element_type=F32)


def iota(rows, cols, dim):
    return lax.broadcasted_iota(jnp.int32, (rows, cols), dim)


def one_hot(cond):
    return cond.astype(F32).astype(BF16)


def ready(cond, ref, few, many, sem):
    @pl.when(cond)
    def _():
        wait_bytes(ref.at[pl.ds(N0, few)], sem)

    @pl.when(jnp.logical_not(cond))
    def _():
        wait_bytes(ref.at[pl.ds(N0, many)], sem)


class Gather:
    def __init__(self, slab, buf, p1, p2, pz, py, s1, s2, s3):
        self.slab, self.buf, self.p1, self.p2, self.pz, self.py = slab, buf, p1, p2, pz, py
        self.s1, self.s2, self.s3 = s1, s2, s3
        me = my_index()
        self.me, self.core, chip, self.half = me, lax.rem(me, N2), me // N2, me // N64
        self.x, self.y, self.z = lax.rem(chip, N4), lax.rem(chip // N4, N4), chip // N16
        self.mine = self.core == self.half
        self.level = lax.rem(self.z, N2)
        self.own = jnp.where(self.core == N0, self.level * N16 + self.y * N4 + self.x, N32 + self.y * N8 + self.x * N2 + self.level)

    def to(self, dz, dy, dx, c):
        return N2 * (lax.rem(self.z + dz, N4) * N16 + lax.rem(self.y + dy, N4) * N4 + lax.rem(self.x + dx, N4)) + c

    def slots(self, start, n):
        return self.buf.at[pl.ds(start, n)]

    def first(self):
        for k in (N1, N3, N2, N0):
            p = jnp.where(self.core == N0, self.to(N0, N0, k, self.half), self.to(k, N0, N0, self.half))

            @pl.when(p != self.me)
            def _(p=p):
                send(self.slab, self.buf.at[self.own], self.s1, self.p1.at[self.core], p)

        @pl.when(self.mine)
        def _():
            self.buf[self.own] = self.slab[ALL]

    def second(self):
        @pl.when(self.mine)
        def _():
            ready(self.core == N0, self.buf, N3, N4, self.p1.at[N0])
            line = self.slots(self.level * N16 + self.y * N4, N4)
            for k in (N1, N3, N2):
                send(line, line, self.s2.at[N0], self.p2.at[N0], self.to(N0, k, N0, self.core))
        ready(jnp.logical_and(self.mine, self.core == N1), self.buf, N1, N2, self.p1.at[N1])
        pair = self.slots(N32 + self.y * N8 + self.x * N2, N2)
        for k in (N1, N3, N2):
            send(pair, pair, self.s2.at[N1], self.p2.at[N1], self.to(N0, N0, k, self.core))

    def third(self):
        @pl.when(self.mine)
        def _():
            wait_bytes(self.slots(N0, 12), self.p2.at[N0])
            plane = self.slots(self.level * N16, N16)
            for k in (N1, N3, N2):
                send(plane, plane, self.s3.at[N0], self.pz.at[self.level], self.to(k, N0, N0, self.core))
        wait_bytes(self.slots(N0, 6), self.p2.at[N1])
        row = self.slots(N32 + self.y * N8, N8)
        for k in (N1, N3, N2):
            send(row, row, self.s3.at[N1], self.py.at[self.y], self.to(N0, k, N0, self.core))

    def plane_ready(self, level):
        @pl.when(jnp.logical_not(jnp.logical_and(self.mine, level == self.level)))
        def _():
            wait_bytes(self.slots(N0, N16), self.pz.at[level])

    def row_ready(self, y):
        @pl.when(y != self.y)
        def _():
            wait_bytes(self.slots(N0, N8), self.py.at[y])

    def sent(self):
        ready(self.mine, self.buf, N3, N4, self.s1)

        @pl.when(self.mine)
        def _():
            wait_bytes(self.slots(N0, 12), self.s2.at[N0])
            wait_bytes(self.slots(N0, 48), self.s3.at[N0])
        wait_bytes(self.slots(N0, 6), self.s2.at[N1])
        wait_bytes(self.slots(N0, 24), self.s3.at[N1])


def slot_device(slot, half):
    first = slot < N32
    rest = slot - N32
    z = jnp.where(first, slot // N16, lax.rem(rest, N2))
    y = jnp.where(first, lax.rem(slot // N4, N4), rest // N8)
    x = jnp.where(first, lax.rem(slot, N4), lax.rem(rest // N2, N4))
    return half * N64 + z * N32 + y * N8 + x * N2 + jnp.where(first, N0, N1)


def kernel(scratch_names, m_ref, z_ref, mask_ref, keep_ref, w_row_in, w_row_bias, w_row_out, w_col_in, w_col_out,
           w_opm_in, w_opm_out, w_s_in, w_s_bias, w_s_out, w_e_in, w_e_bias, w_e_out, m_out, z_out, *scratch):
    r = SimpleNamespace(**dict(zip(scratch_names, scratch)))
    me = my_index()
    core, chip, half = lax.rem(me, N2), me // N2, me // N64
    u, v = me // N8, lax.rem(me, N8)
    slot = me - N64 * half
    mine = core == half
    hrows = pl.ds(pl.multiple_of(core * N256, N256), N256)
    bar = pltpu.get_barrier_semaphore()
    loop(N127, lambda k: pl.semaphore_signal(bar, inc=N1, device_id=dev(lax.rem(me + N1 + k, N128)), device_id_type=MESH))

    for il in range(N4):
        r.slab_f[il * N8:(il + N1) * N8, :] = dot_t(w_row_bias[ALL], layer_norm(z_ref[il]))
    r.slab_a[ALL] = r.slab_f[ALL].astype(BF16)
    for e in range(N2):
        lanes = slice(N512 + e * N256, N768 + e * N256)
        r.wrt[e] = jnp.transpose(w_row_in[:, lanes].astype(F32)).astype(BF16)
    pl.semaphore_wait(bar, N127)
    send(m_ref, r.xm.at[pl.ds(N2 * core, N2)], r.xsem.at[N0], r.xsem.at[N1], me + N1 - N2 * core)

    ga = Gather(r.slab_a, r.bias_a, r.a1, r.a2, r.az3, r.ay3, r.as1, r.as2, r.as3)
    ga.first()
    row = iota(N256, N256, N0)
    r.perm[ALL] = one_hot(iota(N256, N256, N1) == N4 * slot_device(row // N4, N0) + lax.rem(row, N4))
    maskb = mask_ref[ALL].astype(F32).astype(BF16)
    wide = dot_c(maskb, one_hot(iota(N256, N512, N0) == N4 * chip + iota(N256, N512, N1) // N128), N0, N0)
    for e in range(N4):
        r.rmask[e] = wide[:, e * N128:(e + N1) * N128]
        r.cmaskc[e] = dot(maskb, one_hot(iota(N512, N128, N0) == N4 * me + e))
    r.cmask[ALL] = dot_c(one_hot(iota(N4, N512, N1) == N4 * me + iota(N4, N512, N0)), maskb, N1, N1)
    lane = iota(N512, N64, N1)
    mask_j = dot(maskb, one_hot(iota(N512, N64, N0) == N32 * lax.rem(lane, N16) + N4 * v + lane // N16)).astype(BF16)
    mask_i = dot(maskb, one_hot(iota(N512, N32, N0) == N32 * u + iota(N512, N32, N1))).astype(BF16)
    recip = 1.0 / (1e-3 + dot_c(mask_j, mask_i, N0, N0))
    for d in range(N8):
        r.recip[d] = recip[:, d * N4:(d + N1) * N4]

    def project_m(s):
        r.xn_m[ALL] = layer_norm(r.xm[s])
        r.k_m[s] = dot(r.xn_m[ALL], w_row_in[:, N256:N512]).astype(BF16)
        r.v_m[s] = dot_t(r.wrt[N0], r.xn_m[ALL]).astype(BF16)
        xh = dot(r.perm[ALL], r.xn_m[hrows, :]).astype(BF16)
        r.x_half[s] = dot(r.perm[ALL], r.xm[s, hrows, :]).astype(BF16)
        r.q_m[s] = dot(xh, w_row_in[:, N0:N256]).astype(BF16)
        g = dot_t(r.wrt[N1], xh).astype(BF16)
        r.g_m[N0, s] = g[:, N0:N128]
        r.g_m[N1, s] = g[:, N128:N256]

    def own_m(s):
        r.xm[N2 * core + s] = m_ref[s]
        project_m(N2 * core + s)
    loop(N2, own_m)
    ga.second()
    wait_bytes(m_ref, r.xsem.at[N1])
    loop(N2, lambda s: project_m(N2 - N2 * core + s))
    ga.third()

    def block_m(b):
        if b == N1:
            for y in range(N4):
                ga.row_ready(y)
        else:
            for level in range(N2):
                ga.plane_ready(level)
        put(r.wide_a, r.bias_a[pl.ds(b * N32, N32)].astype(F32).reshape(N1024, N512))

        def turn(h):
            for t in range(N4):
                r.bias_t[h, t * N128:(t + N1) * N128, :] = jnp.transpose(r.wide_a[t, pl.ds(h, N128, stride=N8), :]) * LOG2E
        loop(N8, turn)

        def attend_m(s):
            kept = r.rmask[s] > N0
            rows = slice(b * N128, (b + N1) * N128)
            parts = []
            for t in range(N2):
                lanes = slice(t * N128, (t + N1) * N128)
                parts.append(heads_attend(r.q_m[s, rows, lanes], r.k_m[s, :, lanes], r.v_m[s, lanes, :],
                                          lambda h, x, t=t: jnp.where(kept, x + r.bias_t[N4 * t + h], LOW)))
            gated = gate(jnp.concatenate(parts, axis=N0), r.g_m[b, s])
            put(r.y_m, r.x_half[s, rows, :].astype(F32) + dot_c(gated, w_row_out[ALL], N0, N0))
            for jl in range(N4):
                spread(r.f_b, s * N4 + jl, N32, N16, take(r.y_m, jl, N32, N4))
        loop(N4, attend_m, N2)
        r.send_m[b * N32:(b + N1) * N32] = join(r.f_b).astype(BF16).reshape(N32, N16, N256)

        def send_cols_m(k0):
            k = b * N32 + lax.rem(ga.own + N1 + k0, N32)
            q = slot_device(k, core)

            @pl.when(q != me)
            def _():
                send(r.send_m.at[k], r.recv_m.at[chip], r.am.at[N0], r.am.at[N1], q)
        loop(N32, send_cols_m)
    block_m(N1)
    block_m(N0)

    @pl.when(mine)
    def _():
        r.recv_m[chip] = r.send_m[ga.own]

    r.bd[ALL] = jnp.zeros_like(r.bd)
    r.wf[ALL] = w_opm_out[ALL].astype(F32)

    def build(c2):
        for e in range(N2):
            w = r.wf[pl.ds(N2 * c2 + e, N32, stride=N32), :].astype(BF16)
            for il in range(N4):
                r.bd[c2, e * N128 + il * N32:e * N128 + (il + N1) * N32, il * N128:(il + N1) * N128] = w
    loop(N16, build)
    r.rep4[ALL] = head_rep(N128, N4)
    r.hm4[ALL] = head_mask(N512, N4, N128)
    for e in range(N2):
        r.wet[e] = jnp.transpose(w_e_in[:, N256 + e * N128:N384 + e * N128].astype(F32)).astype(BF16)
    keep = jnp.where(iota(N8, N512, N0) == N0, keep_ref[ALL].astype(F32), 0.0).astype(BF16)
    r.keepc[ALL] = dot_c(keep, one_hot(iota(N8, N128, N0) < N8), N0, N0)
    r.keepr[ALL] = keep_ref[ALL].astype(F32)
    for il in range(N4):
        r.zf[il] = z_ref[il].astype(F32)

    def split_z(d):
        for il in range(N4):
            for jl in range(N4):
                r.zsplit[d, jl * N16:(jl + N1) * N16, il * N128:(il + N1) * N128] = r.zf[il, pl.ds(d * N4 + jl, N16, stride=N32), :].astype(BF16)
    loop(N8, split_z)

    for e in range(N2):
        lanes = slice(N512 + e * N256, N768 + e * N256)
        r.wct[e] = jnp.transpose(w_col_in[:, lanes].astype(F32)).astype(BF16)
    ready(mine, r.recv_m, N63, N64, r.am.at[N1])
    def send_z_in(k):
        d = lax.rem(v + N1 + k, N8)
        send(r.zsplit.at[d], r.zin.at[v], r.zsem.at[N0], r.zsem.at[N1], u * N8 + d)
    loop(N7, send_z_in)
    r.zin[v] = r.zsplit[v]

    put(r.xs_m, r.recv_m[ALL].astype(F32).reshape(N1024, N256))

    for jl in range(N4):
        x = take(r.xs_m, jl, N256, N4)
        xn = layer_norm(x)
        qk = dot(xn, w_col_in[:, N0:N512]).astype(BF16)
        vt = dot_t(r.wct[N0], xn).astype(BF16)
        gt = dot_t(r.wct[N1], xn).astype(BF16)
        kept = jnp.concatenate([r.cmaskc[jl], r.cmaskc[jl]], axis=N1) > N0
        parts = []
        for t in range(N2):
            lanes = slice(t * N128, (t + N1) * N128)
            parts.append(heads_attend(qk[:, lanes], qk[:, N256 + t * N128:N384 + t * N128], vt[lanes, :],
                                      lambda h, y, kept=kept: jnp.where(kept, y, LOW)))
        y = (x + dot_c(gate(jnp.concatenate(parts, axis=N0), gt), w_col_out[ALL], N0, N0)).astype(BF16)
        spread(r.yf_m, jl, N256, N4, y.astype(F32))
        ab = dot_t(layer_norm(y), w_opm_in[ALL]).astype(BF16)
        for side, ref in ((N0, r.left), (N1, r.right)):
            pick = one_hot(iota(N32, N64, N1) == iota(N32, N64, N0) + N32 * side)
            ref[jl] = (dot_c(pick, ab, N1, N1) * r.cmask[jl:jl + N1, :]).astype(BF16)

        def send_c(k, jl=jl):
            send(r.right.at[jl], r.rall.at[jl, u], r.csem.at[N0], r.csem.at[N1], lax.rem(u + N1 + k, N16) * N8 + v)
        loop(N15, send_c)

        def send_a(k, jl=jl):
            send(r.left.at[jl], r.lall.at[v, jl], r.lsem.at[N0], r.lsem.at[N1], u * N8 + lax.rem(v + N1 + k, N8))
        loop(N7, send_a)
        r.rall[jl, u] = r.right[jl]
        r.lall[v, jl] = r.left[jl]

    r.mcols[ALL] = join(r.yf_m).astype(BF16).reshape(N128, N8, N256)
    wait_bytes(r.rall.at[:, pl.ds(N0, N15)], r.csem.at[N1])
    wait_bytes(r.lall.at[pl.ds(N0, N7)], r.lsem.at[N1])

    put(r.rf, r.rall[ALL].astype(F32).reshape(N2048, N256))

    def reorder(c):
        r.rc[c] = take(r.rf, c, N64, N32).astype(BF16)
    loop(N32, reorder, N8)

    wait_bytes(r.zin.at[pl.ds(N0, N7)], r.zsem.at[N1])

    def group(g):
        def outer(t):
            d = lax.rem(v + N1 + N4 * g + t, N8)
            r.o[t] = dot_t(r.rc[ALL].reshape(N2048, N256), r.lall[d].reshape(N128, N256)).astype(BF16).reshape(N32, N64, N128)
        loop(N4, outer, N4)

        def mix(c4):
            total = None
            for e in range(N4):
                c = c4 * N8 + N2 * e
                part = dot(jnp.concatenate([r.o[:, c].reshape(N256, N128), r.o[:, c + N1].reshape(N256, N128)], axis=N1), r.bd[c4 * N4 + e])
                total = part if total is None else total + part
            r.acc[ALL] = jnp.where(c4 == N0, 0.0, r.acc[ALL]) + total
        loop(N4, mix, N2)

        def update(t):
            d = lax.rem(v + N1 + N4 * g + t, N8)
            rows = pl.ds(pl.multiple_of(t * N64, N64), N64)
            for il in range(N4):
                cols = slice(il * N128, (il + N1) * N128)
                upd = r.acc[rows, cols] * r.recip[d, :, il:il + N1]
                r.zs[d, :, cols] = (r.zin[d, :, cols].astype(F32) + upd).astype(BF16)

            @pl.when(d != v)
            def _():
                send(r.zs.at[d], r.zback.at[v], r.bsem.at[N0], r.bsem.at[N1], u * N8 + d)
        loop(N4, update, N2)
    loop(N2, group)
    r.zback[v] = r.zs[v]
    wait_bytes(r.zback.at[pl.ds(N0, N7)], r.bsem.at[N1])

    def merge_z(d):
        for il in range(N4):
            for jl in range(N4):
                r.zf[il, pl.ds(d * N4 + jl, N16, stride=N32), :] = r.zback[d, jl * N16:(jl + N1) * N16, il * N128:(il + N1) * N128].astype(F32)
    loop(N8, merge_z)

    for il in range(N4):
        r.zb[il] = r.zf[il].astype(BF16)
        r.e_f[il * N4:(il + N1) * N4, :] = dot_t(w_s_bias[ALL], layer_norm(r.zb[il]))
    r.slab_s[ALL] = r.e_f[N0:N16, :].astype(BF16)
    send(r.zb, r.xz.at[pl.ds(N4 * core, N4)], r.ysem.at[N0], r.ysem.at[N1], me + N1 - N2 * core)

    def send_slab_s(k):
        p = N2 * lax.rem(chip + N1 + k, N64) + half

        @pl.when(p != me)
        def _():
            send(r.slab_s, r.bias_s.at[slot], r.ss, r.gs.at[slot // N32], p)
    loop(N64, send_slab_s)

    @pl.when(mine)
    def _():
        r.bias_s[slot] = r.slab_s[ALL]

    def project_z(i):
        r.xn_z[ALL] = layer_norm(r.xz[i])
        xn = r.xn_z[ALL]
        r.kv_z[i, :, N0:N128] = (dot(xn, w_s_in[:, N128:N256]) * r.keepc[ALL]).astype(BF16)
        r.kv_z[i, :, N128:N256] = dot(xn, w_s_in[:, N256:N384]).astype(BF16)
        xh = r.xn_z[hrows, :]
        r.q_z[i] = dot(xh, w_s_in[:, N0:N128]).astype(BF16)
        r.g_z[i] = dot(xh, w_s_in[:, N384:N512]).astype(BF16)

    def own_z(i):
        r.xz[N4 * core + i] = r.zb[i]
        project_z(N4 * core + i)
    loop(N4, own_z)
    wait_bytes(r.zb, r.ysem.at[N1])
    loop(N4, lambda i: project_z(N4 - N4 * core + i))


    def attend_z(b, i, pv):
        rows = pl.ds(pl.multiple_of(b * N128, N128), N128)
        qx = (dot(r.rep4[ALL], r.q_z[i, rows, :]) * r.hm4[ALL]).astype(BF16)
        t = dot_t(qx, r.kv_z[i, :, N0:N128]) * SCALE + r.biasf[ALL]
        put(pv, dot(softmax_rows(t), r.kv_z[i, :, N128:N256]))
        r.gt_z[i, rows, :] = gate(collapse(pv, N128, N4), r.g_z[i, rows, :])

    def pair_z(b, i2):
        for e in range(N2):
            attend_z(b, N2 * i2 + e, r.pv.at[e, N0:N1])

    def block_z(step):
        b = lax.rem(jnp.where(chip // N32 == core, (chip - N32 * core) // N16, N0) + N1 + step, N2)
        ready(jnp.logical_and(mine, b == slot // N32), r.bias_s, 31, N32, r.gs.at[b])
        got = r.bias_s[pl.ds(b * N32, N32)].reshape(N512, N512).astype(F32)
        r.biasf[ALL] = jnp.where(r.keepr[ALL] > N0, got * LOG2E, LOW)
        loop(N4, lambda i2: pair_z(b, i2))
    loop(N2, block_z)

    for i in range(N8):
        y = (r.xz[i, hrows, :].astype(F32) + dot(r.gt_z[i], w_s_out[ALL])).astype(BF16)
        r.f_z[:, i] = y.astype(F32).reshape(N32, N8, N128)
        spread(r.e_b, i, N4, N8, dot_t(w_e_bias[ALL], layer_norm(y)))
    r.slab_e[ALL] = join(r.e_b).astype(BF16)
    r.send_zc[ALL] = r.f_z[ALL].astype(BF16).reshape(N32, N64, N128)

    def send_cols_z(k0):
        k = N32 * core + lax.rem(chip + N1 + k0, N32)
        q = N2 * k + half

        @pl.when(q != me)
        def _():
            send(r.send_zc.at[k - N32 * core], r.recv_zc.at[chip], r.az.at[N0], r.az.at[N1], q)
    loop(N32, send_cols_z)

    @pl.when(mine)
    def _():
        r.recv_zc[chip] = r.send_zc[chip - N32 * core]

    def send_slab_e(k0):
        send(r.slab_e, r.bias_e.at[chip], r.esem.at[N0], r.esem.at[N1], N2 * lax.rem(chip + N1 + k0, N64) + core)
    loop(N63, send_slab_e)
    r.bias_e[chip] = r.slab_e[ALL]

    ready(mine, r.recv_zc, 31, N32, r.az.at[N1])
    taken = r.recv_zc.at[pl.ds(N32 * core, N32)]
    send(taken, taken, r.fsem.at[N0], r.fsem.at[N1], me + N1 - N2 * core)
    wait_bytes(taken, r.fsem.at[N1])
    r.xs_z[ALL] = r.recv_zc[ALL].astype(F32).reshape(N4096, N128)
    def project_e(j):
        r.xn_z[ALL] = layer_norm(r.xs_z[pl.ds(j, N512, stride=N8), :])
        xn = r.xn_z[ALL]
        r.k_e[j] = (dot(xn, w_e_in[:, N128:N256]) * r.keepc[ALL]).astype(BF16)
        r.v_e[j] = dot_t(r.wet[N0], xn).astype(BF16)
        xh = r.xn_z[hrows, :]
        r.q_z[j] = dot(xh, w_e_in[:, N0:N128]).astype(BF16)
        r.g_e[j] = dot_t(r.wet[N1], xh).astype(BF16)
    loop(N8, project_e, N2)
    wait_bytes(r.bias_e.at[pl.ds(N0, N63)], r.esem.at[N1])

    def widen(b):
        rows = pl.ds(pl.multiple_of(b * N128, N128), N128)
        kept = r.keepc[rows, :].reshape(N16, N8, N128)
        got = r.bias_e[pl.ds(b * N16, N16)].astype(F32).reshape(N16, N4, N8, N256) * LOG2E
        for h in range(N4):
            for t in range(N2):
                lanes = slice(t * N128, (t + N1) * N128)
                r.biasf_e[h, rows, lanes] = jnp.where(kept > N0, got[:, h, :, lanes], LOW).reshape(N128, N128)
    loop(N4, widen)

    def send_m_out(k):
        p = lax.rem(me + N1 + k, N128)
        send(r.mcols.at[p], r.mback.at[me], r.msem.at[N0], r.msem.at[N1], p)
    loop(N127, send_m_out)
    r.mback[me] = r.mcols[me]
    def column(part, j4):
        j = N4 * part + j4
        gated = gate(heads_attend(r.q_z[j], r.k_e[j], r.v_e[j], lambda h, x: x + r.biasf_e[h]), r.g_e[j])
        y = dot_c(gated, w_e_out[ALL], N0, N0)
        r.y_z[part, pl.ds(j4, N256, stride=N4), :] = r.xs_z[pl.ds(core * N2048 + j, N256, stride=N8), :] + y
    for part in range(N2):
        loop(N4, functools.partial(column, part), N4)
        r.send_o[part] = r.y_z[part].astype(BF16).reshape(N64, N16, N128)

        def send_back(k0, part=part):
            k = lax.rem(slot + N1 + k0, N64)
            q = N64 * core + k

            @pl.when(q != me)
            def _():
                send(r.send_o.at[part, k], r.recv_o.at[part, chip], r.osem.at[part], r.oarr.at[part], q)
        loop(N64, send_back)

    @pl.when(mine)
    def _():
        for part in range(N2):
            r.recv_o[part, chip] = r.send_o[part, slot]
    ga.sent()
    ready(mine, r.recv_m, N63, N64, r.am.at[N0])
    ready(mine, r.bias_s, N63, N64, r.ss)
    ready(mine, r.recv_zc, 31, N32, r.az.at[N0])
    wait_bytes(taken, r.fsem.at[N0])
    wait_bytes(m_ref, r.xsem.at[N0])
    wait_bytes(r.zb, r.ysem.at[N0])
    wait_bytes(r.zin.at[pl.ds(N0, N7)], r.zsem.at[N0])
    wait_bytes(r.rall.at[:, pl.ds(N0, N15)], r.csem.at[N0])
    wait_bytes(r.lall.at[pl.ds(N0, N7)], r.lsem.at[N0])
    wait_bytes(r.zback.at[pl.ds(N0, N7)], r.bsem.at[N0])
    wait_bytes(r.mback.at[pl.ds(N0, N127)], r.msem.at[N0])
    wait_bytes(r.bias_e.at[pl.ds(N0, N63)], r.esem.at[N0])
    wait_bytes(r.mback.at[pl.ds(N0, N127)], r.msem.at[N1])
    put(r.yf_m, r.mback[ALL].astype(F32).reshape(N1024, N256))
    for sl in range(N2):
        for jl in range(N4):
            spread(r.f_m, sl * N512 + jl, N128, N4, take(r.yf_m, sl * N4 + jl, N128, N8))
    m_out[ALL] = join(r.f_m).astype(BF16).reshape(N2, N512, N256)

    for part in range(N2):
        ready(mine, r.recv_o.at[part], N63, N64, r.oarr.at[part])
    for part in range(N2):
        r.f_m[part] = r.recv_o[part].astype(F32).reshape(N1024, N128)
        for il in range(N4):
            for j4 in range(N4):
                r.zf[il, pl.ds(N4 * part + j4, N64, stride=N8), :] = r.f_m[part, pl.ds(il * N4 + j4, N64, stride=N16), :]
    for il in range(N4):
        z_out[il] = r.zf[il].astype(BF16)
    for part in range(N2):
        ready(mine, r.recv_o.at[part], N63, N64, r.osem.at[part])


BUFFERS = dict(
    slab_a=(N32, N512), bias_a=(N64, N32, N512), xm=(N4, N512, N256), xn_m=(N512, N256), k_m=(N4, N512, N256), v_m=(N4, N256, N512), q_m=(N4, N256, N256),
    g_m=(N2, N4, N256, N128), wrt=(N2, N256, N256), wct=(N2, N256, N256), perm=(N256, N256), x_half=(N4, N256, N256), zsplit=(N8, N64, N512), zin=(N8, N64, N512), send_m=(N64, N16, N256),
    recv_m=(N64, N16, N256), left=(N4, N32, N256), right=(N4, N32, N256), lall=(N8, N4, N32, N256), rall=(N4, N16, N32, N256),
    mcols=(N128, N8, N256), o=(N4, N32, N64, N128), rc=(N32, N64, N256), mback=(N128, N8, N256), bd=(N16, N256, N512), zs=(N8, N64, N512), zback=(N8, N64, N512), zb=(N4, N512, N128),
    xz=(N8, N512, N128), slab_s=(N16, N512), bias_s=(N64, N16, N512), xn_z=(N512, N128), kv_z=(N8, N512, N256), q_z=(N8, N256, N128),
    g_z=(N8, N256, N128), gt_z=(N8, N256, N128), rep4=(N512, N128), wet=(N2, N128, N128), slab_e=(N32, N256),
    bias_e=(N64, N32, N256), send_zc=(N32, N64, N128), recv_zc=(N64, N64, N128), k_e=(N8, N512, N128), v_e=(N8, N128, N512), g_e=(N8, N128, N256),
    send_o=(N2, N64, N16, N128), recv_o=(N2, N64, N16, N128))
FLOATS = dict(
    slab_f=(N32, N512), rmask=(N4, N512, N128), cmaskc=(N4, N256, N128), wide_a=(N4, N1024, N128), bias_t=(N8, N512, N128), cmask=(N4, N256), recip=(N8, N64, N4), hm4=(N512, N128),
    keepc=(N512, N128), keepr=(N1, N512), zf=(N4, N512, N128), pv=(N4, N2, N512, N128), y_m=(N2, N128, N128), f_b=(N2, N512, N128),
    f_m=(N2, N1024, N128), xs_m=(N2, N1024, N128), yf_m=(N2, N1024, N128), wf=(N1024, N128), rf=(N2, N2048, N128), acc=(N256, N512),
    e_f=(N32, N512), biasf=(N512, N512), f_z=(N32, N8, N8, N128), biasf_e=(N4, N512, N256), e_b=(N2, N32, N128), xs_z=(N4096, N128), y_z=(N2, N1024, N128))
SEMS = dict(a1=N2, a2=N2, az3=N2, ay3=N4, as1=None, as2=N2, as3=N2, gs=N2, ss=None, xsem=N2, ysem=N2, zsem=N2, am=N2, csem=N2, lsem=N2, bsem=N2, msem=N2, az=N2, fsem=N2, esem=N2, osem=N2, oarr=N2)


def solution(mesh):
    rows = P(('data', 'chip', 'dap'))
    in_specs = (rows, rows, P('data'), P('data')) + (P(),) * 13
    specs = {name: pltpu.VMEM(dims, BF16) for name, dims in BUFFERS.items()}
    specs.update({name: pltpu.VMEM(dims, F32) for name, dims in FLOATS.items()})
    specs.update({name: pltpu.SemaphoreType.DMA if n is None else pltpu.SemaphoreType.DMA((n,)) for name, n in SEMS.items()})

    def per_device(m_blk, z_blk, msa_mask, res_mask, *weights):
        w = list(weights)
        for k in (N1, 5, N8, 11):
            w[k] = w[k].T
        args = (m_blk, z_blk, msa_mask, res_mask.reshape(N1, N512), *w)
        vm = pl.BlockSpec(memory_space=pltpu.VMEM)
        return pl.pallas_call(
            functools.partial(kernel, tuple(specs)),
            out_shape=(jax.ShapeDtypeStruct(m_blk.shape, BF16), jax.ShapeDtypeStruct(z_blk.shape, BF16)),
            in_specs=[vm] * len(args), out_specs=(vm, vm), scratch_shapes=list(specs.values()),
            compiler_params=pltpu.CompilerParams(collective_id=N0, has_side_effects=True, vmem_limit_bytes=VMEM_LIMIT),
        )(*args)

    return jax.shard_map(per_device, mesh=mesh, in_specs=in_specs, out_specs=(rows, rows), check_vma=False)
```
